128 devices in a mesh: fsdp: 8 (over x, z_lo), tenant: 8 (over y, z_hi), dp: 2 (over core).
Axes of the slice: x: 4, y: 4, z: 4 (z_hi: 2, z_lo: 2; z = z_hi * 2 + z_lo), core: 2. Of those that a mesh axis runs over, the one named last changes fastest.
Arguments:
- tokens: bfloat16 [6144, 5120], P(('fsdp', 'dp'), 'tenant'), may hold values from -6 to 6
- block_tenant_index: int32 [96], P(('fsdp', 'dp')), may hold values from 0 to 7
- ranks: int32 [8], replicated, may hold values from 16 to 64, as said below
- frozen_up_weight: bfloat16 [5120, 14336], P(('fsdp', 'dp'), 'tenant'), may hold values from -0.078125 to 0.078125
- tenant_down_adapters: bfloat16 [8, 64, 5120], P('tenant'), may hold values from -0.078125 to 0.078125
- tenant_up_adapters: bfloat16 [8, 64, 14336], P('tenant'), may hold values from -0.75 to 0.75
- cotangent: bfloat16 [6144, 14336], P(('fsdp', 'dp'), 'tenant'), may hold values from -6 to 6
Outputs:
- hidden_out: bfloat16 [6144, 14336], P(('fsdp', 'dp'), 'tenant')
- grad_tokens: bfloat16 [6144, 5120], P(('fsdp', 'dp'), 'tenant')
- grad_down: float32 [8, 64, 5120], P('dp', None, 'tenant')
- grad_up: float32 [8, 64, 14336], P('dp', None, 'tenant')
The draws below stay inside these ranges and needn't reach their ends.
Inputs may be any that keep to these rules, and one draw needn't show every extreme that they name: `ranks`: multiples of 16; some tenant has rank 64.
All inputs are finite; a program needn't handle non-finite values.
Results may differ from the reference program's by a relative error of at most 0.0034.
Values may be sent and summed in bfloat16 or wider, within the bound.
A program may use at most 128 MiB of HBM per device.

```python
import math
import jax
import jax.numpy as jnp
import numpy as np

MODEL_WIDTH = 5120
HIDDEN_UNITS = 14336
TENANT_COUNT = 8
ADAPTER_RANK = 64
BLOCK = 64
TOKENS = 6144
BLOCKS = 96


def draw_ranks(key, part):
    levels = jax.random.randint(key, (TENANT_COUNT,), 1, ADAPTER_RANK // 16 + 1)
    chosen = jax.random.randint(jax.random.fold_in(key, 7), (), 0, TENANT_COUNT)
    levels = jnp.where(jnp.arange(TENANT_COUNT) == chosen, ADAPTER_RANK // 16, levels)
    return (levels * 16).astype(jnp.int32)


def place_ends(drawn, key, least, high):
    place = [jax.random.randint(jax.random.fold_in(key, axis), (), 0, length) for axis, length in enumerate(drawn.shape)]
    main_axis = drawn.shape.index(max(drawn.shape))
    next_to = place[:main_axis] + [(place[main_axis] + 1) % drawn.shape[main_axis]] + place[main_axis + 1:]
    return drawn.at[tuple(place)].set(least).at[tuple(next_to)].set(high)


def shard_levels(key, extent, shards, smallest, top_value):
    factor_of = 1.0
    for dim, blocks in shards:
        steps = jax.random.uniform(jax.random.fold_in(jax.random.fold_in(key, 6), dim), (blocks,), jnp.float32, smallest / len(shards), top_value / len(shards))
        factor_of = factor_of * jnp.repeat(jnp.exp(steps), extent[dim] // blocks).reshape((-1,) + (1,) * (len(extent) - 1 - dim))
    return factor_of


def rank_table(number_of, lean):
    weights = [(1 << 20) // math.isqrt(grade ** lean) + 1 for grade in range(1, number_of + 1)]
    deviation = 1 + sum(weights) // (1 << 30)
    return np.cumsum(np.array([max(1, weight // deviation) for weight in weights]))


def ranked(stream_key, extent, number_of, skew):
    grid = rank_table(number_of, skew)
    pick = jax.random.randint(jax.random.fold_in(stream_key, 1), extent, 0, int(grid[number_of - 1]))
    rank = jnp.searchsorted(jnp.asarray(grid, jnp.int32), pick, side="right")
    return jax.random.permutation(jax.random.fold_in(stream_key, 2), number_of)[rank].astype(jnp.int32)


def centred(stream_key, extent, spread, most, shards=(), kind=jnp.bfloat16):
    result = spread * jax.random.normal(stream_key, extent, jnp.float32)
    if shards:
        result = result * shard_levels(stream_key, extent, shards, -0.22, 0.18)
    return jnp.clip(result, -most, most).astype(kind)


def setup_inputs(seed: int = 0) -> dict:
    splits = jax.random.split(jax.random.key(seed), 8)
    return {
        "tokens": centred(splits[0], (TOKENS, MODEL_WIDTH), 1.0, 6.0, ((0, 16), (1, 8))),
        "block_tenant_index": place_ends(ranked(splits[1], (BLOCKS,), TENANT_COUNT, 2), jax.random.fold_in(splits[1], 3), 0, TENANT_COUNT - 1).astype(jnp.int32),
        "ranks": draw_ranks(jax.random.fold_in(splits[7], 71), 0),
        "frozen_up_weight": centred(splits[3], (MODEL_WIDTH, HIDDEN_UNITS), MODEL_WIDTH ** -0.5, 0.078125, ((0, 16), (1, 8))),
        "tenant_down_adapters": centred(splits[4], (TENANT_COUNT, ADAPTER_RANK, MODEL_WIDTH), MODEL_WIDTH ** -0.5, 0.078125, ((0, 8),)),
        "tenant_up_adapters": centred(splits[5], (TENANT_COUNT, ADAPTER_RANK, HIDDEN_UNITS), ADAPTER_RANK ** -0.5, 0.75, ((0, 8),)),
        "cotangent": centred(splits[6], (TOKENS, HIDDEN_UNITS), 1.0, 6.0, ((0, 16), (1, 8))),
    }


alpha_scale = 32.0


def make_gain(block_tenant_index, ranks):
    rows_tenant = jnp.repeat(block_tenant_index, BLOCK, total_repeat_length=TOKENS)
    columns = jnp.arange(TENANT_COUNT * ADAPTER_RANK, dtype=jnp.int32)
    col_tenant = columns // ADAPTER_RANK
    col_slot = columns % ADAPTER_RANK
    ranks_col = jnp.repeat(ranks, ADAPTER_RANK, total_repeat_length=TENANT_COUNT * ADAPTER_RANK)
    keep = (rows_tenant[:, None] == col_tenant[None, :]) & (col_slot[None, :] < ranks_col[None, :])
    scale_col = alpha_scale / ranks_col.astype(jnp.float32)
    return jnp.where(keep, scale_col[None, :], jnp.float32(0.0))


def reference(tokens, block_tenant_index, ranks, frozen_up_weight, tenant_down_adapters, tenant_up_adapters, cotangent):
    gain = make_gain(block_tenant_index, ranks)
    flattened_down = tenant_down_adapters.reshape(TENANT_COUNT * ADAPTER_RANK, MODEL_WIDTH)
    flattened_up = tenant_up_adapters.reshape(TENANT_COUNT * ADAPTER_RANK, HIDDEN_UNITS)
    proj = jnp.dot(tokens, flattened_down.T, preferred_element_type=jnp.float32)
    adapted = (proj * gain).astype(jnp.bfloat16)
    base = jnp.dot(tokens, frozen_up_weight, preferred_element_type=jnp.float32)
    hidden_out = (base + jnp.dot(adapted, flattened_up, preferred_element_type=jnp.float32)).astype(jnp.bfloat16)
    back = jnp.dot(cotangent, flattened_up.T, preferred_element_type=jnp.float32)
    adapted_grad = (back * gain).astype(jnp.bfloat16)
    grad_base = jnp.dot(cotangent, frozen_up_weight.T, preferred_element_type=jnp.float32)
    grad_tokens = (grad_base + jnp.dot(adapted_grad, flattened_down, preferred_element_type=jnp.float32)).astype(jnp.bfloat16)
    grad_up = jnp.dot(adapted.T, cotangent, preferred_element_type=jnp.float32).reshape(TENANT_COUNT, ADAPTER_RANK, HIDDEN_UNITS)
    grad_down = jnp.dot(adapted_grad.T, tokens, preferred_element_type=jnp.float32).reshape(TENANT_COUNT, ADAPTER_RANK, MODEL_WIDTH)
    return hidden_out, grad_tokens, grad_down, grad_up
```

```python
import jax
import jax.numpy as jnp
from jax import lax
from jax.experimental import pallas as pl
from jax.experimental.pallas import tpu as pltpu
from jax.sharding import PartitionSpec as P

MESH = pl.DeviceIdType.MESH
BF = jnp.bfloat16
F32 = jnp.float32
BLOCK = 64
ALPHA = 32.0
ROUNDS = 5
SUB = 64


def dot(a, b, ca, cb):
    return lax.dot_general(a, b, (((ca,), (cb,)), ((), ())), preferred_element_type=F32)


def kernel(
    bti,
    ranks,
    tokr,
    tok_h,
    w_h,
    dq_h,
    u_h,
    cot_h,
    hid_out,
    gt_out,
    gd_out,
    gu_out,
    tok,
    dq,
    cot,
    wall,
    tokq,
    uall,
    hacc,
    gsend,
    gown,
    grecv,
    gzs,
    gzr,
    gcomp,
    cp2,
    brecv,
    agx,
    agj,
    agexp,
    asend,
    arecv,
    aexp,
    gpart,
    gpr,
    rss,
    rsr,
    agg,
    lsem,
    wss,
    wrs,
    prs,
    tss,
    trs,
    uss,
    urs,
    upss,
    uprs,
    bss,
    brs,
    ass_,
    ars,
    dss,
    drs,
    gss,
    grs,
    zss,
    zrs,
    xss,
    xrs,
    rss_s,
    rss_r,
    ags_s,
    ags_r,
):
    f = lax.axis_index("fsdp")
    j = lax.axis_index("tenant")
    c = lax.axis_index("dp")
    rows = cot.shape[0]
    half = rows // 2
    lf = cot.shape[1]

    def ring(i):
        flip = 1 - 2 * lax.rem(i, 2)
        right, left, opp = lax.rem(i + 2, 8), lax.rem(i + 6, 8), lax.rem(i + 4, 8)
        return dict(
            Z=i + flip,
            R=right,
            L=left,
            O=opp,
            RZ=right + flip,
            LZ=left + flip,
            OZ=opp + flip,
        )

    fn, tn = ring(f), ring(j)
    y, zh = j // 2, lax.rem(j, 2)
    partner = {"dp": 1 - c}

    def rc(src, dst, ss, rs, dev):
        return pltpu.make_async_remote_copy(
            src_ref=src, dst_ref=dst, send_sem=ss, recv_sem=rs, device_id=dev, device_id_type=MESH
        )

    def each(lo, hi, body):
        def step(k, carry):
            body(k)
            return carry

        lax.fori_loop(lo, hi, step, 0)

    sent = []

    def go(src, dst, ss, rs, dev):
        d = rc(src, dst, ss, rs, dev)
        d.start()
        sent.append(d)

    def got(dst, rs):
        rc(dst, dst, rs, rs, partner).wait_recv()

    def slot(q, fi, ci):
        return wall.at[q, pl.ds((2 * fi + ci) * SUB, SUB)]

    def part(q, fi, ci, h):
        return wall.at[q, pl.ds((2 * fi + ci) * SUB + h * (SUB // 2), SUB // 2)]

    wloc = [
        pltpu.make_async_copy(w_h.at[pl.ds(q * SUB, SUB)], slot(q, f, c), lsem.at[q])
        for q in range(ROUNDS)
    ]
    tloc = pltpu.make_async_copy(tokr, tokq.at[j], lsem.at[5])
    uloc = pltpu.make_async_copy(
        u_h.at[:, pl.ds(pl.multiple_of(j * lf, 128), lf)], uall.at[j], lsem.at[6]
    )
    cloc = pltpu.make_async_copy(cot_h, cot, lsem.at[7])
    dloc = pltpu.make_async_copy(dq_h, dq, lsem.at[8])
    kloc = pltpu.make_async_copy(tok_h, tok, lsem.at[9])
    for d in [*wloc, tloc, uloc, cloc, dloc, kloc]:
        d.start()

    barrier = pltpu.get_barrier_semaphore()
    for k in range(1, 8):
        pl.semaphore_signal(barrier, 1, device_id={"fsdp": lax.rem(f + k, 8)}, device_id_type=MESH)
        pl.semaphore_signal(
            barrier, 1, device_id={"tenant": lax.rem(j + k, 8)}, device_id_type=MESH
        )
    pl.semaphore_signal(barrier, 1, device_id=partner, device_id_type=MESH)
    pl.semaphore_wait(barrier, 15)

    def fs(i):
        return {"fsdp": fn[i]}

    def w_send(q, name, i, rsem, to, src=None):
        ref = slot(q, fn[name] if name else f, c) if src is None else src
        go(ref, ref, wss.at[q, i], rsem, to)

    def w_got(q, k, ref):
        got(ref, wrs.at[q, k])

    def w_A(q):
        wloc[q].wait()
        w_send(q, None, 0, wrs.at[q, 1], fs("R"))
        w_send(q, None, 1, wrs.at[q, 2], fs("L"))
        w_send(q, None, 2, wrs.at[q, 0], fs("Z"))
        w_send(q, None, 3, prs.at[q, 0], partner)

    def w_B(q):
        w_got(q, 0, slot(q, fn["Z"], c))
        w_send(q, "Z", 4, wrs.at[q, 3], fs("R"))
        w_send(q, "Z", 5, wrs.at[q, 4], fs("L"))
        w_send(q, "Z", 6, prs.at[q, 1], partner)

    def w_CD(q, left, right, kl, kr, kt, kb, i, p):
        w_got(q, kl, slot(q, fn[left], c))
        w_send(q, left, i, wrs.at[q, kt], fs("R"), part(q, fn[left], c, 0))
        w_send(q, left, i + 1, prs.at[q, p], partner)
        w_got(q, kr, slot(q, fn[right], c))
        w_send(q, right, i + 2, wrs.at[q, kb], fs("L"), part(q, fn[right], c, 1))
        w_send(q, right, i + 3, prs.at[q, p + 1], partner)

    def w_C(q):
        w_CD(q, "L", "R", 1, 2, 5, 6, 7, 2)

    def w_D(q):
        w_CD(q, "LZ", "RZ", 3, 4, 7, 8, 11, 4)

    def w_E(q):
        for name, k, i, p in (("O", 5, 15, 6), ("OZ", 7, 16, 7)):
            w_got(q, k, part(q, fn[name], c, 0))
            w_got(q, k + 1, part(q, fn[name], c, 1))
            w_send(q, name, i, prs.at[q, p], partner)

    def w_P(q):
        for p, name in enumerate((None, "Z", "L", "R", "LZ", "RZ", "O", "OZ")):
            got(slot(q, fn[name] if name else f, 1 - c), prs.at[q, p])

    def te(i):
        return {"tenant": tn[i]}

    def t_send(ji, i, k, to, h=None):
        ref = tokq.at[ji] if h is None else tokq.at[ji, :, pl.ds(h * half, half)]
        go(ref, ref, tss.at[i], trs.at[k], to)

    def t_A():
        tloc.wait()
        t_send(j, 2, 0, te("Z"))
        t_send(j, 0, 1, te("R"))
        t_send(j, 1, 2, te("L"))

    def t_B():
        got(tokq.at[tn["Z"]], trs.at[0])
        t_send(tn["Z"], 3, 3, te("R"))
        t_send(tn["Z"], 4, 4, te("L"))

    def t_CD(left, right, kl, kr, kt, kb, i):
        got(tokq.at[tn[left]], trs.at[kl])
        t_send(tn[left], i, kt, te("R"), 0)
        got(tokq.at[tn[right]], trs.at[kr])
        t_send(tn[right], i + 1, kb, te("L"), 1)

    def t_E():
        for name, k in (("O", 5), ("OZ", 7)):
            for h in range(2):
                got(tokq.at[tn[name], :, pl.ds(h * half, half)], trs.at[k + h])

    def u_half(ji, ci):
        return uall.at[ji, pl.ds(ci * 32, 32)]

    def u_desc(k):
        to = lax.rem(j + k, 8)
        return rc(
            u_h.at[pl.ds(c * 32, 32), pl.ds(pl.multiple_of(to * lf, 128), lf)],
            u_half(j, c),
            uss.at[k],
            urs.at[k],
            {"tenant": to},
        )

    def up_desc(k):
        ref = u_half(lax.rem(j + 8 - k, 8), c)
        return rc(ref, ref, upss.at[k], uprs.at[k], partner)

    def u_recv(k):
        got(u_half(lax.rem(j + 8 - k, 8), c), urs.at[k])
        up_desc(k).start()

    def tenant_is(b, t, shape):
        return jnp.full(shape, bti[b], jnp.int32) == t

    def make_gain():
        lane = lax.broadcasted_iota(jnp.int32, (BLOCK, BLOCK), 1)
        gains = []
        for t in range(8):
            r = jnp.full((BLOCK, BLOCK), ranks[t], jnp.int32)
            gains.append(jnp.where(lane < r, ALPHA / r.astype(F32), 0.0))
        for b in range(6):
            g = jnp.zeros((BLOCK, BLOCK), F32)
            for t in range(8):
                g = jnp.where(tenant_is(b, t, g.shape), gains[t], g)
            gcomp[pl.ds(b * BLOCK, BLOCK), :] = g

    def back_part():
        for h in range(2):
            u = uall[pl.ds(4 * h, 4)].reshape(256, lf)
            p = dot(cot[...], u, 1, 1)
            for b in range(6):
                rs = slice(b * BLOCK, (b + 1) * BLOCK)
                acc = jnp.zeros((BLOCK, BLOCK), F32)
                for t in range(4):
                    acc = jnp.where(
                        tenant_is(b, 4 * h + t, acc.shape), p[rs, 64 * t : 64 * t + 64], acc
                    )
                at = (slice(rs.start % half, rs.start % half + BLOCK), slice(64 * (b // 3), 64 * (b // 3) + 64))
                cp2[at] = acc if h == 0 else cp2[at] + acc

    def b_desc(k):
        to = lax.rem(j + k, 8)
        return rc(cp2.at[pl.ds(to * 24, 24)], brecv.at[k], bss.at[k], brs.at[k], {"tenant": to})

    def b_sum():
        s = cp2[pl.ds(pl.multiple_of(j * 24, 8), 24), :]
        for k in range(1, 8):
            got(brecv.at[k], brs.at[k])
            s = s + brecv[k]
        agx[j] = s

    def ag_desc(k):
        return rc(agx.at[j], agx.at[j], ass_.at[k], ars.at[k], {"tenant": lax.rem(j + k, 8)})

    def ag_use():
        for k in range(1, 8):
            got(agx.at[lax.rem(j + 8 - k, 8)], ars.at[k])
        packed = jnp.concatenate([agx[k] for k in range(8)], axis=0)
        for b in range(6):
            r0 = (b % 3) * BLOCK
            s = packed[r0 : r0 + BLOCK, 64 * (b // 3) : 64 * (b // 3) + 64]
            v = (s * gcomp[b * BLOCK : (b + 1) * BLOCK, :]).astype(BF).astype(F32)
            zero = jnp.zeros_like(v)
            rs = slice(b * BLOCK, (b + 1) * BLOCK)
            agj[rs, :] = jnp.where(tenant_is(b, j, v.shape), v, zero).astype(BF)
            for t in range(0, 8, 2):
                pair = jnp.concatenate(
                    [jnp.where(tenant_is(b, t + e, v.shape), v, zero) for e in range(2)], axis=1
                )
                agexp[rs, 64 * t : 64 * t + 128] = pair.astype(BF)

    def lhs(q):
        return jnp.concatenate([tokq[i, q] for i in range(8)], axis=1)

    def adapted_part():
        p = dot(lhs(0), dq[0], 1, 1)
        for q in range(1, ROUNDS):
            p = p + dot(lhs(q), dq[q], 1, 1)
        outs = []
        for b in range(6):
            rs = slice(b * BLOCK, (b + 1) * BLOCK)
            v = p[rs] * gcomp[rs, :]
            outs.append(jnp.where(tenant_is(b, j, v.shape), v, jnp.zeros_like(v)))
        for b in range(3):
            pair = jnp.concatenate([outs[b], outs[b + 3]], axis=1).astype(BF)
            asend[b * BLOCK : (b + 1) * BLOCK, :] = pair
            arecv[j, pl.ds(b * BLOCK, BLOCK), :] = pair

    def d_desc(k):
        return rc(asend, arecv.at[j], dss.at[k], drs.at[k], {"tenant": lax.rem(j + k, 8)})

    def adapted_use():
        for k in range(1, 8):
            got(arecv.at[lax.rem(j + 8 - k, 8)], drs.at[k])
        for t in range(0, 8, 2):
            a0, a1 = arecv[t], arecv[t + 1]
            aexp[:half, 64 * t : 64 * t + 128] = jnp.concatenate([a0[:, :64], a1[:, :64]], axis=1)
            aexp[half:, 64 * t : 64 * t + 128] = jnp.concatenate([a0[:, 64:], a1[:, 64:]], axis=1)

    def grad_down_part():
        p = dot(agexp[...], tok[...], 0, 0)
        gpart[0, :, 0:640] = p[:256]
        gpart[1, :, 0:640] = p[256:]

    def grad_up_part():
        def body(n):
            at = pl.ds(pl.multiple_of(n * 256, 256), 256)
            to = pl.ds(pl.multiple_of(640 + n * 256, 128), 256)
            p = dot(aexp[...], cot[:, at], 0, 0)
            gpart[0, :, to] = p[:256]
            gpart[1, :, to] = p[256:]

        each(0, lf // 256, body)

    def rs_make():
        got(gpr, xrs)

        def body(k):
            at = pl.ds(pl.multiple_of(k * 32, 32), 32)
            rss[k] = (gpart[c, at, :] + gpr[at, :]).astype(BF)

        each(0, 8, body)

    def rs_desc(k):
        to = lax.rem(f + k, 8)
        return rc(rss.at[to], rsr.at[k], rss_s.at[k], rss_r.at[k], {"fsdp": to})

    def rs_sum():
        at = pl.ds(pl.multiple_of(f * 32, 32), 32)
        for k in range(1, 8):
            got(rsr.at[k], rss_r.at[k])
        s = gpart[c, at, :] + gpr[at, :]
        for k in range(1, 8):
            s = s + rsr[k].astype(F32)
        agg[f] = s.astype(BF)

    def gg_desc(k):
        return rc(agg.at[f], agg.at[f], ags_s.at[k], ags_r.at[k], {"fsdp": lax.rem(f + k, 8)})

    def grads_out():
        for k in range(1, 8):
            got(agg.at[lax.rem(f + 8 - k, 8)], ags_r.at[k])

        def body(k):
            at = pl.ds(pl.multiple_of(k * 32, 32), 32)
            v = agg[k].astype(F32)
            gd_out[at, :] = v[:, :640]
            gu_out[at, :] = v[:, 640:]

        each(0, 8, body)

    def g_desc(q, i):
        rel = lax.rem(y - i + 4, 4) - 1
        return rc(
            gsend.at[q, i], grecv.at[q, rel], gss.at[q, i], grs.at[q, rel], {"tenant": 2 * i + zh}
        )

    def compute_g(q):
        def body(k):
            i = lax.rem(y + k, 4)
            at = pl.ds(pl.multiple_of(i * 256, 256), 256)
            p = dot(cot[...], wall[q, at, :], 1, 1) + dot(agj[...], dq[q, :, at], 1, 0)

            @pl.when(k < 4)
            def _():
                gsend[q, i] = p.astype(BF)
                g_desc(q, i).start()

            @pl.when(k == 4)
            def _():
                gown[q] = p

        each(1, 5, body)

    def compute_h(q):
        def body(n):
            at = pl.ds(pl.multiple_of(n * 256, 256), 256)
            p = dot(lhs(q), wall[q, :, at], 1, 0)
            if q == 0:
                hacc[:, at] = p
            elif q < ROUNDS - 1:
                hacc[:, at] += p
            else:
                u = uall[:, :, at].reshape(512, 256)
                hid_out[:, at] = (hacc[:, at] + p + dot(aexp[...], u, 1, 0)).astype(BF)

        each(0, lf // 256, body)

    def compute(q):
        w_P(q)
        compute_g(q)
        compute_h(q)

    def g_sum(q):
        for k in range(3):
            got(grecv.at[q, k], grs.at[q, k])
        mine = pl.ds(pl.multiple_of(zh * 128, 128), 128)
        other = pl.ds(pl.multiple_of(128 - zh * 128, 128), 128)

        def total(at):
            s = gown[q, :, at]
            for k in range(3):
                s = s + grecv[q, k, :, at].astype(F32)
            return s

        gzs[q] = total(other).astype(BF)
        go(gzs.at[q], gzr.at[q], zss.at[q], zrs.at[q], te("Z"))
        gown[q, :, mine] = total(mine)

    def gt_final():
        mine = pl.ds(pl.multiple_of(zh * 128, 128), 128)
        for q in range(ROUNDS):
            got(gzr.at[q], zrs.at[q])

        def body(b):
            at = pl.ds(pl.multiple_of(b * BLOCK, BLOCK), BLOCK)
            s = [gown[q, at, mine] + gzr[q, at, :].astype(F32) for q in range(ROUNDS)]
            row = jnp.concatenate([v[:, :64] for v in s] + [v[:, 64:] for v in s], axis=1)
            gt_out[at, :] = row.astype(BF)

        each(0, 6, body)

    w_A(0)
    w_A(1)
    each(1, 8, lambda k: u_desc(k).start())
    t_A()
    make_gain()

    w_B(0)
    w_C(0)
    w_A(2)
    t_B()
    w_D(0)

    w_B(1)
    w_C(1)
    w_A(3)
    each(1, 8, u_recv)
    t_CD("L", "R", 1, 2, 5, 6, 5)
    w_D(1)
    w_E(0)
    uloc.wait()
    cloc.wait()
    each(1, 8, lambda k: got(u_half(lax.rem(j + 8 - k, 8), 1 - c), uprs.at[k]))
    back_part()
    each(1, 8, lambda k: b_desc(k).start())

    w_B(2)
    w_C(2)
    w_A(4)
    b_sum()
    each(1, 8, lambda k: ag_desc(k).start())
    t_CD("LZ", "RZ", 3, 4, 7, 8, 7)
    w_D(2)
    w_E(1)
    ag_use()
    kloc.wait()
    grad_down_part()
    t_E()
    dloc.wait()
    adapted_part()
    each(1, 8, lambda k: d_desc(k).start())
    compute(0)

    w_B(3)
    w_C(3)
    w_D(3)
    w_E(2)
    adapted_use()
    grad_up_part()
    go(gpart.at[1 - c], gpr, xss, xrs, partner)
    compute(1)

    w_B(4)
    w_C(4)
    rs_make()
    each(1, 8, lambda k: rs_desc(k).start())
    w_D(4)
    w_E(3)
    compute(2)
    g_sum(0)
    compute(3)
    g_sum(1)

    w_E(4)
    rs_sum()
    each(1, 8, lambda k: gg_desc(k).start())
    g_sum(2)
    compute(4)
    g_sum(3)
    g_sum(4)
    grads_out()
    gt_final()

    for d in sent:
        d.wait_send()
    each(1, 8, lambda k: u_desc(k).wait_send())
    each(1, 8, lambda k: up_desc(k).wait_send())
    each(1, 8, lambda k: b_desc(k).wait_send())
    each(1, 8, lambda k: ag_desc(k).wait_send())
    each(1, 8, lambda k: d_desc(k).wait_send())
    each(1, 8, lambda k: rs_desc(k).wait_send())
    each(1, 8, lambda k: gg_desc(k).wait_send())
    for q in range(ROUNDS):
        each(1, 4, lambda k: g_desc(q, lax.rem(y + k, 4)).wait_send())


def shards(tokens, bti, ranks, w, down, up, cot):
    rows, ld = tokens.shape
    lf = cot.shape[1]
    d = down.shape[2]
    tokr = tokens.reshape(rows, 2, ROUNDS, SUB).transpose(2, 0, 1, 3).reshape(ROUNDS, rows, 128)
    dq = down.reshape(64, 8, 2, ROUNDS, SUB).transpose(3, 0, 1, 2, 4).reshape(ROUNDS, 64, 1024)
    up = up.reshape(64, up.shape[2])
    dma = pltpu.SemaphoreType.DMA
    vm = pltpu.VMEM
    smem = pl.BlockSpec(memory_space=pltpu.SMEM)
    hbm = pl.BlockSpec(memory_space=pl.ANY)
    out = pl.BlockSpec(memory_space=pltpu.VMEM)
    half = rows // 2
    hid, gt, gd, gu = pl.pallas_call(
        kernel,
        out_shape=(
            jax.ShapeDtypeStruct((rows, lf), BF),
            jax.ShapeDtypeStruct((rows, ld), BF),
            jax.ShapeDtypeStruct((256, ld), F32),
            jax.ShapeDtypeStruct((256, lf), F32),
        ),
        in_specs=[smem, smem, hbm, hbm, hbm, hbm, hbm, hbm],
        out_specs=(out, out, out, out),
        scratch_shapes=[
            vm((rows, ld), BF),
            vm((ROUNDS, 64, 1024), BF),
            vm((rows, lf), BF),
            vm((ROUNDS, 1024, lf), BF),
            vm((8, ROUNDS, rows, 128), BF),
            vm((8, 64, lf), BF),
            vm((rows, lf), F32),
            vm((ROUNDS, 4, rows, 256), BF),
            vm((ROUNDS, rows, 256), F32),
            vm((ROUNDS, 3, rows, 256), BF),
            vm((ROUNDS, rows, 128), BF),
            vm((ROUNDS, rows, 128), BF),
            vm((rows, 64), F32),
            vm((half, 128), F32),
            vm((8, 24, 128), F32),
            vm((8, 24, 128), F32),
            vm((rows, 64), BF),
            vm((rows, 512), BF),
            vm((half, 128), BF),
            vm((8, half, 128), BF),
            vm((rows, 512), BF),
            vm((2, 256, ld + lf), F32),
            vm((256, ld + lf), F32),
            vm((8, 32, ld + lf), BF),
            vm((8, 32, ld + lf), BF),
            vm((8, 32, ld + lf), BF),
            dma((10,)),
            dma((ROUNDS, 17)),
            dma((ROUNDS, 9)),
            dma((ROUNDS, 8)),
            dma((9,)),
            dma((9,)),
            dma((8,)),
            dma((8,)),
            dma((8,)),
            dma((8,)),
            dma((8,)),
            dma((8,)),
            dma((8,)),
            dma((8,)),
            dma((8,)),
            dma((8,)),
            dma((ROUNDS, 4)),
            dma((ROUNDS, 3)),
            dma((ROUNDS,)),
            dma((ROUNDS,)),
            dma,
            dma,
            dma((8,)),
            dma((8,)),
            dma((8,)),
            dma((8,)),
        ],
        compiler_params=pltpu.CompilerParams(
            collective_id=0, has_side_effects=True, vmem_limit_bytes=67043328
        ),
    )(bti, ranks, tokr, tokens, w, dq, up, cot)
    return hid, gt, gd.reshape(4, 64, ld), gu.reshape(4, 64, lf)


def solution(mesh):
    return jax.shard_map(
        shards,
        mesh=mesh,
        in_specs=(
            P(("fsdp", "dp"), "tenant"),
            P(("fsdp", "dp")),
            P(),
            P(("fsdp", "dp"), "tenant"),
            P("tenant", None, None),
            P("tenant", None, None),
            P(("fsdp", "dp"), "tenant"),
        ),
        out_specs=(
            P(("fsdp", "dp"), "tenant"),
            P(("fsdp", "dp"), "tenant"),
            P("dp", None, "tenant"),
            P("dp", None, "tenant"),
        ),
        check_vma=False,
    )
```

```python
import jax
import jax.numpy as jnp
from jax import lax
from jax.experimental import pallas as pl
from jax.experimental.pallas import tpu as pltpu
from jax.sharding import PartitionSpec as P

MESH = pl.DeviceIdType.MESH
BF = jnp.bfloat16
F32 = jnp.float32
BLOCK = 64
ALPHA = 32.0
ROUNDS = 5
SUB = 64


def dot(a, b, ca, cb):
    return lax.dot_general(a, b, (((ca,), (cb,)), ((), ())), preferred_element_type=F32)


def kernel(
    bti,
    ranks,
    tok_h,
    w_h,
    d_h,
    u_h,
    cot_h,
    hid_out,
    gt_out,
    gd_out,
    gu_out,
    tok,
    dq,
    cot,
    wall,
    tokq,
    dmine,
    uall,
    dall,
    ux,
    dx,
    hacc,
    gsend,
    gown,
    grecv,
    gzs,
    gzr,
    gcomp,
    cp2,
    brecv,
    agx,
    agj,
    agexp,
    aexp,
    gpart,
    gpr,
    rss,
    rsr,
    agg,
    lsem,
    wss,
    wrs,
    prs,
    tss,
    trs,
    uss,
    urs,
    upss,
    uprs,
    bss,
    brs,
    ass_,
    ars,
    gss,
    grs,
    zss,
    zrs,
    xss,
    xrs,
    rss_s,
    rss_r,
    ags_s,
    ags_r,
):
    f = lax.axis_index("fsdp")
    j = lax.axis_index("tenant")
    c = lax.axis_index("dp")
    rows = cot.shape[0]
    half = rows // 2
    lf, ld = cot.shape[1], tok.shape[1]

    def ring(i):
        flip = 1 - 2 * lax.rem(i, 2)
        right, left, opp = lax.rem(i + 2, 8), lax.rem(i + 6, 8), lax.rem(i + 4, 8)
        return dict(
            Z=i + flip,
            R=right,
            L=left,
            O=opp,
            RZ=right + flip,
            LZ=left + flip,
            OZ=opp + flip,
        )

    fn, tn = ring(f), ring(j)
    y, zh = j // 2, lax.rem(j, 2)
    partner = {"dp": 1 - c}

    def rc(src, dst, ss, rs, dev):
        return pltpu.make_async_remote_copy(
            src_ref=src, dst_ref=dst, send_sem=ss, recv_sem=rs, device_id=dev, device_id_type=MESH
        )

    def each(lo, hi, body):
        def step(k, carry):
            body(k)
            return carry

        lax.fori_loop(lo, hi, step, 0)

    sent = []

    def go(src, dst, ss, rs, dev):
        d = rc(src, dst, ss, rs, dev)
        d.start()
        sent.append(d)

    def got(dst, rs):
        rc(dst, dst, rs, rs, partner).wait_recv()

    def slot(q, fi, ci):
        return wall.at[q, pl.ds((2 * fi + ci) * SUB, SUB)]

    def part(q, fi, ci, h):
        return wall.at[q, pl.ds((2 * fi + ci) * SUB + h * (SUB // 2), SUB // 2)]

    wloc = [
        pltpu.make_async_copy(w_h.at[pl.ds(q * SUB, SUB)], slot(q, f, c), lsem.at[q])
        for q in range(ROUNDS)
    ]
    ucol = pl.ds(pl.multiple_of(j * lf, 128), lf)
    dcol = pl.ds(pl.multiple_of(j * ld, 128), ld)
    kloc = pltpu.make_async_copy(tok_h, tok, lsem.at[5])
    mloc = pltpu.make_async_copy(d_h, dmine, lsem.at[6])
    uloc = pltpu.make_async_copy(u_h.at[:, ucol], uall.at[j], lsem.at[7])
    dloc = pltpu.make_async_copy(d_h.at[:, dcol], dall.at[j], lsem.at[8])
    cloc = pltpu.make_async_copy(cot_h, cot, lsem.at[9])
    for d in [*wloc, kloc, mloc, uloc, dloc, cloc]:
        d.start()

    barrier = pltpu.get_barrier_semaphore()
    for k in range(1, 8):
        pl.semaphore_signal(barrier, 1, device_id={"fsdp": lax.rem(f + k, 8)}, device_id_type=MESH)
        pl.semaphore_signal(
            barrier, 1, device_id={"tenant": lax.rem(j + k, 8)}, device_id_type=MESH
        )
    pl.semaphore_signal(barrier, 1, device_id=partner, device_id_type=MESH)
    pl.semaphore_signal(
        barrier, 1, device_id={"fsdp": fn["Z"], "tenant": tn["Z"]}, device_id_type=MESH
    )
    pl.semaphore_wait(barrier, 16)

    def fs(i):
        return {"fsdp": fn[i]}

    def w_send(q, name, i, rsem, to, src=None):
        ref = slot(q, fn[name] if name else f, c) if src is None else src
        go(ref, ref, wss.at[q, i], rsem, to)

    def w_got(q, k, ref):
        got(ref, wrs.at[q, k])

    def w_A(q):
        wloc[q].wait()
        w_send(q, None, 0, wrs.at[q, 1], fs("R"))
        w_send(q, None, 1, wrs.at[q, 2], fs("L"))
        w_send(q, None, 2, wrs.at[q, 0], fs("Z"))
        w_send(q, None, 3, prs.at[q, 0], partner)

    def w_B(q):
        w_got(q, 0, slot(q, fn["Z"], c))
        w_send(q, "Z", 4, wrs.at[q, 3], fs("R"))
        w_send(q, "Z", 5, wrs.at[q, 4], fs("L"))
        w_send(q, "Z", 6, prs.at[q, 1], partner)

    def w_CD(q, left, right, kl, kr, kt, kb, i, p):
        w_got(q, kl, slot(q, fn[left], c))
        w_send(q, left, i, wrs.at[q, kt], fs("R"), part(q, fn[left], c, 0))
        w_send(q, left, i + 1, prs.at[q, p], partner)
        w_got(q, kr, slot(q, fn[right], c))
        w_send(q, right, i + 2, wrs.at[q, kb], fs("L"), part(q, fn[right], c, 1))
        w_send(q, right, i + 3, prs.at[q, p + 1], partner)

    def w_C(q):
        w_CD(q, "L", "R", 1, 2, 5, 6, 7, 2)

    def w_D(q):
        w_CD(q, "LZ", "RZ", 3, 4, 7, 8, 11, 4)

    def w_E(q):
        for name, k, i, p in (("O", 5, 15, 6), ("OZ", 7, 16, 7)):
            w_got(q, k, part(q, fn[name], c, 0))
            w_got(q, k + 1, part(q, fn[name], c, 1))
            w_send(q, name, i, prs.at[q, p], partner)

    def w_P(q):
        for p, name in enumerate((None, "Z", "L", "R", "LZ", "RZ", "O", "OZ")):
            got(slot(q, fn[name] if name else f, 1 - c), prs.at[q, p])

    def te(i):
        return {"tenant": tn[i]}

    def t_send(ji, i, k, to, h=None):
        ref = tokq.at[ji] if h is None else tokq.at[ji, :, pl.ds(h * half, half)]
        go(ref, ref, tss.at[i], trs.at[k], to)

    def pieces(v):
        return [
            jnp.concatenate([v[:, SUB * q : SUB * q + SUB], v[:, 320 + SUB * q : 384 + SUB * q]], axis=1)
            for q in range(ROUNDS)
        ]

    def t_make():
        kloc.wait()
        for q, v in enumerate(pieces(tok[...])):
            tokq[j, q] = v

    def dq_make():
        mloc.wait()
        for i in range(8):
            for q, v in enumerate(pieces(dmine[:, ld * i : ld * i + ld])):
                dq[q, :, 128 * i : 128 * i + 128] = v

    def t_A():
        t_send(j, 0, 1, te("R"))
        t_send(j, 1, 2, te("L"))

    def t_Z():
        t_send(j, 2, 0, te("Z"))

    def t_B():
        got(tokq.at[tn["Z"]], trs.at[0])
        t_send(tn["Z"], 3, 3, te("R"))
        t_send(tn["Z"], 4, 4, te("L"))

    def t_CD(left, right, kl, kr, kt, kb, i):
        got(tokq.at[tn[left]], trs.at[kl])
        t_send(tn[left], i, kt, te("R"), 0)
        got(tokq.at[tn[right]], trs.at[kr])
        t_send(tn[right], i + 1, kb, te("L"), 1)

    def t_C():
        t_CD("L", "R", 1, 2, 5, 6, 5)

    def t_D():
        t_CD("LZ", "RZ", 3, 4, 7, 8, 7)

    def t_E():
        for name, k in (("O", 5), ("OZ", 7)):
            for h in range(2):
                got(tokq.at[tn[name], :, pl.ds(h * half, half)], trs.at[k + h])

    def adapter(src, width, all_, relay, s):
        def own(ji, ci):
            return all_.at[ji, pl.ds(ci * 32, 32)]

        def out(ji):
            return src.at[pl.ds(c * 32, 32), pl.ds(pl.multiple_of(ji * width, 128), width)]

        return own, out, relay, s

    kinds = (adapter(d_h, ld, dall, dx, 0), adapter(u_h, lf, uall, ux, 10))
    cross = {"fsdp": fn["Z"], "tenant": tn["Z"]}

    def at_y(r):
        return lax.rem(y + r, 4)

    def u_cross():
        for own, out, relay, s in kinds:
            for r in range(4):
                dst = own(j, c) if r == 0 else relay.at[r]
                go(out(2 * at_y(r) + 1 - zh), dst, uss.at[s + r], urs.at[s + r], cross)

    def u_own():
        for own, out, relay, s in kinds:
            for r in range(1, 4):
                to, k = 2 * at_y(r) + zh, s + 3 + r
                go(out(to), own(j, c), uss.at[k], urs.at[k], {"tenant": to})

    def u_fwd():
        for own, out, relay, s in kinds:
            for r in range(1, 4):
                got(relay.at[r], urs.at[s + r])
                to, k = 2 * at_y(r) + zh, s + 6 + r
                go(relay.at[r], own(tn["Z"], c), uss.at[k], urs.at[k], {"tenant": to})

    def u_slots(s):
        yield tn["Z"], s, s
        for r in range(1, 4):
            yield 2 * at_y(4 - r) + zh, s + 3 + r, s + r
        for r in range(1, 4):
            yield 2 * at_y(4 - r) + 1 - zh, s + 6 + r, s + 3 + r

    def u_recv():
        for own, out, relay, s in kinds:
            for ji, k, p in u_slots(s):
                got(own(ji, c), urs.at[k])
                go(own(ji, c), own(ji, c), upss.at[p], uprs.at[p], partner)

    def u_from_partner():
        for own, out, relay, s in kinds:
            for ji, k, p in u_slots(s):
                got(own(ji, 1 - c), uprs.at[p])

    def tenant_is(b, t, shape):
        return jnp.full(shape, bti[b], jnp.int32) == t

    def make_gain():
        lane = lax.broadcasted_iota(jnp.int32, (BLOCK, BLOCK), 1)
        gains = []
        for t in range(8):
            r = jnp.full((BLOCK, BLOCK), ranks[t], jnp.int32)
            gains.append(jnp.where(lane < r, ALPHA / r.astype(F32), 0.0))
        for b in range(6):
            g = jnp.zeros((BLOCK, BLOCK), F32)
            for t in range(8):
                g = jnp.where(tenant_is(b, t, g.shape), gains[t], g)
            gcomp[pl.ds(b * BLOCK, BLOCK), :] = g

    def compact(w, a, all_):
        for h in range(2):
            u = all_[pl.ds(4 * h, 4)].reshape(256, a.shape[1])
            p = dot(a[...], u, 1, 1)
            for b in range(6):
                rs = slice(b * BLOCK, (b + 1) * BLOCK)
                acc = jnp.zeros((BLOCK, BLOCK), F32)
                for t in range(4):
                    acc = jnp.where(
                        tenant_is(b, 4 * h + t, acc.shape), p[rs, 64 * t : 64 * t + 64], acc
                    )
                r0, l0 = (b % 3) * BLOCK, 64 * (b // 3)
                at = (w, slice(r0, r0 + BLOCK), slice(l0, l0 + 64))
                cp2[at] = acc if h == 0 else cp2[at] + acc

    def b_desc(k):
        to = lax.rem(j + k, 8)
        return rc(
            cp2.at[:, pl.ds(to * 24, 24)], brecv.at[k], bss.at[k], brs.at[k], {"tenant": to}
        )

    def b_sum():
        s = cp2[:, pl.ds(pl.multiple_of(j * 24, 8), 24), :]
        for k in range(1, 8):
            got(brecv.at[k], brs.at[k])
            s = s + brecv[k]
        agx[j] = s

    def ag_desc(k):
        return rc(agx.at[j], agx.at[j], ass_.at[k], ars.at[k], {"tenant": lax.rem(j + k, 8)})

    def ag_use():
        for k in range(1, 8):
            got(agx.at[lax.rem(j + 8 - k, 8)], ars.at[k])
        for w, dst in ((0, agexp), (1, aexp)):
            packed = jnp.concatenate([agx[k, w] for k in range(8)], axis=0)
            for b in range(6):
                r0 = (b % 3) * BLOCK
                s = packed[r0 : r0 + BLOCK, 64 * (b // 3) : 64 * (b // 3) + 64]
                v = (s * gcomp[b * BLOCK : (b + 1) * BLOCK, :]).astype(BF).astype(F32)
                zero = jnp.zeros_like(v)
                rs = slice(b * BLOCK, (b + 1) * BLOCK)
                if w == 0:
                    agj[rs, :] = jnp.where(tenant_is(b, j, v.shape), v, zero).astype(BF)
                for t in range(0, 8, 2):
                    pair = jnp.concatenate(
                        [jnp.where(tenant_is(b, t + e, v.shape), v, zero) for e in range(2)], axis=1
                    )
                    dst[rs, 64 * t : 64 * t + 128] = pair.astype(BF)

    def lhs(q):
        return jnp.concatenate([tokq[i, q] for i in range(8)], axis=1)

    def grad_down_part():
        p = dot(agexp[...], tok[...], 0, 0)
        gpart[0, :, 0:ld] = p[:256]
        gpart[1, :, 0:ld] = p[256:]

    def grad_up_part(lo, hi):
        def body(n):
            at = pl.ds(pl.multiple_of(n * 256, 256), 256)
            to = pl.ds(pl.multiple_of(ld + n * 256, 128), 256)
            p = dot(aexp[...], cot[:, at], 0, 0)
            gpart[0, :, to] = p[:256]
            gpart[1, :, to] = p[256:]

        each(lo, hi, body)

    fx, fz = f // 2, lax.rem(f, 2)
    cols = (pl.ds(0, 1152), pl.ds(1152, 1280))

    def gx(p):
        go(gpart.at[1 - c, :, cols[p]], gpr.at[:, cols[p]], xss.at[p], xrs.at[p], partner)

    def chunk(k, p):
        at = pl.ds(pl.multiple_of(k * 32, 32), 32)
        return gpart[c, at, cols[p]] + gpr[at, cols[p]]

    def rs_z(p):
        got(gpr.at[:, cols[p]], xrs.at[p])

        def body(k):
            rss[k, :, cols[p]] = chunk(2 * k + 1 - fz, p).astype(BF)

        each(0, 4, body)
        at = (pl.ds(0, 4), slice(None), cols[p])
        go(rss.at[at], rsr.at[at], rss_s.at[p, 0], rss_r.at[p, 0], fs("Z"))

    def fx_to(r):
        return {"fsdp": lax.rem(f + 2 * r, 8)}

    def rs_x(p):
        got(rsr.at[pl.ds(0, 4), :, cols[p]], rss_r.at[p, 0])
        for r in range(1, 4):
            k = lax.rem(fx + r, 4)
            rss[3 + r, :, cols[p]] = (
                chunk(2 * k + fz, p) + rsr[k, :, cols[p]].astype(F32)
            ).astype(BF)
            at = (3 + r, slice(None), cols[p])
            go(rss.at[at], rsr.at[at], rss_s.at[p, r], rss_r.at[p, r], fx_to(r))

    def rs_sum(p):
        s = chunk(f, p) + rsr[fx, :, cols[p]].astype(F32)
        for r in range(1, 4):
            got(rsr.at[3 + r, :, cols[p]], rss_r.at[p, r])
            s = s + rsr[3 + r, :, cols[p]].astype(F32)
        agg[f, :, cols[p]] = s.astype(BF)
        ref = agg.at[f, :, cols[p]]
        for r in range(1, 4):
            go(ref, ref, ags_s.at[p, r], ags_r.at[p, r], fx_to(r))
        go(ref, ref, ags_s.at[p, 4], ags_r.at[p, 4], fs("Z"))

    def ag_z(p):
        for r in range(1, 4):
            ref = agg.at[lax.rem(f + 8 - 2 * r, 8), :, cols[p]]
            got(ref, ags_r.at[p, r])
            go(ref, ref, ags_s.at[p, 4 + r], ags_r.at[p, 4 + r], fs("Z"))

    def grads_out(p):
        got(agg.at[fn["Z"], :, cols[p]], ags_r.at[p, 4])
        for r in range(1, 4):
            got(agg.at[lax.rem(fn["Z"] + 8 - 2 * r, 8), :, cols[p]], ags_r.at[p, 4 + r])

        def body(k):
            at = pl.ds(pl.multiple_of(k * 32, 32), 32)
            v = agg[k, :, cols[p]].astype(F32)
            if p == 0:
                gd_out[at, :] = v[:, :ld]
                gu_out[at, 0:512] = v[:, ld:]
            else:
                gu_out[at, 512:] = v

        each(0, 8, body)

    def g_desc(q, i):
        rel = lax.rem(y - i + 4, 4) - 1
        return rc(
            gsend.at[q, i], grecv.at[q, rel], gss.at[q, i], grs.at[q, rel], {"tenant": 2 * i + zh}
        )

    def compute_g(q):
        def body(k):
            i = lax.rem(y + k, 4)
            at = pl.ds(pl.multiple_of(i * 256, 256), 256)
            p = dot(cot[...], wall[q, at, :], 1, 1) + dot(agj[...], dq[q, :, at], 1, 0)

            @pl.when(k < 4)
            def _():
                gsend[q, i] = p.astype(BF)
                g_desc(q, i).start()

            @pl.when(k == 4)
            def _():
                gown[q] = p

        each(1, 5, body)

    def compute_h(q):
        def body(n):
            at = pl.ds(pl.multiple_of(n * 256, 256), 256)
            p = dot(lhs(q), wall[q, :, at], 1, 0)
            if q == 0:
                hacc[:, at] = p
            elif q < ROUNDS - 1:
                hacc[:, at] += p
            else:
                u = uall[:, :, at].reshape(512, 256)
                hid_out[:, at] = (hacc[:, at] + p + dot(aexp[...], u, 1, 0)).astype(BF)

        each(0, lf // 256, body)

    def g_sum(q):
        for k in range(3):
            got(grecv.at[q, k], grs.at[q, k])
        mine = pl.ds(pl.multiple_of(zh * 128, 128), 128)
        other = pl.ds(pl.multiple_of(128 - zh * 128, 128), 128)

        def total(at):
            s = gown[q, :, at]
            for k in range(3):
                s = s + grecv[q, k, :, at].astype(F32)
            return s

        gzs[q] = total(other).astype(BF)
        go(gzs.at[q], gzr.at[q], zss.at[q], zrs.at[q], te("Z"))
        gown[q, :, mine] = total(mine)

    def gt_final():
        mine = pl.ds(pl.multiple_of(zh * 128, 128), 128)
        for q in range(ROUNDS):
            got(gzr.at[q], zrs.at[q])

        def body(b):
            at = pl.ds(pl.multiple_of(b * BLOCK, BLOCK), BLOCK)
            s = [gown[q, at, mine] + gzr[q, at, :].astype(F32) for q in range(ROUNDS)]
            row = jnp.concatenate([v[:, :64] for v in s] + [v[:, 64:] for v in s], axis=1)
            gt_out[at, :] = row.astype(BF)

        each(0, 6, body)

    w_A(0)
    u_cross()
    u_own()
    t_make()
    t_A()
    w_A(1)
    make_gain()
    dq_make()

    w_B(0)
    w_C(0)
    w_A(2)
    u_fwd()
    t_Z()
    w_D(0)
    t_C()

    w_B(1)
    w_C(1)
    w_A(3)
    u_recv()
    uloc.wait()
    dloc.wait()
    cloc.wait()
    u_from_partner()
    compact(0, cot, uall)
    compact(1, tok, dall)
    each(1, 8, lambda k: b_desc(k).start())
    w_D(1)
    w_E(0)
    b_sum()
    each(1, 8, lambda k: ag_desc(k).start())
    t_B()

    w_B(2)
    w_C(2)
    w_A(4)
    ag_use()
    grad_down_part()
    grad_up_part(0, 2)
    gx(0)
    t_D()
    w_D(2)
    w_E(1)
    grad_up_part(2, 7)
    gx(1)
    w_P(0)
    compute_g(0)
    rs_z(0)
    w_B(3)
    w_C(3)
    rs_z(1)
    w_P(1)
    compute_g(1)
    w_D(3)
    w_E(2)
    rs_x(0)
    t_E()
    compute_h(0)
    g_sum(0)
    w_B(4)
    w_C(4)
    rs_x(1)
    w_P(2)
    compute_g(2)
    rs_sum(0)
    compute_h(1)
    g_sum(1)
    rs_sum(1)
    w_D(4)
    w_E(3)
    w_P(3)
    compute_g(3)
    ag_z(0)
    compute_h(2)
    g_sum(2)
    ag_z(1)
    w_E(4)
    w_P(4)
    compute_g(4)
    compute_h(3)
    g_sum(3)
    grads_out(0)
    compute_h(4)
    grads_out(1)
    g_sum(4)
    gt_final()

    for d in sent:
        d.wait_send()
    each(1, 8, lambda k: b_desc(k).wait_send())
    each(1, 8, lambda k: ag_desc(k).wait_send())
    for q in range(ROUNDS):
        each(1, 4, lambda k: g_desc(q, lax.rem(y + k, 4)).wait_send())


def shards(tokens, bti, ranks, w, down, up, cot):
    rows, ld = tokens.shape
    lf = cot.shape[1]
    up = up.reshape(up.shape[1:])
    down = down.reshape(down.shape[1:])
    dma = pltpu.SemaphoreType.DMA
    vm = pltpu.VMEM
    smem = pl.BlockSpec(memory_space=pltpu.SMEM)
    hbm = pl.BlockSpec(memory_space=pl.ANY)
    out = pl.BlockSpec(memory_space=pltpu.VMEM)
    half = rows // 2
    hid, gt, gd, gu = pl.pallas_call(
        kernel,
        out_shape=(
            jax.ShapeDtypeStruct((rows, lf), BF),
            jax.ShapeDtypeStruct((rows, ld), BF),
            jax.ShapeDtypeStruct((256, ld), F32),
            jax.ShapeDtypeStruct((256, lf), F32),
        ),
        in_specs=[smem, smem, hbm, hbm, hbm, hbm, hbm],
        out_specs=(out, out, out, out),
        scratch_shapes=[
            vm((rows, ld), BF),
            vm((ROUNDS, 64, 1024), BF),
            vm((rows, lf), BF),
            vm((ROUNDS, 1024, lf), BF),
            vm((8, ROUNDS, rows, 128), BF),
            vm((64, 5120), BF),
            vm((8, 64, lf), BF),
            vm((8, 64, ld), BF),
            vm((4, 32, lf), BF),
            vm((4, 32, ld), BF),
            vm((rows, lf), F32),
            vm((ROUNDS, 4, rows, 256), BF),
            vm((ROUNDS, rows, 256), F32),
            vm((ROUNDS, 3, rows, 256), BF),
            vm((ROUNDS, rows, 128), BF),
            vm((ROUNDS, rows, 128), BF),
            vm((rows, 64), F32),
            vm((2, half, 128), F32),
            vm((8, 2, 24, 128), F32),
            vm((8, 2, 24, 128), F32),
            vm((rows, 64), BF),
            vm((rows, 512), BF),
            vm((rows, 512), BF),
            vm((2, 256, ld + lf), F32),
            vm((256, ld + lf), F32),
            vm((8, 32, ld + lf), BF),
            vm((8, 32, ld + lf), BF),
            vm((8, 32, ld + lf), BF),
            dma((10,)),
            dma((ROUNDS, 17)),
            dma((ROUNDS, 9)),
            dma((ROUNDS, 8)),
            dma((9,)),
            dma((9,)),
            dma((20,)),
            dma((20,)),
            dma((17,)),
            dma((17,)),
            dma((8,)),
            dma((8,)),
            dma((8,)),
            dma((8,)),
            dma((ROUNDS, 4)),
            dma((ROUNDS, 3)),
            dma((ROUNDS,)),
            dma((ROUNDS,)),
            dma((2,)),
            dma((2,)),
            dma((2, 4)),
            dma((2, 4)),
            dma((2, 8)),
            dma((2, 8)),
        ],
        compiler_params=pltpu.CompilerParams(
            collective_id=0, has_side_effects=True, vmem_limit_bytes=67043328
        ),
    )(bti, ranks, tokens, w, down, up, cot)
    return hid, gt, gd.reshape(4, 64, ld), gu.reshape(4, 64, lf)


def solution(mesh):
    return jax.shard_map(
        shards,
        mesh=mesh,
        in_specs=(
            P(("fsdp", "dp"), "tenant"),
            P(("fsdp", "dp")),
            P(),
            P(("fsdp", "dp"), "tenant"),
            P("tenant", None, None),
            P("tenant", None, None),
            P(("fsdp", "dp"), "tenant"),
        ),
        out_specs=(
            P(("fsdp", "dp"), "tenant"),
            P(("fsdp", "dp"), "tenant"),
            P("dp", None, "tenant"),
            P("dp", None, "tenant"),
        ),
        check_vma=False,
    )
```

```python
import jax
import jax.numpy as jnp
from jax import lax
from jax.experimental import pallas as pl
from jax.experimental.pallas import tpu as pltpu
from jax.sharding import PartitionSpec as P

MESH = pl.DeviceIdType.MESH
BF = jnp.bfloat16
F32 = jnp.float32
BLOCK = 64
ALPHA = 32.0
ROUNDS = 5
SUB = 64


def dot(a, b, ca, cb):
    return lax.dot_general(a, b, (((ca,), (cb,)), ((), ())), preferred_element_type=F32)


def kernel(
    bti,
    ranks,
    tok_h,
    w_h,
    d_h,
    u_h,
    cot_h,
    hid_out,
    gt_out,
    gd_out,
    gu_out,
    tok,
    dq,
    cot,
    wall,
    tokq,
    dmine,
    uall,
    dall,
    ux,
    dx,
    hacc,
    gsend,
    gown,
    grecv,
    gzs,
    gzr,
    gcomp,
    cp2,
    brecv,
    agx,
    agj,
    agexp,
    aexp,
    gpart,
    gpr,
    rss,
    rsr,
    agg,
    lsem,
    wss,
    wrs,
    prs,
    tss,
    trs,
    uss,
    urs,
    upss,
    uprs,
    bss,
    brs,
    ass_,
    ars,
    gss,
    grs,
    zss,
    zrs,
    xss,
    xrs,
    rss_s,
    rss_r,
    ags_s,
    ags_r,
):
    f = lax.axis_index("fsdp")
    j = lax.axis_index("tenant")
    c = lax.axis_index("dp")
    rows = cot.shape[0]
    half = rows // 2
    lf, ld = cot.shape[1], tok.shape[1]

    def ring(i):
        flip = 1 - 2 * lax.rem(i, 2)
        right, left, opp = lax.rem(i + 2, 8), lax.rem(i + 6, 8), lax.rem(i + 4, 8)
        return dict(
            Z=i + flip,
            R=right,
            L=left,
            O=opp,
            RZ=right + flip,
            LZ=left + flip,
            OZ=opp + flip,
        )

    fn, tn = ring(f), ring(j)
    y, zh = j // 2, lax.rem(j, 2)
    partner = {"dp": 1 - c}

    def rc(src, dst, ss, rs, dev):
        return pltpu.make_async_remote_copy(
            src_ref=src, dst_ref=dst, send_sem=ss, recv_sem=rs, device_id=dev, device_id_type=MESH
        )

    def each(lo, hi, body):
        def step(k, carry):
            body(k)
            return carry

        lax.fori_loop(lo, hi, step, 0)

    def go(src, dst, ss, rs, dev):
        rc(src, dst, ss, rs, dev).start()

    def gone(ref, ss):
        rc(ref, ref, ss, ss, partner).wait_send()

    def got(dst, rs):
        rc(dst, dst, rs, rs, partner).wait_recv()

    def slot(q, fi, ci):
        return wall.at[q, pl.ds((2 * fi + ci) * SUB, SUB)]

    def part(q, fi, ci, h):
        return wall.at[q, pl.ds((2 * fi + ci) * SUB + h * (SUB // 2), SUB // 2)]

    wloc = pltpu.make_async_copy(w_h, wall.at[:, pl.ds((2 * f + c) * SUB, SUB)], lsem.at[0])
    ucol = pl.ds(pl.multiple_of(j * lf, 128), lf)
    dcol = pl.ds(pl.multiple_of(j * ld, 128), ld)
    kloc = pltpu.make_async_copy(tok_h, tok, lsem.at[1])
    mloc = pltpu.make_async_copy(d_h, dmine, lsem.at[2])
    uloc = pltpu.make_async_copy(u_h.at[:, ucol], uall.at[j], lsem.at[3])
    dloc = pltpu.make_async_copy(d_h.at[:, dcol], dall.at[j], lsem.at[4])
    cloc = pltpu.make_async_copy(cot_h, cot, lsem.at[5])
    for d in [wloc, kloc, mloc, uloc, dloc, cloc]:
        d.start()

    barrier = pltpu.get_barrier_semaphore()
    for k in range(1, 8):
        pl.semaphore_signal(barrier, 1, device_id={"fsdp": lax.rem(f + k, 8)}, device_id_type=MESH)
        pl.semaphore_signal(
            barrier, 1, device_id={"tenant": lax.rem(j + k, 8)}, device_id_type=MESH
        )
    pl.semaphore_signal(barrier, 1, device_id=partner, device_id_type=MESH)
    pl.semaphore_signal(
        barrier, 1, device_id={"fsdp": fn["Z"], "tenant": tn["Z"]}, device_id_type=MESH
    )
    pl.semaphore_wait(barrier, 16)

    def fs(i):
        return {"fsdp": fn[i]}

    def w_send(q, name, rsem, to, src=None):
        ref = slot(q, fn[name] if name else f, c) if src is None else src
        go(ref, ref, wss, rsem, to)

    def w_got(q, k, ref):
        got(ref, wrs.at[q, k])

    def w_A(q):
        w_send(q, None, wrs.at[q, 1], fs("R"))
        w_send(q, None, wrs.at[q, 2], fs("L"))
        w_send(q, None, wrs.at[q, 0], fs("Z"))
        w_send(q, None, prs.at[q], partner)

    def w_B(q):
        w_got(q, 0, slot(q, fn["Z"], c))
        w_send(q, "Z", wrs.at[q, 3], fs("R"))
        w_send(q, "Z", wrs.at[q, 4], fs("L"))
        w_send(q, "Z", prs.at[q], partner)

    def w_CD(q, left, right, kl, kr, ko):
        w_got(q, kl, slot(q, fn[left], c))
        w_send(q, left, wrs.at[q, ko], fs("R"), part(q, fn[left], c, 0))
        w_send(q, left, prs.at[q], partner)
        w_got(q, kr, slot(q, fn[right], c))
        w_send(q, right, wrs.at[q, ko], fs("L"), part(q, fn[right], c, 1))
        w_send(q, right, prs.at[q], partner)

    def w_C(q):
        w_CD(q, "L", "R", 1, 2, 5)

    def w_D(q):
        w_CD(q, "LZ", "RZ", 3, 4, 6)

    def w_E(q):
        for name, k in (("O", 5), ("OZ", 6)):
            w_got(q, k, slot(q, fn[name], c))
            w_send(q, name, prs.at[q], partner)

    def w_P(q):
        got(wall.at[q, pl.ds(0, 8 * SUB)], prs.at[q])

    def te(i):
        return {"tenant": tn[i]}

    tq = (pl.ds(0, 3), pl.ds(3, 2))

    def t_ref(ji, p, h=None):
        rows_ = slice(None) if h is None else pl.ds(h * half, half)
        return tokq.at[ji, tq[p], rows_]

    def t_send(p, ji, k, to, h=None):
        ref = t_ref(ji, p, h)
        go(ref, ref, tss, trs.at[p, k], to)

    def pieces(v):
        return [
            jnp.concatenate([v[:, SUB * q : SUB * q + SUB], v[:, 320 + SUB * q : 384 + SUB * q]], axis=1)
            for q in range(ROUNDS)
        ]

    def t_make():
        kloc.wait()
        for q, v in enumerate(pieces(tok[...])):
            tokq[j, q] = v

    def dq_make():
        mloc.wait()
        for i in range(8):
            for q, v in enumerate(pieces(dmine[:, ld * i : ld * i + ld])):
                dq[q, :, 128 * i : 128 * i + 128] = v

    def t_A(p):
        t_send(p, j, 1, te("R"))
        t_send(p, j, 2, te("L"))

    def t_Z(p):
        t_send(p, j, 0, te("Z"))

    def t_B(p):
        got(t_ref(tn["Z"], p), trs.at[p, 0])
        t_send(p, tn["Z"], 3, te("R"))
        t_send(p, tn["Z"], 4, te("L"))

    def t_CD(p, left, right, kl, kr):
        got(t_ref(tn[left], p), trs.at[p, kl])
        t_send(p, tn[left], 5, te("R"), 0)
        got(t_ref(tn[right], p), trs.at[p, kr])
        t_send(p, tn[right], 5, te("L"), 1)

    def t_C(p):
        t_CD(p, "L", "R", 1, 2)

    def t_D(p):
        t_CD(p, "LZ", "RZ", 3, 4)

    def t_E():
        for p in range(2):
            got(tokq.at[pl.ds(0, 2), tq[p]], trs.at[p, 5])

    def adapter(src, width, all_, relay, s):
        def own(ji, ci):
            return all_.at[ji, pl.ds(ci * 32, 32)]

        def out(ji):
            return src.at[pl.ds(c * 32, 32), pl.ds(pl.multiple_of(ji * width, 128), width)]

        return own, out, relay, s

    kinds = (adapter(d_h, ld, dall, dx, 0), adapter(u_h, lf, uall, ux, 1))
    cross = {"fsdp": fn["Z"], "tenant": tn["Z"]}

    def at_y(r):
        return lax.rem(y + r, 4)

    def u_cross():
        for own, out, relay, s in kinds:
            for r in (1, 2, 3, 0):
                dst = own(j, c) if r == 0 else relay.at[r]
                go(out(2 * at_y(r) + 1 - zh), dst, uss.at[s], urs.at[s, r], cross)

    def u_own():
        for own, out, relay, s in kinds:
            for r in range(1, 4):
                to = 2 * at_y(r) + zh
                go(out(to), own(j, c), uss.at[s], urs.at[s, 0], {"tenant": to})

    def u_fwd():
        for own, out, relay, s in kinds:
            for r in range(1, 4):
                got(relay.at[r], urs.at[s, r])
                to = 2 * at_y(r) + zh
                go(relay.at[r], own(tn["Z"], c), uss.at[s], urs.at[s, 0], {"tenant": to})

    def u_recv():
        for (own, out, relay, s), all_ in zip(kinds, (dall, uall)):
            got(all_.at[pl.ds(0, 7), pl.ds(0, 32)], urs.at[s, 0])
            for k in range(1, 8):
                ref = own(lax.rem(j + k, 8), c)
                go(ref, ref, upss.at[s], uprs.at[s], partner)

    def u_from_partner():
        for s, all_ in ((0, dall), (1, uall)):
            got(all_.at[pl.ds(0, 7), pl.ds(0, 32)], uprs.at[s])

    def tenant_is(b, t, shape):
        return jnp.full(shape, bti[b], jnp.int32) == t

    def make_gain():
        lane = lax.broadcasted_iota(jnp.int32, (BLOCK, BLOCK), 1)
        gains = []
        for t in range(8):
            r = jnp.full((BLOCK, BLOCK), ranks[t], jnp.int32)
            gains.append(jnp.where(lane < r, ALPHA / r.astype(F32), 0.0))
        for b in range(6):
            g = jnp.zeros((BLOCK, BLOCK), F32)
            for t in range(8):
                g = jnp.where(tenant_is(b, t, g.shape), gains[t], g)
            gcomp[pl.ds(b * BLOCK, BLOCK), :] = g

    def compact(w, a, all_):
        for h in range(2):
            u = all_[pl.ds(4 * h, 4)].reshape(256, a.shape[1])
            p = dot(a[...], u, 1, 1)
            for b in range(6):
                rs = slice(b * BLOCK, (b + 1) * BLOCK)
                acc = jnp.zeros((BLOCK, BLOCK), F32)
                for t in range(4):
                    acc = jnp.where(
                        tenant_is(b, 4 * h + t, acc.shape), p[rs, 64 * t : 64 * t + 64], acc
                    )
                r0, l0 = (b % 3) * BLOCK, 64 * (b // 3)
                at = (w, slice(r0, r0 + BLOCK), slice(l0, l0 + 64))
                cp2[at] = acc if h == 0 else cp2[at] + acc

    def b_desc(k):
        to = lax.rem(j + k, 8)
        return rc(
            cp2.at[:, pl.ds(to * 24, 24)], brecv.at[k], bss, brs, {"tenant": to}
        )

    def b_sum():
        s = cp2[:, pl.ds(pl.multiple_of(j * 24, 8), 24), :]
        got(brecv.at[pl.ds(1, 7)], brs)
        for k in range(1, 8):
            s = s + brecv[k]
        agx[j] = s

    def ag_desc(k):
        return rc(agx.at[j], agx.at[j], ass_, ars, {"tenant": lax.rem(j + k, 8)})

    def ag_use():
        got(agx.at[pl.ds(0, 7)], ars)
        for w, dst in ((0, agexp), (1, aexp)):
            packed = jnp.concatenate([agx[k, w] for k in range(8)], axis=0)
            for b in range(6):
                r0 = (b % 3) * BLOCK
                s = packed[r0 : r0 + BLOCK, 64 * (b // 3) : 64 * (b // 3) + 64]
                v = (s * gcomp[b * BLOCK : (b + 1) * BLOCK, :]).astype(BF).astype(F32)
                zero = jnp.zeros_like(v)
                rs = slice(b * BLOCK, (b + 1) * BLOCK)
                if w == 0:
                    agj[rs, :] = jnp.where(tenant_is(b, j, v.shape), v, zero).astype(BF)
                for t in range(0, 8, 2):
                    pair = jnp.concatenate(
                        [jnp.where(tenant_is(b, t + e, v.shape), v, zero) for e in range(2)], axis=1
                    )
                    dst[rs, 64 * t : 64 * t + 128] = pair.astype(BF)

    def lhs(q):
        return jnp.concatenate([tokq[i, q] for i in range(8)], axis=1)

    def grad_down_part():
        p = dot(agexp[...], tok[...], 0, 0)
        gpart[0, :, 0:ld] = p[:256]
        gpart[1, :, 0:ld] = p[256:]

    def grad_up_part(lo, hi):
        def body(n):
            at = pl.ds(pl.multiple_of(n * 256, 256), 256)
            to = pl.ds(pl.multiple_of(ld + n * 256, 128), 256)
            p = dot(aexp[...], cot[:, at], 0, 0)
            gpart[0, :, to] = p[:256]
            gpart[1, :, to] = p[256:]

        each(lo, hi, body)

    fx, fz = f // 2, lax.rem(f, 2)
    cols = (pl.ds(0, 1152), pl.ds(1152, 1280))

    def gx(p):
        go(gpart.at[1 - c, :, cols[p]], gpr.at[:, cols[p]], xss, xrs.at[p], partner)

    def chunk(k, p):
        at = pl.ds(pl.multiple_of(k * 32, 32), 32)
        return gpart[c, at, cols[p]] + gpr[at, cols[p]]

    def rs_z(p):
        got(gpr.at[:, cols[p]], xrs.at[p])

        def body(k):
            rss[k, :, cols[p]] = chunk(2 * k + 1 - fz, p).astype(BF)

        each(0, 4, body)
        at = (pl.ds(0, 4), slice(None), cols[p])
        go(rss.at[at], rsr.at[at], rss_s, rss_r.at[p, 0], fs("Z"))

    def fx_to(r):
        return {"fsdp": lax.rem(f + 2 * r, 8)}

    def rs_x(p):
        got(rsr.at[pl.ds(0, 4), :, cols[p]], rss_r.at[p, 0])
        for r in range(1, 4):
            k = lax.rem(fx + r, 4)
            rss[3 + r, :, cols[p]] = (
                chunk(2 * k + fz, p) + rsr[k, :, cols[p]].astype(F32)
            ).astype(BF)
            at = (3 + r, slice(None), cols[p])
            go(rss.at[at], rsr.at[at], rss_s, rss_r.at[p, 1], fx_to(r))

    def rs_sum(p):
        s = chunk(f, p) + rsr[fx, :, cols[p]].astype(F32)
        got(rsr.at[pl.ds(4, 3), :, cols[p]], rss_r.at[p, 1])
        for r in range(1, 4):
            s = s + rsr[3 + r, :, cols[p]].astype(F32)
        agg[f, :, cols[p]] = s.astype(BF)
        ref = agg.at[f, :, cols[p]]
        for r in range(1, 4):
            go(ref, ref, ags_s, ags_r.at[p, 0], fx_to(r))
        go(ref, ref, ags_s, ags_r.at[p, 1], fs("Z"))

    def ag_z(p):
        got(agg.at[pl.ds(0, 3), :, cols[p]], ags_r.at[p, 0])
        for r in range(1, 4):
            ref = agg.at[lax.rem(f + 8 - 2 * r, 8), :, cols[p]]
            go(ref, ref, ags_s, ags_r.at[p, 1], fs("Z"))

    def grads_out(p):
        got(agg.at[pl.ds(0, 4), :, cols[p]], ags_r.at[p, 1])

        def body(k):
            at = pl.ds(pl.multiple_of(k * 32, 32), 32)
            v = agg[k, :, cols[p]].astype(F32)
            if p == 0:
                gd_out[at, :] = v[:, :ld]
                gu_out[at, 0:512] = v[:, ld:]
            else:
                gu_out[at, 512:] = v

        each(0, 8, body)

    def g_desc(q, i):
        rel = lax.rem(y - i + 4, 4) - 1
        return rc(
            gsend.at[q, i], grecv.at[q, rel], gss, grs.at[q], {"tenant": 2 * i + zh}
        )

    def compute_g(q):
        def body(k):
            i = lax.rem(y + k, 4)
            at = pl.ds(pl.multiple_of(i * 256, 256), 256)
            p = dot(cot[...], wall[q, at, :], 1, 1) + dot(agj[...], dq[q, :, at], 1, 0)

            @pl.when(k < 4)
            def _():
                gsend[q, i] = p.astype(BF)
                g_desc(q, i).start()

            @pl.when(k == 4)
            def _():
                gown[q] = p

        each(1, 5, body)

    def compute_h(q):
        def body(n):
            at = pl.ds(pl.multiple_of(n * 256, 256), 256)
            p = dot(lhs(q), wall[q, :, at], 1, 0)
            if q == 0:
                hacc[:, at] = p
            elif q < ROUNDS - 1:
                hacc[:, at] += p
            else:
                u = uall[:, :, at].reshape(512, 256)
                hid_out[:, at] = (hacc[:, at] + p + dot(aexp[...], u, 1, 0)).astype(BF)

        each(0, lf // 256, body)

    def g_sum(q):
        got(grecv.at[q], grs.at[q])
        mine = pl.ds(pl.multiple_of(zh * 128, 128), 128)
        other = pl.ds(pl.multiple_of(128 - zh * 128, 128), 128)

        def total(at):
            s = gown[q, :, at]
            for k in range(3):
                s = s + grecv[q, k, :, at].astype(F32)
            return s

        gzs[q] = total(other).astype(BF)
        go(gzs.at[q], gzr.at[q], zss, zrs, te("Z"))
        gown[q, :, mine] = total(mine)

    def gt_final():
        mine = pl.ds(pl.multiple_of(zh * 128, 128), 128)
        got(gzr, zrs)

        def body(b):
            at = pl.ds(pl.multiple_of(b * BLOCK, BLOCK), BLOCK)
            s = [gown[q, at, mine] + gzr[q, at, :].astype(F32) for q in range(ROUNDS)]
            row = jnp.concatenate([v[:, :64] for v in s] + [v[:, 64:] for v in s], axis=1)
            gt_out[at, :] = row.astype(BF)

        each(0, 6, body)

    wloc.wait()
    w_A(0)
    u_cross()
    u_own()
    w_A(1)
    t_make()
    t_A(0)
    make_gain()
    dq_make()
    w_B(0)
    w_C(0)
    w_A(2)
    u_fwd()
    t_A(1)
    t_Z(0)
    t_Z(1)
    t_C(0)
    w_D(0)
    w_B(1)
    w_C(1)
    w_A(3)
    u_recv()
    t_B(0)
    uloc.wait()
    dloc.wait()
    cloc.wait()
    u_from_partner()
    compact(0, cot, uall)
    compact(1, tok, dall)
    each(1, 8, lambda k: b_desc(k).start())
    t_C(1)
    w_E(0)
    w_B(2)
    w_C(2)
    w_D(1)
    b_sum()
    each(1, 8, lambda k: ag_desc(k).start())
    t_B(1)
    w_A(4)
    t_D(0)
    ag_use()
    w_P(0)
    compute_g(0)
    t_D(1)
    w_E(1)
    w_P(1)
    compute_g(1)
    w_D(2)
    w_B(3)
    w_C(3)
    grad_down_part()
    grad_up_part(0, 2)
    gx(0)
    grad_up_part(2, 7)
    gx(1)
    w_E(2)
    w_P(2)
    compute_g(2)
    rs_z(0)
    rs_z(1)
    g_sum(0)
    w_D(3)
    w_B(4)
    w_C(4)
    t_E()
    compute_h(0)
    w_E(3)
    w_P(3)
    compute_g(3)
    w_D(4)
    rs_x(0)
    rs_x(1)
    g_sum(1)
    compute_h(1)
    w_E(4)
    w_P(4)
    compute_g(4)
    rs_sum(0)
    rs_sum(1)
    g_sum(2)
    compute_h(2)
    ag_z(0)
    ag_z(1)
    compute_h(3)
    g_sum(3)
    compute_h(4)
    grads_out(0)
    grads_out(1)
    g_sum(4)
    gt_final()

    gone(wall.at[:, pl.ds(0, 15 * SUB)], wss)
    gone(tokq.at[pl.ds(0, 7)], tss)
    for s, all_ in ((0, dall), (1, uall)):
        gone(all_.at[pl.ds(0, 5)], uss.at[s])
        gone(all_.at[pl.ds(0, 7), pl.ds(0, 32)], upss.at[s])
    gone(brecv.at[pl.ds(0, 7)], bss)
    gone(agx.at[pl.ds(0, 7)], ass_)
    gone(gsend.at[:, pl.ds(0, 3)], gss)
    gone(gzs, zss)
    gone(gpr, xss)
    gone(rss.at[pl.ds(0, 7)], rss_s)
    gone(agg.at[pl.ds(0, 7)], ags_s)


def shards(tokens, bti, ranks, w, down, up, cot):
    rows, ld = tokens.shape
    lf = cot.shape[1]
    up = up.reshape(up.shape[1:])
    w = w.reshape(ROUNDS, SUB, lf)
    down = down.reshape(down.shape[1:])
    dma = pltpu.SemaphoreType.DMA
    vm = pltpu.VMEM
    smem = pl.BlockSpec(memory_space=pltpu.SMEM)
    hbm = pl.BlockSpec(memory_space=pl.ANY)
    out = pl.BlockSpec(memory_space=pltpu.VMEM)
    half = rows // 2
    hid, gt, gd, gu = pl.pallas_call(
        kernel,
        out_shape=(
            pltpu.VMEM((rows, lf), BF),
            pltpu.VMEM((rows, ld), BF),
            pltpu.VMEM((256, ld), F32),
            pltpu.VMEM((256, lf), F32),
        ),
        in_specs=[smem, smem, hbm, hbm, hbm, hbm, hbm],
        out_specs=(out, out, out, out),
        scratch_shapes=[
            vm((rows, ld), BF),
            vm((ROUNDS, 64, 1024), BF),
            vm((rows, lf), BF),
            vm((ROUNDS, 1024, lf), BF),
            vm((8, ROUNDS, rows, 128), BF),
            vm((64, 5120), BF),
            vm((8, 64, lf), BF),
            vm((8, 64, ld), BF),
            vm((4, 32, lf), BF),
            vm((4, 32, ld), BF),
            vm((rows, lf), F32),
            vm((ROUNDS, 4, rows, 256), BF),
            vm((ROUNDS, rows, 256), F32),
            vm((ROUNDS, 3, rows, 256), BF),
            vm((ROUNDS, rows, 128), BF),
            vm((ROUNDS, rows, 128), BF),
            vm((rows, 64), F32),
            vm((2, half, 128), F32),
            vm((8, 2, 24, 128), F32),
            vm((8, 2, 24, 128), F32),
            vm((rows, 64), BF),
            vm((rows, 512), BF),
            vm((rows, 512), BF),
            vm((2, 256, ld + lf), F32),
            vm((256, ld + lf), F32),
            vm((8, 32, ld + lf), BF),
            vm((8, 32, ld + lf), BF),
            vm((8, 32, ld + lf), BF),
            dma((6,)),
            dma,
            dma((ROUNDS, 7)),
            dma((ROUNDS,)),
            dma,
            dma((2, 6)),
            dma((2,)),
            dma((2, 4)),
            dma((2,)),
            dma((2,)),
            dma,
            dma,
            dma,
            dma,
            dma,
            dma((ROUNDS,)),
            dma,
            dma,
            dma,
            dma((2,)),
            dma,
            dma((2, 2)),
            dma,
            dma((2, 2)),
        ],
        compiler_params=pltpu.CompilerParams(
            collective_id=0, has_side_effects=True, vmem_limit_bytes=58 << 20
        ),
    )(bti, ranks, tokens, w, down, up, cot)
    return hid, gt, gd.reshape(4, 64, ld), gu.reshape(4, 64, lf)


def solution(mesh):
    return jax.shard_map(
        shards,
        mesh=mesh,
        in_specs=(
            P(("fsdp", "dp"), "tenant"),
            P(("fsdp", "dp")),
            P(),
            P(("fsdp", "dp"), "tenant"),
            P("tenant", None, None),
            P("tenant", None, None),
            P(("fsdp", "dp"), "tenant"),
        ),
        out_specs=(
            P(("fsdp", "dp"), "tenant"),
            P(("fsdp", "dp"), "tenant"),
            P("dp", None, "tenant"),
            P("dp", None, "tenant"),
        ),
        check_vma=False,
    )
```

```python
import jax
import jax.numpy as jnp
from jax import lax
from jax.experimental import pallas as pl
from jax.experimental.pallas import tpu as pltpu
from jax.sharding import PartitionSpec as P

MESH = pl.DeviceIdType.MESH
BF = jnp.bfloat16
F32 = jnp.float32
BLOCK = 64
ALPHA = 32.0
ROUNDS = 5
SUB = 64


def dot(a, b, ca, cb):
    return lax.dot_general(a, b, (((ca,), (cb,)), ((), ())), preferred_element_type=F32)


def kernel(
    bti,
    ranks,
    tok_h,
    w_h,
    d_h,
    u_h,
    cot_h,
    hid_out,
    gt_out,
    gd_out,
    gu_out,
    tok,
    dq,
    cot,
    wall,
    tokq,
    dmine,
    uall,
    dall,
    ux,
    dx,
    hacc,
    gopp,
    gn,
    gf,
    gor,
    gown,
    grecv,
    gzs,
    gzr,
    gcomp,
    cp2,
    brecv,
    agx,
    agj,
    agexp,
    aexp,
    gpart,
    gpr,
    rss,
    rsr,
    agg,
    lsem,
    wss,
    wrs,
    prs,
    tss,
    trs,
    uss,
    urs,
    upss,
    uprs,
    bss,
    brs,
    ass_,
    ars,
    gos,
    gors,
    gns,
    grs,
    zss,
    zrs,
    xss,
    xrs,
    rss_s,
    rss_r,
    ags_s,
    ags_r,
):
    f = lax.axis_index("fsdp")
    j = lax.axis_index("tenant")
    c = lax.axis_index("dp")
    rows = cot.shape[0]
    half = rows // 2
    lf, ld = cot.shape[1], tok.shape[1]

    def ring(i):
        flip = 1 - 2 * lax.rem(i, 2)
        right, left, opp = lax.rem(i + 2, 8), lax.rem(i + 6, 8), lax.rem(i + 4, 8)
        return dict(
            Z=i + flip,
            R=right,
            L=left,
            O=opp,
            RZ=right + flip,
            LZ=left + flip,
            OZ=opp + flip,
        )

    fn, tn = ring(f), ring(j)
    y, zh = j // 2, lax.rem(j, 2)
    partner = {"dp": 1 - c}

    def rc(src, dst, ss, rs, dev):
        return pltpu.make_async_remote_copy(
            src_ref=src, dst_ref=dst, send_sem=ss, recv_sem=rs, device_id=dev, device_id_type=MESH
        )

    def each(lo, hi, body):
        def step(k, carry):
            body(k)
            return carry

        lax.fori_loop(lo, hi, step, 0)

    def go(src, dst, ss, rs, dev):
        rc(src, dst, ss, rs, dev).start()

    def gone(ref, ss):
        rc(ref, ref, ss, ss, partner).wait_send()

    def got(dst, rs):
        rc(dst, dst, rs, rs, partner).wait_recv()

    def slot(q, fi, ci):
        return wall.at[q, pl.ds((2 * fi + ci) * SUB, SUB)]

    def part(q, fi, ci, h):
        return wall.at[q, pl.ds((2 * fi + ci) * SUB + h * (SUB // 2), SUB // 2)]

    wloc = pltpu.make_async_copy(w_h, wall.at[:, pl.ds((2 * f + c) * SUB, SUB)], lsem.at[0])
    ucol = pl.ds(pl.multiple_of(j * lf, 128), lf)
    dcol = pl.ds(pl.multiple_of(j * ld, 128), ld)
    kloc = pltpu.make_async_copy(tok_h, tok, lsem.at[1])
    mloc = pltpu.make_async_copy(d_h, dmine, lsem.at[2])
    uloc = pltpu.make_async_copy(u_h.at[:, ucol], uall.at[j], lsem.at[3])
    dloc = pltpu.make_async_copy(d_h.at[:, dcol], dall.at[j], lsem.at[4])
    cloc = pltpu.make_async_copy(cot_h, cot, lsem.at[5])
    for d in [wloc, kloc, mloc, uloc, dloc, cloc]:
        d.start()

    barrier = pltpu.get_barrier_semaphore()
    for k in range(1, 8):
        pl.semaphore_signal(barrier, 1, device_id={"fsdp": lax.rem(f + k, 8)}, device_id_type=MESH)
        pl.semaphore_signal(
            barrier, 1, device_id={"tenant": lax.rem(j + k, 8)}, device_id_type=MESH
        )
    pl.semaphore_signal(barrier, 1, device_id=partner, device_id_type=MESH)
    pl.semaphore_signal(
        barrier, 1, device_id={"fsdp": fn["Z"], "tenant": tn["Z"]}, device_id_type=MESH
    )

    def fs(i):
        return {"fsdp": fn[i]}

    def w_send(q, name, rsem, to, src=None):
        ref = slot(q, fn[name] if name else f, c) if src is None else src
        go(ref, ref, wss, rsem, to)

    def w_got(q, k, ref):
        got(ref, wrs.at[q, k])

    def w_A(q):
        w_send(q, None, wrs.at[q, 1], fs("R"))
        w_send(q, None, wrs.at[q, 2], fs("L"))
        w_send(q, None, wrs.at[q, 0], fs("Z"))
        w_send(q, None, prs.at[q], partner)

    def w_B(q):
        w_got(q, 0, slot(q, fn["Z"], c))
        w_send(q, "Z", wrs.at[q, 3], fs("R"))
        w_send(q, "Z", wrs.at[q, 4], fs("L"))
        w_send(q, "Z", prs.at[q], partner)

    def w_CD(q, left, right, kl, kr, ko):
        w_got(q, kl, slot(q, fn[left], c))
        w_send(q, left, wrs.at[q, ko], fs("R"), part(q, fn[left], c, 0))
        w_send(q, left, prs.at[q], partner)
        w_got(q, kr, slot(q, fn[right], c))
        w_send(q, right, wrs.at[q, ko], fs("L"), part(q, fn[right], c, 1))
        w_send(q, right, prs.at[q], partner)

    def w_C(q):
        w_CD(q, "L", "R", 1, 2, 5)

    def w_D(q):
        w_CD(q, "LZ", "RZ", 3, 4, 6)

    def w_E(q):
        for name, k in (("O", 5), ("OZ", 6)):
            w_got(q, k, slot(q, fn[name], c))
            w_send(q, name, prs.at[q], partner)

    def x_C(q):
        for name, k, h, kz, to in (("L", 1, 0, 3, "R"), ("R", 2, 1, 4, "L")):
            w_got(q, k, slot(q, fn[name], c))
            w_send(q, name, wrs.at[q, 5], fs(to), part(q, fn[name], c, h))
            w_send(q, name, wrs.at[q, kz], fs("Z"))
            w_send(q, name, prs.at[q], partner)

    def x_D(q):
        for name, k in (("Z", 0), ("LZ", 3), ("RZ", 4)):
            w_got(q, k, slot(q, fn[name], c))
            w_send(q, name, prs.at[q], partner)

    def x_O(q):
        w_got(q, 5, slot(q, fn["O"], c))
        w_send(q, "O", wrs.at[q, 6], fs("Z"))
        w_send(q, "O", prs.at[q], partner)

    def x_E(q):
        w_got(q, 6, slot(q, fn["OZ"], c))
        w_send(q, "OZ", prs.at[q], partner)

    def w_P(q):
        got(wall.at[q, pl.ds(0, 8 * SUB)], prs.at[q])

    def te(i):
        return {"tenant": tn[i]}

    tq = (pl.ds(0, 3), pl.ds(3, 2))

    def t_ref(ji, p, h=None):
        rows_ = slice(None) if h is None else pl.ds(h * half, half)
        return tokq.at[ji, tq[p], rows_]

    def t_send(p, ji, k, to, h=None):
        ref = t_ref(ji, p, h)
        go(ref, ref, tss, trs.at[p, k], to)

    def pieces(v):
        return [
            jnp.concatenate([v[:, SUB * q : SUB * q + SUB], v[:, 320 + SUB * q : 384 + SUB * q]], axis=1)
            for q in range(ROUNDS)
        ]

    def t_make():
        kloc.wait()
        for q, v in enumerate(pieces(tok[...])):
            tokq[j, q] = v

    def dq_make():
        mloc.wait()
        for i in range(8):
            for q, v in enumerate(pieces(dmine[:, ld * i : ld * i + ld])):
                dq[q, :, 128 * i : 128 * i + 128] = v

    def t_A(p):
        t_send(p, j, 1, te("R"))
        t_send(p, j, 2, te("L"))

    def t_Z(p):
        t_send(p, j, 0, te("Z"))

    def t_B(p):
        got(t_ref(tn["Z"], p), trs.at[p, 0])
        t_send(p, tn["Z"], 3, te("R"))
        t_send(p, tn["Z"], 4, te("L"))

    def t_CD(p, left, right, kl, kr):
        got(t_ref(tn[left], p), trs.at[p, kl])
        t_send(p, tn[left], 5, te("R"), 0)
        got(t_ref(tn[right], p), trs.at[p, kr])
        t_send(p, tn[right], 5, te("L"), 1)

    def t_C(p):
        t_CD(p, "L", "R", 1, 2)

    def t_D(p):
        t_CD(p, "LZ", "RZ", 3, 4)

    def t_E():
        for p in range(2):
            got(tokq.at[pl.ds(0, 2), tq[p]], trs.at[p, 5])

    def adapter(src, width, all_, relay, s):
        def own(ji, ci):
            return all_.at[ji, pl.ds(ci * 32, 32)]

        def out(ji):
            return src.at[pl.ds(c * 32, 32), pl.ds(pl.multiple_of(ji * width, 128), width)]

        return own, out, relay, s

    kinds = (adapter(d_h, ld, dall, dx, 0), adapter(u_h, lf, uall, ux, 1))
    cross = {"fsdp": fn["Z"], "tenant": tn["Z"]}

    def at_y(r):
        return lax.rem(y + r, 4)

    def u_cross():
        for own, out, relay, s in kinds:
            for r in (1, 2, 3, 0):
                dst = own(j, c) if r == 0 else relay.at[r]
                go(out(2 * at_y(r) + 1 - zh), dst, uss.at[s], urs.at[s, r], cross)

    def u_own():
        for own, out, relay, s in kinds:
            for r in range(1, 4):
                to = 2 * at_y(r) + zh
                go(out(to), own(j, c), uss.at[s], urs.at[s, 0], {"tenant": to})

    def u_fwd():
        for own, out, relay, s in kinds:
            for r in range(1, 4):
                got(relay.at[r], urs.at[s, r])
                to = 2 * at_y(r) + zh
                go(relay.at[r], own(tn["Z"], c), uss.at[s], urs.at[s, 4], {"tenant": to})

    def u_recv(e):
        for (own, out, relay, s), all_ in zip(kinds, (dall, uall)):
            got(all_.at[pl.ds(0, 4 - e), pl.ds(0, 32)], urs.at[s, 4 * e])
            for r in range(e, 4):
                ji = 2 * at_y(4 - r) + (1 - zh if e == 1 or r == 0 else zh)
                go(own(ji, c), own(ji, c), upss.at[s], uprs.at[s], partner)

    def u_from_partner():
        for s, all_ in ((0, dall), (1, uall)):
            got(all_.at[pl.ds(0, 7), pl.ds(0, 32)], uprs.at[s])

    def tenant_is(b, t, shape):
        return jnp.full(shape, bti[b], jnp.int32) == t

    def make_gain():
        lane = lax.broadcasted_iota(jnp.int32, (BLOCK, BLOCK), 1)
        gains = []
        for t in range(8):
            r = jnp.full((BLOCK, BLOCK), ranks[t], jnp.int32)
            gains.append(jnp.where(lane < r, ALPHA / r.astype(F32), 0.0))
        for b in range(6):
            g = jnp.zeros((BLOCK, BLOCK), F32)
            for t in range(8):
                g = jnp.where(tenant_is(b, t, g.shape), gains[t], g)
            gcomp[pl.ds(b * BLOCK, BLOCK), :] = g

    def compact(w, a, all_):
        for h in range(2):
            u = all_[pl.ds(4 * h, 4)].reshape(256, a.shape[1])
            p = dot(a[...], u, 1, 1)
            for b in range(6):
                rs = slice(b * BLOCK, (b + 1) * BLOCK)
                acc = jnp.zeros((BLOCK, BLOCK), F32)
                for t in range(4):
                    acc = jnp.where(
                        tenant_is(b, 4 * h + t, acc.shape), p[rs, 64 * t : 64 * t + 64], acc
                    )
                r0, l0 = (b % 3) * BLOCK, 64 * (b // 3)
                at = (w, slice(r0, r0 + BLOCK), slice(l0, l0 + 64))
                cp2[at] = acc if h == 0 else cp2[at] + acc

    def b_desc(k):
        to = lax.rem(j + k, 8)
        return rc(
            cp2.at[:, pl.ds(to * 24, 24)], brecv.at[k], bss, brs, {"tenant": to}
        )

    def b_sum():
        s = cp2[:, pl.ds(pl.multiple_of(j * 24, 8), 24), :]
        got(brecv.at[pl.ds(1, 7)], brs)
        for k in range(1, 8):
            s = s + brecv[k]
        agx[j] = s

    def ag_desc(k):
        return rc(agx.at[j], agx.at[j], ass_, ars, {"tenant": lax.rem(j + k, 8)})

    def ag_use():
        got(agx.at[pl.ds(0, 7)], ars)
        for w, dst in ((0, agexp), (1, aexp)):
            packed = jnp.concatenate([agx[k, w] for k in range(8)], axis=0)
            for b in range(6):
                r0 = (b % 3) * BLOCK
                s = packed[r0 : r0 + BLOCK, 64 * (b // 3) : 64 * (b // 3) + 64]
                v = (s * gcomp[b * BLOCK : (b + 1) * BLOCK, :]).astype(BF).astype(F32)
                zero = jnp.zeros_like(v)
                rs = slice(b * BLOCK, (b + 1) * BLOCK)
                if w == 0:
                    agj[rs, :] = jnp.where(tenant_is(b, j, v.shape), v, zero).astype(BF)
                for t in range(0, 8, 2):
                    pair = jnp.concatenate(
                        [jnp.where(tenant_is(b, t + e, v.shape), v, zero) for e in range(2)], axis=1
                    )
                    dst[rs, 64 * t : 64 * t + 128] = pair.astype(BF)

    def lhs(q):
        return jnp.concatenate([tokq[i, q] for i in range(8)], axis=1)

    def grad_down_part():
        p = dot(agexp[...], tok[...], 0, 0)
        gpart[0, :, 0:ld] = p[:256]
        gpart[1, :, 0:ld] = p[256:]

    def grad_up_part(lo, hi):
        def body(n):
            at = pl.ds(pl.multiple_of(n * 256, 256), 256)
            to = pl.ds(pl.multiple_of(ld + n * 256, 128), 256)
            p = dot(aexp[...], cot[:, at], 0, 0)
            gpart[0, :, to] = p[:256]
            gpart[1, :, to] = p[256:]

        each(lo, hi, body)

    fx, fz = f // 2, lax.rem(f, 2)
    cols = (pl.ds(0, 896), pl.ds(896, 1536))

    def gx(p):
        go(gpart.at[1 - c, :, cols[p]], gpr.at[:, cols[p]], xss, xrs.at[p], partner)

    def chunk(k, p):
        at = pl.ds(pl.multiple_of(k * 32, 32), 32)
        return gpart[c, at, cols[p]] + gpr[at, cols[p]]

    def rs_z(p):
        got(gpr.at[:, cols[p]], xrs.at[p])

        def body(k):
            rss[k, :, cols[p]] = chunk(2 * k + 1 - fz, p).astype(BF)

        each(0, 4, body)
        at = (pl.ds(0, 4), slice(None), cols[p])
        go(rss.at[at], rsr.at[at], rss_s, rss_r.at[p, 0], fs("Z"))

    def fx_to(r):
        return {"fsdp": lax.rem(f + 2 * r, 8)}

    def rs_x(p):
        got(rsr.at[pl.ds(0, 4), :, cols[p]], rss_r.at[p, 0])
        for r in range(1, 4):
            k = lax.rem(fx + r, 4)
            rss[3 + r, :, cols[p]] = (
                chunk(2 * k + fz, p) + rsr[k, :, cols[p]].astype(F32)
            ).astype(BF)
            at = (3 + r, slice(None), cols[p])
            go(rss.at[at], rsr.at[at], rss_s, rss_r.at[p, 1], fx_to(r))

    def to_x(ref, sem):
        for r in range(1, 4):
            go(ref, ref, ags_s, sem, fx_to(r))

    def rs_sum(p):
        s = chunk(f, p) + rsr[fx, :, cols[p]].astype(F32)
        got(rsr.at[pl.ds(4, 3), :, cols[p]], rss_r.at[p, 1])
        for r in range(1, 4):
            s = s + rsr[3 + r, :, cols[p]].astype(F32)
        agg[f, :, cols[p]] = s.astype(BF)
        ref = agg.at[f, :, cols[p]]
        go(ref, ref, ags_s, ags_r.at[p, 1], fs("Z"))
        to_x(ref, ags_r.at[p, 0])

    def ag_z():
        got(agg.at[pl.ds(0, 3), :, cols[0]], ags_r.at[0, 0])
        for r in range(1, 4):
            ref = agg.at[lax.rem(f + 8 - 2 * r, 8), :, cols[0]]
            go(ref, ref, ags_s, ags_r.at[0, 1], fs("Z"))

    def ag_x():
        ref = agg.at[fn["Z"], :, cols[1]]
        got(ref, ags_r.at[1, 1])
        to_x(ref, ags_r.at[1, 0])

    def grads_out(p):
        if p == 0:
            got(agg.at[pl.ds(0, 4), :, cols[p]], ags_r.at[p, 1])
        else:
            got(agg.at[pl.ds(0, 6), :, cols[p]], ags_r.at[p, 0])

        def body(k):
            at = pl.ds(pl.multiple_of(k * 32, 32), 32)
            v = agg[k, :, cols[p]].astype(F32)
            if p == 0:
                gd_out[at, :] = v[:, :ld]
                gu_out[at, 0:256] = v[:, ld:]
            else:
                gu_out[at, 256:] = v

        each(0, 8, body)

    top, bottom = pl.ds(0, half), pl.ds(half, half)

    def g_near(q, e, at):
        go(gn.at[q, e, at], grecv.at[q, e, at], gns, grs.at[q], te("RL"[e]))

    def compute_g(q):
        def body(k):
            i = lax.rem(y + 2 + 3 * k, 4)
            at = pl.ds(pl.multiple_of(i * 256, 256), 256)
            p = dot(cot[...], wall[q, at, :], 1, 1) + dot(agj[...], dq[q, :, at], 1, 0)

            @pl.when(k == 0)
            def _():
                gopp[q] = p.astype(BF)
                go(gopp.at[q, top], gor.at[q, 0], gos, gors.at[q], te("R"))
                go(gopp.at[q, bottom], gor.at[q, 1], gos, gors.at[q], te("L"))

            @pl.when(k == 1)
            def _():
                gf[q, 0] = p[:half]
                gn[q, 0, half:] = p[half:].astype(BF)
                g_near(q, 0, bottom)

            @pl.when(k == 2)
            def _():
                gown[q] = p

            @pl.when(k == 3)
            def _():
                gf[q, 1] = p[half:]
                gn[q, 1, :half] = p[:half].astype(BF)
                g_near(q, 1, top)

        each(0, 4, body)

    def g_acc(q):
        got(gor.at[q], gors.at[q])
        for e, at in enumerate((top, bottom)):
            gn[q, e, at] = (gf[q, e] + gor[q, e].astype(F32)).astype(BF)
            g_near(q, e, at)

    def compute_h(q):
        def body(n):
            at = pl.ds(pl.multiple_of(n * 256, 256), 256)
            p = dot(lhs(q), wall[q, :, at], 1, 0)
            if q == 0:
                hacc[:, at] = p
            elif q < ROUNDS - 1:
                hacc[:, at] += p
            else:
                u = uall[:, :, at].reshape(512, 256)
                hid_out[:, at] = (hacc[:, at] + p + dot(aexp[...], u, 1, 0)).astype(BF)

        each(0, lf // 256, body)

    def g_sum(q):
        got(grecv.at[q], grs.at[q])
        mine = pl.ds(pl.multiple_of(zh * 128, 128), 128)
        other = pl.ds(pl.multiple_of(128 - zh * 128, 128), 128)

        def total(at):
            s = gown[q, :, at]
            for k in range(2):
                s = s + grecv[q, k, :, at].astype(F32)
            return s

        gzs[q] = total(other).astype(BF)
        go(gzs.at[q], gzr.at[q], zss, zrs, te("Z"))
        gown[q, :, mine] = total(mine)

    def gt_final():
        mine = pl.ds(pl.multiple_of(zh * 128, 128), 128)
        got(gzr, zrs)

        def body(b):
            at = pl.ds(pl.multiple_of(b * BLOCK, BLOCK), BLOCK)
            s = [gown[q, at, mine] + gzr[q, at, :].astype(F32) for q in range(ROUNDS)]
            row = jnp.concatenate([v[:, :64] for v in s] + [v[:, 64:] for v in s], axis=1)
            gt_out[at, :] = row.astype(BF)

        each(0, 6, body)

    t_make()
    dq_make()
    make_gain()
    wloc.wait()
    pl.semaphore_wait(barrier, 16)
    w_A(0)
    u_cross()
    u_own()
    w_A(1)
    t_A(0)
    w_B(0)
    w_C(0)
    w_A(2)
    u_fwd()
    t_A(1)
    t_Z(0)
    t_Z(1)
    t_C(0)
    u_recv(0)
    w_D(0)
    w_B(1)
    w_C(1)
    w_A(3)
    u_recv(1)
    uloc.wait()
    dloc.wait()
    cloc.wait()
    u_from_partner()
    compact(0, cot, uall)
    compact(1, tok, dall)
    each(1, 8, lambda k: b_desc(k).start())
    t_C(1)
    w_E(0)
    b_sum()
    each(1, 8, lambda k: ag_desc(k).start())
    t_B(0)
    t_B(1)
    w_A(4)
    w_D(1)
    x_C(2)
    ag_use()
    w_P(0)
    compute_g(0)
    w_B(3)
    w_C(3)
    grad_down_part()
    grad_up_part(0, 1)
    gx(0)
    grad_up_part(1, 7)
    gx(1)
    w_E(1)
    t_D(0)
    w_B(4)
    x_O(2)
    rs_z(0)
    t_D(1)
    w_P(1)
    compute_g(1)
    g_acc(0)
    x_D(2)
    w_D(3)
    w_C(4)
    rs_z(1)
    t_E()
    compute_h(0)
    x_E(2)
    w_D(4)
    w_P(2)
    compute_g(2)
    g_acc(1)
    compute_h(1)
    w_E(3)
    w_P(3)
    compute_g(3)
    rs_x(0)
    rs_x(1)
    g_sum(0)
    g_acc(2)
    w_E(4)
    w_P(4)
    compute_g(4)
    g_sum(1)
    compute_h(2)
    g_acc(3)
    rs_sum(0)
    rs_sum(1)
    g_acc(4)
    g_sum(2)
    compute_h(3)
    ag_x()
    g_sum(3)
    g_sum(4)
    ag_z()
    compute_h(4)
    grads_out(1)
    grads_out(0)
    gt_final()

    gone(wall.at[:, pl.ds(0, 15 * SUB)], wss)
    gone(tokq.at[pl.ds(0, 7)], tss)
    for s, all_ in ((0, dall), (1, uall)):
        gone(all_.at[pl.ds(0, 5)], uss.at[s])
        gone(all_.at[pl.ds(0, 7), pl.ds(0, 32)], upss.at[s])
    gone(brecv.at[pl.ds(0, 7)], bss)
    gone(agx.at[pl.ds(0, 7)], ass_)
    gone(gopp, gos)
    gone(gn, gns)
    gone(gzs, zss)
    gone(gpr, xss)
    gone(rss.at[pl.ds(0, 7)], rss_s)
    gone(agg.at[pl.ds(0, 7)], ags_s)


def shards(tokens, bti, ranks, w, down, up, cot):
    rows, ld = tokens.shape
    lf = cot.shape[1]
    up = up.reshape(up.shape[1:])
    w = w.reshape(ROUNDS, SUB, lf)
    down = down.reshape(down.shape[1:])
    dma = pltpu.SemaphoreType.DMA
    vm = pltpu.VMEM
    smem = pl.BlockSpec(memory_space=pltpu.SMEM)
    hbm = pl.BlockSpec(memory_space=pl.ANY)
    out = pl.BlockSpec(memory_space=pltpu.VMEM)
    half = rows // 2
    hid, gt, gd, gu = pl.pallas_call(
        kernel,
        out_shape=(
            pltpu.VMEM((rows, lf), BF),
            pltpu.VMEM((rows, ld), BF),
            pltpu.VMEM((256, ld), F32),
            pltpu.VMEM((256, lf), F32),
        ),
        in_specs=[smem, smem, hbm, hbm, hbm, hbm, hbm],
        out_specs=(out, out, out, out),
        scratch_shapes=[
            vm((rows, ld), BF),
            vm((ROUNDS, 64, 1024), BF),
            vm((rows, lf), BF),
            vm((ROUNDS, 1024, lf), BF),
            vm((8, ROUNDS, rows, 128), BF),
            vm((64, 5120), BF),
            vm((8, 64, lf), BF),
            vm((8, 64, ld), BF),
            vm((4, 32, lf), BF),
            vm((4, 32, ld), BF),
            vm((rows, lf), F32),
            vm((ROUNDS, rows, 256), BF),
            vm((ROUNDS, 2, rows, 256), BF),
            vm((ROUNDS, 2, half, 256), F32),
            vm((ROUNDS, 2, half, 256), BF),
            vm((ROUNDS, rows, 256), F32),
            vm((ROUNDS, 2, rows, 256), BF),
            vm((ROUNDS, rows, 128), BF),
            vm((ROUNDS, rows, 128), BF),
            vm((rows, 64), F32),
            vm((2, half, 128), F32),
            vm((8, 2, 24, 128), F32),
            vm((8, 2, 24, 128), F32),
            vm((rows, 64), BF),
            vm((rows, 512), BF),
            vm((rows, 512), BF),
            vm((2, 256, ld + lf), F32),
            vm((256, ld + lf), F32),
            vm((8, 32, ld + lf), BF),
            vm((8, 32, ld + lf), BF),
            vm((8, 32, ld + lf), BF),
            dma((6,)),
            dma,
            dma((ROUNDS, 7)),
            dma((ROUNDS,)),
            dma,
            dma((2, 6)),
            dma((2,)),
            dma((2, 5)),
            dma((2,)),
            dma((2,)),
            dma,
            dma,
            dma,
            dma,
            dma,
            dma((ROUNDS,)),
            dma,
            dma((ROUNDS,)),
            dma,
            dma,
            dma,
            dma((2,)),
            dma,
            dma((2, 2)),
            dma,
            dma((2, 2)),
        ],
        compiler_params=pltpu.CompilerParams(
            collective_id=0, has_side_effects=True, vmem_limit_bytes=58 << 20
        ),
    )(bti, ranks, tokens, w, down, up, cot)
    return hid, gt, gd.reshape(4, 64, ld), gu.reshape(4, 64, lf)


def solution(mesh):
    return jax.shard_map(
        shards,
        mesh=mesh,
        in_specs=(
            P(("fsdp", "dp"), "tenant"),
            P(("fsdp", "dp")),
            P(),
            P(("fsdp", "dp"), "tenant"),
            P("tenant", None, None),
            P("tenant", None, None),
            P(("fsdp", "dp"), "tenant"),
        ),
        out_specs=(
            P(("fsdp", "dp"), "tenant"),
            P(("fsdp", "dp"), "tenant"),
            P("dp", None, "tenant"),
            P("dp", None, "tenant"),
        ),
        check_vma=False,
    )
```

```python
import jax
import jax.numpy as jnp
from jax import lax
from jax.experimental import pallas as pl
from jax.experimental.pallas import tpu as pltpu
from jax.sharding import PartitionSpec as P

MESH = pl.DeviceIdType.MESH
BF = jnp.bfloat16
F32 = jnp.float32
BLOCK = 64
ALPHA = 32.0
ROUNDS = 5
SUB = 64


def dot(a, b, ca, cb):
    return lax.dot_general(a, b, (((ca,), (cb,)), ((), ())), preferred_element_type=F32)


def kernel(
    bti,
    ranks,
    tok_h,
    w_h,
    d_h,
    u_h,
    cot_h,
    hid_out,
    gt_out,
    gd_out,
    gu_out,
    tok,
    dq,
    cot,
    wall,
    tokq,
    dmine,
    uall,
    dall,
    ux,
    dx,
    hacc,
    gopp,
    gn,
    gf,
    gor,
    gown,
    grecv,
    gzs,
    gzr,
    gcomp,
    cp2,
    brecv,
    agx,
    agj,
    agexp,
    aexp,
    gpart,
    gpr,
    rss,
    rsr,
    agg,
    lsem,
    wss,
    wrs,
    prs,
    tss,
    trs,
    uss,
    urs,
    upss,
    uprs,
    bss,
    brs,
    ass_,
    ars,
    gos,
    gors,
    gns,
    grs,
    zss,
    zrs,
    xss,
    xrs,
    rss_s,
    rss_r,
    ags_s,
    ags_r,
):
    f = lax.axis_index("fsdp")
    j = lax.axis_index("tenant")
    c = lax.axis_index("dp")
    rows = cot.shape[0]
    half = rows // 2
    lf, ld = cot.shape[1], tok.shape[1]

    def ring(i):
        flip = 1 - 2 * lax.rem(i, 2)
        right, left, opp = lax.rem(i + 2, 8), lax.rem(i + 6, 8), lax.rem(i + 4, 8)
        return dict(
            Z=i + flip,
            R=right,
            L=left,
            O=opp,
            RZ=right + flip,
            LZ=left + flip,
            OZ=opp + flip,
        )

    fn, tn = ring(f), ring(j)
    y, zh = j // 2, lax.rem(j, 2)
    partner = {"dp": 1 - c}

    def rc(src, dst, ss, rs, dev):
        return pltpu.make_async_remote_copy(
            src_ref=src, dst_ref=dst, send_sem=ss, recv_sem=rs, device_id=dev, device_id_type=MESH
        )

    def each(lo, hi, body):
        def step(k, carry):
            body(k)
            return carry

        lax.fori_loop(lo, hi, step, 0)

    def go(src, dst, ss, rs, dev):
        rc(src, dst, ss, rs, dev).start()

    def gone(ref, ss):
        rc(ref, ref, ss, ss, partner).wait_send()

    def got(dst, rs):
        rc(dst, dst, rs, rs, partner).wait_recv()

    barrier = pltpu.get_barrier_semaphore()
    for k in range(1, 8):
        pl.semaphore_signal(barrier, 1, device_id={"fsdp": lax.rem(f + k, 8)}, device_id_type=MESH)
        pl.semaphore_signal(
            barrier, 1, device_id={"tenant": lax.rem(j + k, 8)}, device_id_type=MESH
        )
    pl.semaphore_signal(barrier, 1, device_id=partner, device_id_type=MESH)
    pl.semaphore_signal(
        barrier, 1, device_id={"fsdp": fn["Z"], "tenant": tn["Z"]}, device_id_type=MESH
    )

    def slot(q, fi, ci):
        return wall.at[q, pl.ds((2 * fi + ci) * SUB, SUB)]

    def part(q, fi, ci, h):
        return wall.at[q, pl.ds((2 * fi + ci) * SUB + h * (SUB // 2), SUB // 2)]

    wloc = pltpu.make_async_copy(w_h, wall.at[:, pl.ds((2 * f + c) * SUB, SUB)], lsem.at[0])
    ucol = pl.ds(pl.multiple_of(j * lf, 128), lf)
    dcol = pl.ds(pl.multiple_of(j * ld, 128), ld)
    kloc = pltpu.make_async_copy(tok_h, tok, lsem.at[1])
    mloc = pltpu.make_async_copy(d_h, dmine, lsem.at[2])
    uloc = pltpu.make_async_copy(u_h.at[:, ucol], uall.at[j], lsem.at[3])
    dloc = pltpu.make_async_copy(d_h.at[:, dcol], dall.at[j], lsem.at[4])
    cloc = pltpu.make_async_copy(cot_h, cot, lsem.at[5])
    for d in [wloc, kloc, mloc, uloc, dloc, cloc]:
        d.start()

    def fs(i):
        return {"fsdp": fn[i]}

    def w_send(q, name, rsem, to, src=None):
        ref = slot(q, fn[name] if name else f, c) if src is None else src
        go(ref, ref, wss, rsem, to)

    def w_got(q, k, ref):
        got(ref, wrs.at[q, k])

    def w_A(q):
        w_send(q, None, wrs.at[q, 1], fs("R"))
        w_send(q, None, wrs.at[q, 2], fs("L"))
        w_send(q, None, wrs.at[q, 0], fs("Z"))
        w_send(q, None, prs.at[q], partner)

    def w_B(q):
        w_got(q, 0, slot(q, fn["Z"], c))
        w_send(q, "Z", wrs.at[q, 3], fs("R"))
        w_send(q, "Z", wrs.at[q, 4], fs("L"))
        w_send(q, "Z", prs.at[q], partner)

    def w_CD(q, left, right, kl, kr, ko):
        w_got(q, kl, slot(q, fn[left], c))
        w_send(q, left, wrs.at[q, ko], fs("R"), part(q, fn[left], c, 0))
        w_send(q, left, prs.at[q], partner)
        w_got(q, kr, slot(q, fn[right], c))
        w_send(q, right, wrs.at[q, ko], fs("L"), part(q, fn[right], c, 1))
        w_send(q, right, prs.at[q], partner)

    def w_C(q):
        w_CD(q, "L", "R", 1, 2, 5)

    def w_D(q):
        w_CD(q, "LZ", "RZ", 3, 4, 6)

    def w_E(q):
        for name, k in (("O", 5), ("OZ", 6)):
            w_got(q, k, slot(q, fn[name], c))
            w_send(q, name, prs.at[q], partner)

    def x_C(q):
        for name, k, h, kz, to in (("L", 1, 0, 3, "R"), ("R", 2, 1, 4, "L")):
            w_got(q, k, slot(q, fn[name], c))
            w_send(q, name, wrs.at[q, 5], fs(to), part(q, fn[name], c, h))
            w_send(q, name, wrs.at[q, kz], fs("Z"))
            w_send(q, name, prs.at[q], partner)

    def x_D(q):
        for name, k in (("Z", 0), ("LZ", 3), ("RZ", 4)):
            w_got(q, k, slot(q, fn[name], c))
            w_send(q, name, prs.at[q], partner)

    def x_O(q):
        w_got(q, 5, slot(q, fn["O"], c))
        w_send(q, "O", wrs.at[q, 6], fs("Z"))
        w_send(q, "O", prs.at[q], partner)

    def x_E(q):
        w_got(q, 6, slot(q, fn["OZ"], c))
        w_send(q, "OZ", prs.at[q], partner)

    def w_P(q):
        got(wall.at[q, pl.ds(0, 8 * SUB)], prs.at[q])

    def te(i):
        return {"tenant": tn[i]}

    tq = (pl.ds(0, 3), pl.ds(3, 2))

    def t_ref(ji, p, h=None):
        rows_ = slice(None) if h is None else pl.ds(h * half, half)
        return tokq.at[ji, tq[p], rows_]

    def t_send(p, ji, k, to, h=None):
        ref = t_ref(ji, p, h)
        go(ref, ref, tss, trs.at[p, k], to)

    def pieces(v):
        return [
            jnp.concatenate([v[:, SUB * q : SUB * q + SUB], v[:, 320 + SUB * q : 384 + SUB * q]], axis=1)
            for q in range(ROUNDS)
        ]

    def t_make():
        kloc.wait()
        for q, v in enumerate(pieces(tok[...])):
            tokq[j, q] = v

    def dq_make():
        mloc.wait()
        for i in range(8):
            for q, v in enumerate(pieces(dmine[:, ld * i : ld * i + ld])):
                dq[q, :, 128 * i : 128 * i + 128] = v

    def t_A(p):
        t_send(p, j, 1, te("R"))
        t_send(p, j, 2, te("L"))

    def t_Z(p):
        t_send(p, j, 0, te("Z"))

    def t_B(p):
        got(t_ref(tn["Z"], p), trs.at[p, 0])
        t_send(p, tn["Z"], 3, te("R"))
        t_send(p, tn["Z"], 4, te("L"))

    def t_CD(p, left, right, kl, kr):
        got(t_ref(tn[left], p), trs.at[p, kl])
        t_send(p, tn[left], 5, te("R"), 0)
        got(t_ref(tn[right], p), trs.at[p, kr])
        t_send(p, tn[right], 5, te("L"), 1)

    def t_C(p):
        t_CD(p, "L", "R", 1, 2)

    def t_D(p):
        t_CD(p, "LZ", "RZ", 3, 4)

    def t_E():
        for p in range(2):
            got(tokq.at[pl.ds(0, 2), tq[p]], trs.at[p, 5])

    def adapter(src, width, all_, relay, s):
        def own(ji, ci):
            return all_.at[ji, pl.ds(ci * 32, 32)]

        def out(ji):
            return src.at[pl.ds(c * 32, 32), pl.ds(pl.multiple_of(ji * width, 128), width)]

        return own, out, relay, s

    kinds = (adapter(d_h, ld, dall, dx, 0), adapter(u_h, lf, uall, ux, 1))
    cross = {"fsdp": fn["Z"], "tenant": tn["Z"]}

    def at_y(r):
        return lax.rem(y + r, 4)

    def u_cross():
        for own, out, relay, s in kinds:
            for r in (1, 2, 3, 0):
                dst = own(j, c) if r == 0 else relay.at[r]
                go(out(2 * at_y(r) + 1 - zh), dst, uss.at[s], urs.at[s, r], cross)

    def u_own():
        for own, out, relay, s in kinds:
            for r in range(1, 4):
                to = 2 * at_y(r) + zh
                go(out(to), own(j, c), uss.at[s], urs.at[s, 0], {"tenant": to})

    def u_fwd():
        for own, out, relay, s in kinds:
            for r in range(1, 4):
                got(relay.at[r], urs.at[s, r])
                to = 2 * at_y(r) + zh
                go(relay.at[r], own(tn["Z"], c), uss.at[s], urs.at[s, 4], {"tenant": to})

    def u_recv(e):
        for (own, out, relay, s), all_ in zip(kinds, (dall, uall)):
            got(all_.at[pl.ds(0, 4 - e), pl.ds(0, 32)], urs.at[s, 4 * e])
            for r in range(e, 4):
                ji = 2 * at_y(4 - r) + (1 - zh if e == 1 or r == 0 else zh)
                go(own(ji, c), own(ji, c), upss.at[s], uprs.at[s], partner)

    def u_from_partner():
        for s, all_ in ((0, dall), (1, uall)):
            got(all_.at[pl.ds(0, 7), pl.ds(0, 32)], uprs.at[s])

    def tenant_is(b, t, shape):
        return jnp.full(shape, bti[b], jnp.int32) == t

    def make_gain():
        shape = (BLOCK, 128)
        slot_ = lax.rem(lax.broadcasted_iota(jnp.int32, shape, 1), 64)
        gains = []
        for t in range(8):
            r = jnp.full(shape, ranks[t], jnp.int32)
            gains.append(jnp.where(slot_ < r, ALPHA / r.astype(F32), 0.0))
        for b in range(6):
            g = jnp.zeros(shape, F32)
            for t in range(8):
                g = jnp.where(tenant_is(b, t, g.shape), gains[t], g)
            gcomp[pl.ds(b * BLOCK, BLOCK), :] = g

    def compact(w, a, all_):
        for h in range(2):
            u = all_[pl.ds(4 * h, 4)].reshape(256, a.shape[1])
            p = dot(a[...], u, 1, 1)
            for b in range(6):
                rs = slice(b * BLOCK, (b + 1) * BLOCK)
                acc = jnp.zeros((BLOCK, BLOCK), F32)
                for t in range(4):
                    acc = jnp.where(
                        tenant_is(b, 4 * h + t, acc.shape), p[rs, 64 * t : 64 * t + 64], acc
                    )
                at = (rs, slice(64 * w, 64 * w + 64))
                cp2[at] = acc if h == 0 else cp2[at] + acc

    def b_desc(k):
        to = lax.rem(j + k, 8)
        return rc(cp2.at[pl.ds(to * 48, 48)], brecv.at[k], bss, brs, {"tenant": to})

    def b_sum():
        at = pl.ds(pl.multiple_of(j * 48, 16), 48)
        s = cp2[at, :]
        got(brecv.at[pl.ds(1, 7)], brs)
        for k in range(1, 8):
            s = s + brecv[k]
        agx[j] = (s * gcomp[at, :]).astype(BF)

    def ag_desc(k):
        return rc(agx.at[j], agx.at[j], ass_, ars, {"tenant": lax.rem(j + k, 8)})

    def ag_use():
        got(agx.at[pl.ds(0, 7)], ars)
        both = jnp.concatenate([agx[k] for k in range(8)], axis=0).astype(F32)
        for w, dst in ((0, agexp), (1, aexp)):
            for b in range(6):
                rs = slice(b * BLOCK, (b + 1) * BLOCK)
                v = both[rs, 64 * w : 64 * w + 64]
                zero = jnp.zeros_like(v)
                if w == 0:
                    agj[rs, :] = jnp.where(tenant_is(b, j, v.shape), v, zero).astype(BF)
                for t in range(0, 8, 2):
                    pair = jnp.concatenate(
                        [jnp.where(tenant_is(b, t + e, v.shape), v, zero) for e in range(2)], axis=1
                    )
                    dst[rs, 64 * t : 64 * t + 128] = pair.astype(BF)

    def lhs(q):
        return jnp.concatenate([tokq[i, q] for i in range(8)], axis=1)

    def grad_down_part():
        p = dot(agexp[...], tok[...], 0, 0)
        gpart[0, :, 0:ld] = p[:256]
        gpart[1, :, 0:ld] = p[256:]

    def grad_up_part(lo, hi):
        def body(n):
            at = pl.ds(pl.multiple_of(n * 256, 256), 256)
            to = pl.ds(pl.multiple_of(ld + n * 256, 128), 256)
            p = dot(aexp[...], cot[:, at], 0, 0)
            gpart[0, :, to] = p[:256]
            gpart[1, :, to] = p[256:]

        each(lo, hi, body)

    fx, fz = f // 2, lax.rem(f, 2)
    cols = (pl.ds(0, 896), pl.ds(896, 1536))

    def gx(p):
        go(gpart.at[1 - c, :, cols[p]], gpr.at[:, cols[p]], xss, xrs.at[p], partner)

    def chunk(k, p):
        at = pl.ds(pl.multiple_of(k * 32, 32), 32)
        return gpart[c, at, cols[p]] + gpr[at, cols[p]]

    def rs_z(p):
        got(gpr.at[:, cols[p]], xrs.at[p])

        def body(k):
            rss[k, :, cols[p]] = chunk(2 * k + 1 - fz, p).astype(BF)

        each(0, 4, body)
        at = (pl.ds(0, 4), slice(None), cols[p])
        go(rss.at[at], rsr.at[at], rss_s, rss_r.at[p, 0], fs("Z"))

    def fx_to(r):
        return {"fsdp": lax.rem(f + 2 * r, 8)}

    def rs_x(p):
        got(rsr.at[pl.ds(0, 4), :, cols[p]], rss_r.at[p, 0])
        for r in range(1, 4):
            k = lax.rem(fx + r, 4)
            rss[3 + r, :, cols[p]] = (
                chunk(2 * k + fz, p) + rsr[k, :, cols[p]].astype(F32)
            ).astype(BF)
            at = (3 + r, slice(None), cols[p])
            go(rss.at[at], rsr.at[at], rss_s, rss_r.at[p, 1], fx_to(r))

    def to_x(ref, sem):
        for r in range(1, 4):
            go(ref, ref, ags_s, sem, fx_to(r))

    def rs_sum(p):
        s = chunk(f, p) + rsr[fx, :, cols[p]].astype(F32)
        got(rsr.at[pl.ds(4, 3), :, cols[p]], rss_r.at[p, 1])
        for r in range(1, 4):
            s = s + rsr[3 + r, :, cols[p]].astype(F32)
        agg[f, :, cols[p]] = s.astype(BF)
        ref = agg.at[f, :, cols[p]]
        go(ref, ref, ags_s, ags_r.at[p, 1], fs("Z"))
        to_x(ref, ags_r.at[p, 0])

    def ag_z():
        got(agg.at[pl.ds(0, 3), :, cols[0]], ags_r.at[0, 0])
        for r in range(1, 4):
            ref = agg.at[lax.rem(f + 8 - 2 * r, 8), :, cols[0]]
            go(ref, ref, ags_s, ags_r.at[0, 1], fs("Z"))

    def ag_x():
        ref = agg.at[fn["Z"], :, cols[1]]
        got(ref, ags_r.at[1, 1])
        to_x(ref, ags_r.at[1, 0])

    def grads_out(p):
        if p == 0:
            got(agg.at[pl.ds(0, 4), :, cols[p]], ags_r.at[p, 1])
        else:
            got(agg.at[pl.ds(0, 6), :, cols[p]], ags_r.at[p, 0])

        def body(k):
            at = pl.ds(pl.multiple_of(k * 32, 32), 32)
            v = agg[k, :, cols[p]].astype(F32)
            if p == 0:
                gd_out[at, :] = v[:, :ld]
                gu_out[at, 0:256] = v[:, ld:]
            else:
                gu_out[at, 256:] = v

        each(0, 8, body)

    top, bottom = pl.ds(0, half), pl.ds(half, half)

    def g_near(q, e, at):
        go(gn.at[q, e, at], grecv.at[q, e, at], gns, grs.at[q], te("RL"[e]))

    def compute_g(q):
        def body(k):
            i = lax.rem(y + 2 + 3 * k, 4)
            at = pl.ds(pl.multiple_of(i * 256, 256), 256)
            p = dot(cot[...], wall[q, at, :], 1, 1) + dot(agj[...], dq[q, :, at], 1, 0)

            @pl.when(k == 0)
            def _():
                gopp[q] = p.astype(BF)
                go(gopp.at[q, top], gor.at[q, 0], gos, gors.at[q], te("R"))
                go(gopp.at[q, bottom], gor.at[q, 1], gos, gors.at[q], te("L"))

            @pl.when(k == 1)
            def _():
                gf[q, 0] = p[:half]
                gn[q, 0, half:] = p[half:].astype(BF)
                g_near(q, 0, bottom)

            @pl.when(k == 2)
            def _():
                gown[q] = p

            @pl.when(k == 3)
            def _():
                gf[q, 1] = p[half:]
                gn[q, 1, :half] = p[:half].astype(BF)
                g_near(q, 1, top)

        each(0, 4, body)

    def g_acc(q):
        got(gor.at[q], gors.at[q])
        for e, at in enumerate((top, bottom)):
            gn[q, e, at] = (gf[q, e] + gor[q, e].astype(F32)).astype(BF)
            g_near(q, e, at)

    def compute_h(q):
        def body(n):
            at = pl.ds(pl.multiple_of(n * 256, 256), 256)
            p = dot(lhs(q), wall[q, :, at], 1, 0)
            if q == 0:
                hacc[:, at] = p
            elif q < ROUNDS - 1:
                hacc[:, at] += p
            else:
                u = uall[:, :, at].reshape(512, 256)
                hid_out[:, at] = (hacc[:, at] + p + dot(aexp[...], u, 1, 0)).astype(BF)

        each(0, lf // 256, body)

    def g_sum(q):
        got(grecv.at[q], grs.at[q])
        mine = pl.ds(pl.multiple_of(zh * 128, 128), 128)
        other = pl.ds(pl.multiple_of(128 - zh * 128, 128), 128)

        def total(at):
            s = gown[q, :, at]
            for k in range(2):
                s = s + grecv[q, k, :, at].astype(F32)
            return s

        gzs[q] = total(other).astype(BF)
        go(gzs.at[q], gzr.at[q], zss, zrs, te("Z"))
        gown[q, :, mine] = total(mine)

    def gt_final():
        mine = pl.ds(pl.multiple_of(zh * 128, 128), 128)
        got(gzr, zrs)

        def body(b):
            at = pl.ds(pl.multiple_of(b * BLOCK, BLOCK), BLOCK)
            s = [gown[q, at, mine] + gzr[q, at, :].astype(F32) for q in range(ROUNDS)]
            row = jnp.concatenate([v[:, :64] for v in s] + [v[:, 64:] for v in s], axis=1)
            gt_out[at, :] = row.astype(BF)

        each(0, 6, body)

    t_make()
    dq_make()
    make_gain()
    wloc.wait()
    pl.semaphore_wait(barrier, 16)
    w_A(0)
    u_cross()
    u_own()
    w_A(1)
    t_A(0)
    w_B(0)
    w_C(0)
    w_A(2)
    u_fwd()
    t_A(1)
    t_Z(0)
    t_Z(1)
    t_C(0)
    u_recv(0)
    w_D(0)
    w_B(1)
    w_C(1)
    w_A(3)
    u_recv(1)
    uloc.wait()
    dloc.wait()
    cloc.wait()
    u_from_partner()
    compact(0, cot, uall)
    compact(1, tok, dall)
    each(1, 8, lambda k: b_desc(k).start())
    t_C(1)
    w_E(0)
    b_sum()
    each(1, 8, lambda k: ag_desc(k).start())
    t_B(0)
    t_B(1)
    w_A(4)
    w_D(1)
    x_C(2)
    ag_use()
    w_P(0)
    compute_g(0)
    w_B(3)
    w_C(3)
    grad_down_part()
    grad_up_part(0, 1)
    gx(0)
    grad_up_part(1, 7)
    gx(1)
    w_E(1)
    t_D(0)
    w_B(4)
    x_O(2)
    rs_z(0)
    t_D(1)
    w_P(1)
    compute_g(1)
    g_acc(0)
    x_D(2)
    w_D(3)
    w_C(4)
    rs_z(1)
    x_E(2)
    w_P(2)
    compute_g(2)
    g_acc(1)
    w_D(4)
    t_E()
    compute_h(0)
    w_E(3)
    rs_x(0)
    w_P(3)
    compute_g(3)
    g_acc(2)
    rs_x(1)
    g_sum(0)
    w_E(4)
    compute_h(1)
    w_P(4)
    compute_g(4)
    g_acc(3)
    g_sum(1)
    compute_h(2)
    rs_sum(0)
    rs_sum(1)
    g_sum(2)
    g_acc(4)
    compute_h(3)
    ag_x()
    ag_z()
    g_sum(3)
    g_sum(4)
    compute_h(4)
    grads_out(1)
    grads_out(0)
    gt_final()

    gone(wall.at[:, pl.ds(0, 15 * SUB)], wss)
    gone(tokq.at[pl.ds(0, 7)], tss)
    for s, all_ in ((0, dall), (1, uall)):
        gone(all_.at[pl.ds(0, 5)], uss.at[s])
        gone(all_.at[pl.ds(0, 7), pl.ds(0, 32)], upss.at[s])
    gone(brecv.at[pl.ds(0, 7)], bss)
    gone(agx.at[pl.ds(0, 7)], ass_)
    gone(gopp, gos)
    gone(gn, gns)
    gone(gzs, zss)
    gone(gpr, xss)
    gone(rss.at[pl.ds(0, 7)], rss_s)
    gone(agg.at[pl.ds(0, 7)], ags_s)


def store(*refs):
    sems = refs[8]
    copies = [pltpu.make_async_copy(refs[i], refs[4 + i], sems.at[i]) for i in range(4)]
    for d in copies:
        d.start()
    for d in copies:
        d.wait()


def shards(tokens, bti, ranks, w, down, up, cot):
    rows, ld = tokens.shape
    lf = cot.shape[1]
    up = up.reshape(up.shape[1:])
    w = w.reshape(ROUNDS, SUB, lf)
    down = down.reshape(down.shape[1:])
    dma = pltpu.SemaphoreType.DMA
    vm = pltpu.VMEM
    smem = pl.BlockSpec(memory_space=pltpu.SMEM)
    hbm = pl.BlockSpec(memory_space=pl.ANY)
    out = pl.BlockSpec(memory_space=pltpu.VMEM)
    half = rows // 2
    hid, gt, gd, gu = pl.pallas_call(
        kernel,
        out_shape=(
            pltpu.VMEM((rows, lf), BF),
            pltpu.VMEM((rows, ld), BF),
            pltpu.VMEM((256, ld), F32),
            pltpu.VMEM((256, lf), F32),
        ),
        in_specs=[smem, smem, hbm, hbm, hbm, hbm, hbm],
        out_specs=(out, out, out, out),
        scratch_shapes=[
            vm((rows, ld), BF),
            vm((ROUNDS, 64, 1024), BF),
            vm((rows, lf), BF),
            vm((ROUNDS, 1024, lf), BF),
            vm((8, ROUNDS, rows, 128), BF),
            vm((64, 5120), BF),
            vm((8, 64, lf), BF),
            vm((8, 64, ld), BF),
            vm((4, 32, lf), BF),
            vm((4, 32, ld), BF),
            vm((rows, lf), F32),
            vm((ROUNDS, rows, 256), BF),
            vm((ROUNDS, 2, rows, 256), BF),
            vm((ROUNDS, 2, half, 256), F32),
            vm((ROUNDS, 2, half, 256), BF),
            vm((ROUNDS, rows, 256), F32),
            vm((ROUNDS, 2, rows, 256), BF),
            vm((ROUNDS, rows, 128), BF),
            vm((ROUNDS, rows, 128), BF),
            vm((rows, 128), F32),
            vm((rows, 128), F32),
            vm((8, 48, 128), F32),
            vm((8, 48, 128), BF),
            vm((rows, 64), BF),
            vm((rows, 512), BF),
            vm((rows, 512), BF),
            vm((2, 256, ld + lf), F32),
            vm((256, ld + lf), F32),
            vm((8, 32, ld + lf), BF),
            vm((8, 32, ld + lf), BF),
            vm((8, 32, ld + lf), BF),
            dma((6,)),
            dma,
            dma((ROUNDS, 7)),
            dma((ROUNDS,)),
            dma,
            dma((2, 6)),
            dma((2,)),
            dma((2, 5)),
            dma((2,)),
            dma((2,)),
            dma,
            dma,
            dma,
            dma,
            dma,
            dma((ROUNDS,)),
            dma,
            dma((ROUNDS,)),
            dma,
            dma,
            dma,
            dma((2,)),
            dma,
            dma((2, 2)),
            dma,
            dma((2, 2)),
        ],
        compiler_params=pltpu.CompilerParams(
            collective_id=0, has_side_effects=True, vmem_limit_bytes=58 << 20
        ),
    )(bti, ranks, tokens, w, down, up, cot)
    kept = [pltpu.with_memory_space_constraint(r, pltpu.VMEM) for r in (hid, gt, gd, gu)]
    hid, gt, gd, gu = pl.pallas_call(
        store,
        out_shape=tuple(jax.ShapeDtypeStruct(r.shape, r.dtype) for r in kept),
        in_specs=[out] * 4,
        out_specs=[hbm] * 4,
        scratch_shapes=[dma((4,))],
        compiler_params=pltpu.CompilerParams(vmem_limit_bytes=1 << 20),
    )(*kept)
    return hid, gt, gd.reshape(4, 64, ld), gu.reshape(4, 64, lf)


def solution(mesh):
    return jax.shard_map(
        shards,
        mesh=mesh,
        in_specs=(
            P(("fsdp", "dp"), "tenant"),
            P(("fsdp", "dp")),
            P(),
            P(("fsdp", "dp"), "tenant"),
            P("tenant", None, None),
            P("tenant", None, None),
            P(("fsdp", "dp"), "tenant"),
        ),
        out_specs=(
            P(("fsdp", "dp"), "tenant"),
            P(("fsdp", "dp"), "tenant"),
            P("dp", None, "tenant"),
            P("dp", None, "tenant"),
        ),
        check_vma=False,
    )
```

```python
import jax
import jax.numpy as jnp
from jax import lax
from jax.experimental import pallas as pl
from jax.experimental.pallas import tpu as pltpu
from jax.sharding import PartitionSpec as P

MESH = pl.DeviceIdType.MESH
BF = jnp.bfloat16
F32 = jnp.float32
BLOCK = 64
ALPHA = 32.0
ROUNDS = 5
SUB = 64


def dot(a, b, ca, cb):
    return lax.dot_general(a, b, (((ca,), (cb,)), ((), ())), preferred_element_type=F32)


def kernel(
    bti,
    ranks,
    tok_h,
    w_h,
    d_h,
    u_h,
    cot_h,
    hid_out,
    gt_out,
    gd_out,
    gu_out,
    tok,
    dq,
    cot,
    wall,
    tokq,
    dmine,
    uall,
    dall,
    ux,
    dx,
    hacc,
    gopp,
    gn,
    gf,
    gor,
    gown,
    grecv,
    gzs,
    gzr,
    gcomp,
    cp2,
    brecv,
    agx,
    agj,
    agexp,
    aexp,
    gpart,
    gpr,
    rss,
    rsr,
    agg,
    lsem,
    wss,
    wrs,
    prs,
    tss,
    trs,
    uss,
    urs,
    upss,
    uprs,
    bss,
    brs,
    ass_,
    ars,
    gos,
    gors,
    gns,
    grs,
    zss,
    zrs,
    xss,
    xrs,
    rss_s,
    rss_r,
    ags_s,
    ags_r,
):
    f = lax.axis_index("fsdp")
    j = lax.axis_index("tenant")
    c = lax.axis_index("dp")
    rows = cot.shape[0]
    half = rows // 2
    lf, ld = cot.shape[1], tok.shape[1]

    def ring(i):
        flip = 1 - 2 * lax.rem(i, 2)
        right, left, opp = lax.rem(i + 2, 8), lax.rem(i + 6, 8), lax.rem(i + 4, 8)
        return dict(
            Z=i + flip,
            R=right,
            L=left,
            O=opp,
            RZ=right + flip,
            LZ=left + flip,
            OZ=opp + flip,
        )

    fn, tn = ring(f), ring(j)
    y, zh = j // 2, lax.rem(j, 2)
    partner = {"dp": 1 - c}

    def rc(src, dst, ss, rs, dev):
        return pltpu.make_async_remote_copy(
            src_ref=src, dst_ref=dst, send_sem=ss, recv_sem=rs, device_id=dev, device_id_type=MESH
        )

    def each(lo, hi, body):
        def step(k, carry):
            body(k)
            return carry

        lax.fori_loop(lo, hi, step, 0)

    def go(src, dst, ss, rs, dev):
        rc(src, dst, ss, rs, dev).start()

    def gone(ref, ss):
        rc(ref, ref, ss, ss, partner).wait_send()

    def got(dst, rs):
        rc(dst, dst, rs, rs, partner).wait_recv()

    barrier = pltpu.get_barrier_semaphore()
    for k in range(1, 8):
        pl.semaphore_signal(barrier, 1, device_id={"fsdp": lax.rem(f + k, 8)}, device_id_type=MESH)
        pl.semaphore_signal(
            barrier, 1, device_id={"tenant": lax.rem(j + k, 8)}, device_id_type=MESH
        )
    pl.semaphore_signal(barrier, 1, device_id=partner, device_id_type=MESH)
    pl.semaphore_signal(
        barrier, 1, device_id={"fsdp": fn["Z"], "tenant": tn["Z"]}, device_id_type=MESH
    )

    def slot(q, fi, ci):
        return wall.at[q, pl.ds((2 * fi + ci) * SUB, SUB)]

    def part(q, fi, ci, h):
        return wall.at[q, pl.ds((2 * fi + ci) * SUB + h * (SUB // 2), SUB // 2)]

    wloc = pltpu.make_async_copy(w_h, wall.at[:, pl.ds((2 * f + c) * SUB, SUB)], lsem.at[0])
    ucol = pl.ds(pl.multiple_of(j * lf, 128), lf)
    dcol = pl.ds(pl.multiple_of(j * ld, 128), ld)
    kloc = pltpu.make_async_copy(tok_h, tok, lsem.at[1])
    mloc = pltpu.make_async_copy(d_h, dmine, lsem.at[2])
    uloc = pltpu.make_async_copy(u_h.at[:, ucol], uall.at[j], lsem.at[3])
    dloc = pltpu.make_async_copy(d_h.at[:, dcol], dall.at[j], lsem.at[4])
    cloc = pltpu.make_async_copy(cot_h, cot, lsem.at[5])
    for d in [wloc, kloc, mloc, uloc, dloc, cloc]:
        d.start()

    def fs(i):
        return {"fsdp": fn[i]}

    def w_send(q, name, rsem, to, src=None):
        ref = slot(q, fn[name] if name else f, c) if src is None else src
        go(ref, ref, wss, rsem, to)

    def w_got(q, k, ref):
        got(ref, wrs.at[q, k])

    def w_A(q):
        w_send(q, None, wrs.at[q, 1], fs("R"))
        w_send(q, None, wrs.at[q, 2], fs("L"))
        w_send(q, None, wrs.at[q, 0], fs("Z"))
        w_send(q, None, prs.at[q], partner)

    def w_B(q):
        w_got(q, 0, slot(q, fn["Z"], c))
        w_send(q, "Z", wrs.at[q, 3], fs("R"))
        w_send(q, "Z", wrs.at[q, 4], fs("L"))
        w_send(q, "Z", prs.at[q], partner)

    def w_CD(q, left, right, kl, kr, ko):
        w_got(q, kl, slot(q, fn[left], c))
        w_send(q, left, wrs.at[q, ko], fs("R"), part(q, fn[left], c, 0))
        w_send(q, left, prs.at[q], partner)
        w_got(q, kr, slot(q, fn[right], c))
        w_send(q, right, wrs.at[q, ko], fs("L"), part(q, fn[right], c, 1))
        w_send(q, right, prs.at[q], partner)

    def w_C(q):
        w_CD(q, "L", "R", 1, 2, 5)

    def w_D(q):
        w_CD(q, "LZ", "RZ", 3, 4, 6)

    def w_E(q):
        for name, k in (("O", 5), ("OZ", 6)):
            w_got(q, k, slot(q, fn[name], c))
            w_send(q, name, prs.at[q], partner)

    def x_C(q):
        for name, k, h, kz, to in (("L", 1, 0, 3, "R"), ("R", 2, 1, 4, "L")):
            w_got(q, k, slot(q, fn[name], c))
            w_send(q, name, wrs.at[q, 5], fs(to), part(q, fn[name], c, h))
            w_send(q, name, wrs.at[q, kz], fs("Z"))
            w_send(q, name, prs.at[q], partner)

    def x_D(q):
        for name, k in (("Z", 0), ("LZ", 3), ("RZ", 4)):
            w_got(q, k, slot(q, fn[name], c))
            w_send(q, name, prs.at[q], partner)

    def x_O(q):
        w_got(q, 5, slot(q, fn["O"], c))
        w_send(q, "O", wrs.at[q, 6], fs("Z"))
        w_send(q, "O", prs.at[q], partner)

    def x_E(q):
        w_got(q, 6, slot(q, fn["OZ"], c))
        w_send(q, "OZ", prs.at[q], partner)

    def w_P(q):
        got(wall.at[q, pl.ds(0, 8 * SUB)], prs.at[q])

    def te(i):
        return {"tenant": tn[i]}

    tq = (pl.ds(0, 3), pl.ds(3, 2))

    def t_ref(ji, p, h=None):
        rows_ = slice(None) if h is None else pl.ds(h * half, half)
        return tokq.at[ji, tq[p], rows_]

    def t_send(p, ji, k, to, h=None):
        ref = t_ref(ji, p, h)
        go(ref, ref, tss, trs.at[p, k], to)

    def pieces(v):
        return [
            jnp.concatenate([v[:, SUB * q : SUB * q + SUB], v[:, 320 + SUB * q : 384 + SUB * q]], axis=1)
            for q in range(ROUNDS)
        ]

    def t_make():
        kloc.wait()
        for q, v in enumerate(pieces(tok[...])):
            tokq[j, q] = v

    def dq_make():
        mloc.wait()
        for i in range(8):
            for q, v in enumerate(pieces(dmine[:, ld * i : ld * i + ld])):
                dq[q, :, 128 * i : 128 * i + 128] = v

    def t_A(p):
        t_send(p, j, 1, te("R"))
        t_send(p, j, 2, te("L"))

    def t_Z(p):
        t_send(p, j, 0, te("Z"))

    def t_B(p):
        got(t_ref(tn["Z"], p), trs.at[p, 0])
        t_send(p, tn["Z"], 3, te("R"))
        t_send(p, tn["Z"], 4, te("L"))

    def t_CD(p, left, right, kl, kr):
        got(t_ref(tn[left], p), trs.at[p, kl])
        t_send(p, tn[left], 5, te("R"), 0)
        got(t_ref(tn[right], p), trs.at[p, kr])
        t_send(p, tn[right], 5, te("L"), 1)

    def t_C(p):
        t_CD(p, "L", "R", 1, 2)

    def t_D(p):
        t_CD(p, "LZ", "RZ", 3, 4)

    def t_E():
        for p in range(2):
            got(tokq.at[pl.ds(0, 2), tq[p]], trs.at[p, 5])

    def adapter(src, width, all_, relay, s):
        def own(ji, ci):
            return all_.at[ji, pl.ds(ci * 32, 32)]

        def out(ji):
            return src.at[pl.ds(c * 32, 32), pl.ds(pl.multiple_of(ji * width, 128), width)]

        return own, out, relay, s

    kinds = (adapter(d_h, ld, dall, dx, 0), adapter(u_h, lf, uall, ux, 1))
    cross = {"fsdp": fn["Z"], "tenant": tn["Z"]}

    def at_y(r):
        return lax.rem(y + r, 4)

    def u_cross():
        for own, out, relay, s in kinds:
            for r in (1, 2, 3, 0):
                dst = own(j, c) if r == 0 else relay.at[r]
                go(out(2 * at_y(r) + 1 - zh), dst, uss.at[s], urs.at[s, r], cross)

    def u_own():
        for own, out, relay, s in kinds:
            for r in range(1, 4):
                to = 2 * at_y(r) + zh
                go(out(to), own(j, c), uss.at[s], urs.at[s, 0], {"tenant": to})

    def u_fwd():
        for own, out, relay, s in kinds:
            for r in range(1, 4):
                got(relay.at[r], urs.at[s, r])
                to = 2 * at_y(r) + zh
                go(relay.at[r], own(tn["Z"], c), uss.at[s], urs.at[s, 4], {"tenant": to})

    def u_recv(e):
        for (own, out, relay, s), all_ in zip(kinds, (dall, uall)):
            got(all_.at[pl.ds(0, 4 - e), pl.ds(0, 32)], urs.at[s, 4 * e])
            for r in range(e, 4):
                ji = 2 * at_y(4 - r) + (1 - zh if e == 1 or r == 0 else zh)
                go(own(ji, c), own(ji, c), upss.at[s], uprs.at[s], partner)

    def u_from_partner():
        for s, all_ in ((0, dall), (1, uall)):
            got(all_.at[pl.ds(0, 7), pl.ds(0, 32)], uprs.at[s])

    def tenant_is(b, t, shape):
        return jnp.full(shape, bti[b], jnp.int32) == t

    def make_gain():
        shape = (BLOCK, 128)
        slot_ = lax.rem(lax.broadcasted_iota(jnp.int32, shape, 1), 64)
        gains = []
        for t in range(8):
            r = jnp.full(shape, ranks[t], jnp.int32)
            gains.append(jnp.where(slot_ < r, ALPHA / r.astype(F32), 0.0))
        for b in range(6):
            g = jnp.zeros(shape, F32)
            for t in range(8):
                g = jnp.where(tenant_is(b, t, g.shape), gains[t], g)
            gcomp[pl.ds(b * BLOCK, BLOCK), :] = g

    def compact(w, a, all_):
        for h in range(2):
            u = all_[pl.ds(4 * h, 4)].reshape(256, a.shape[1])
            p = dot(a[...], u, 1, 1)
            for b in range(6):
                rs = slice(b * BLOCK, (b + 1) * BLOCK)
                acc = jnp.zeros((BLOCK, BLOCK), F32)
                for t in range(4):
                    acc = jnp.where(
                        tenant_is(b, 4 * h + t, acc.shape), p[rs, 64 * t : 64 * t + 64], acc
                    )
                at = (rs, slice(64 * w, 64 * w + 64))
                cp2[at] = acc if h == 0 else cp2[at] + acc

    def b_desc(k):
        to = lax.rem(j + k, 8)
        return rc(cp2.at[pl.ds(to * 48, 48)], brecv.at[k], bss, brs, {"tenant": to})

    def b_sum():
        at = pl.ds(pl.multiple_of(j * 48, 16), 48)
        s = cp2[at, :]
        got(brecv.at[pl.ds(1, 7)], brs)
        for k in range(1, 8):
            s = s + brecv[k]
        agx[j] = (s * gcomp[at, :]).astype(BF)

    def ag_desc(k):
        return rc(agx.at[j], agx.at[j], ass_, ars, {"tenant": lax.rem(j + k, 8)})

    def ag_use():
        got(agx.at[pl.ds(0, 7)], ars)
        both = jnp.concatenate([agx[k] for k in range(8)], axis=0).astype(F32)
        for w, dst in ((0, agexp), (1, aexp)):
            for b in range(6):
                rs = slice(b * BLOCK, (b + 1) * BLOCK)
                v = both[rs, 64 * w : 64 * w + 64]
                zero = jnp.zeros_like(v)
                if w == 0:
                    agj[rs, :] = jnp.where(tenant_is(b, j, v.shape), v, zero).astype(BF)
                for t in range(0, 8, 2):
                    pair = jnp.concatenate(
                        [jnp.where(tenant_is(b, t + e, v.shape), v, zero) for e in range(2)], axis=1
                    )
                    dst[rs, 64 * t : 64 * t + 128] = pair.astype(BF)

    def lhs(q):
        return jnp.concatenate([tokq[i, q] for i in range(8)], axis=1)

    def grad_down_part():
        p = dot(agexp[...], tok[...], 0, 0)
        gpart[0, :, 0:ld] = p[:256]
        gpart[1, :, 0:ld] = p[256:]

    def grad_up_part(lo, hi):
        def body(n):
            at = pl.ds(pl.multiple_of(n * 256, 256), 256)
            to = pl.ds(pl.multiple_of(ld + n * 256, 128), 256)
            p = dot(aexp[...], cot[:, at], 0, 0)
            gpart[0, :, to] = p[:256]
            gpart[1, :, to] = p[256:]

        each(lo, hi, body)

    fx, fz = f // 2, lax.rem(f, 2)
    cols = (pl.ds(0, 1152), pl.ds(1152, 1280))

    def gx(p):
        go(gpart.at[1 - c, :, cols[p]], gpr.at[:, cols[p]], xss, xrs.at[p], partner)

    def chunk(k, p):
        at = pl.ds(pl.multiple_of(k * 32, 32), 32)
        return gpart[c, at, cols[p]] + gpr[at, cols[p]]

    def rs_z(p):
        got(gpr.at[:, cols[p]], xrs.at[p])

        def body(k):
            rss[k, :, cols[p]] = chunk(2 * k + 1 - fz, p).astype(BF)

        each(0, 4, body)
        at = (pl.ds(0, 4), slice(None), cols[p])
        go(rss.at[at], rsr.at[at], rss_s, rss_r.at[p, 0], fs("Z"))

    def fx_to(r):
        return {"fsdp": lax.rem(f + 2 * r, 8)}

    def rs_x(p):
        got(rsr.at[pl.ds(0, 4), :, cols[p]], rss_r.at[p, 0])
        for r in range(1, 4):
            k = lax.rem(fx + r, 4)
            rss[3 + r, :, cols[p]] = (
                chunk(2 * k + fz, p) + rsr[k, :, cols[p]].astype(F32)
            ).astype(BF)
            at = (3 + r, slice(None), cols[p])
            go(rss.at[at], rsr.at[at], rss_s, rss_r.at[p, 1], fx_to(r))

    def to_x(ref, sem):
        for r in range(1, 4):
            go(ref, ref, ags_s, sem, fx_to(r))

    def rs_sum(p):
        s = chunk(f, p) + rsr[fx, :, cols[p]].astype(F32)
        got(rsr.at[pl.ds(4, 3), :, cols[p]], rss_r.at[p, 1])
        for r in range(1, 4):
            s = s + rsr[3 + r, :, cols[p]].astype(F32)
        agg[f, :, cols[p]] = s.astype(BF)
        ref = agg.at[f, :, cols[p]]
        go(ref, ref, ags_s, ags_r.at[p, 1], fs("Z"))
        to_x(ref, ags_r.at[p, 0])

    def ag_x(p):
        ref = agg.at[fn["Z"], :, cols[p]]
        got(ref, ags_r.at[p, 1])
        to_x(ref, ags_r.at[p, 0])

    def grads_out(p):
        got(agg.at[pl.ds(0, 6), :, cols[p]], ags_r.at[p, 0])

        def body(k):
            at = pl.ds(pl.multiple_of(k * 32, 32), 32)
            v = agg[k, :, cols[p]].astype(F32)
            if p == 0:
                gd_out[at, :] = v[:, :ld]
                gu_out[at, 0:512] = v[:, ld:]
            else:
                gu_out[at, 512:] = v

        each(0, 8, body)

    top, bottom = pl.ds(0, half), pl.ds(half, half)

    def g_near(q, e, at):
        go(gn.at[q, e, at], grecv.at[q, e, at], gns, grs.at[q], te("RL"[e]))

    def compute_g(q):
        def body(k):
            i = lax.rem(y + 2 + 3 * k, 4)
            at = pl.ds(pl.multiple_of(i * 256, 256), 256)
            p = dot(cot[...], wall[q, at, :], 1, 1) + dot(agj[...], dq[q, :, at], 1, 0)

            @pl.when(k == 0)
            def _():
                gopp[q] = p.astype(BF)
                go(gopp.at[q, top], gor.at[q, 0], gos, gors.at[q], te("R"))
                go(gopp.at[q, bottom], gor.at[q, 1], gos, gors.at[q], te("L"))

            @pl.when(k == 1)
            def _():
                gf[q, 0] = p[:half]
                gn[q, 0, half:] = p[half:].astype(BF)
                g_near(q, 0, bottom)

            @pl.when(k == 2)
            def _():
                gown[q] = p

            @pl.when(k == 3)
            def _():
                gf[q, 1] = p[half:]
                gn[q, 1, :half] = p[:half].astype(BF)
                g_near(q, 1, top)

        each(0, 4, body)

    def g_acc(q):
        got(gor.at[q], gors.at[q])
        for e, at in enumerate((top, bottom)):
            gn[q, e, at] = (gf[q, e] + gor[q, e].astype(F32)).astype(BF)
            g_near(q, e, at)

    def compute_h(q):
        def body(n):
            at = pl.ds(pl.multiple_of(n * 256, 256), 256)
            p = dot(lhs(q), wall[q, :, at], 1, 0)
            if q == 0:
                hacc[:, at] = p
            elif q < ROUNDS - 1:
                hacc[:, at] += p
            else:
                u = uall[:, :, at].reshape(512, 256)
                hid_out[:, at] = (hacc[:, at] + p + dot(aexp[...], u, 1, 0)).astype(BF)

        each(0, lf // 256, body)

    def g_sum(q):
        got(grecv.at[q], grs.at[q])
        mine = pl.ds(pl.multiple_of(zh * 128, 128), 128)
        other = pl.ds(pl.multiple_of(128 - zh * 128, 128), 128)

        def total(at):
            s = gown[q, :, at]
            for k in range(2):
                s = s + grecv[q, k, :, at].astype(F32)
            return s

        gzs[q] = total(other).astype(BF)
        go(gzs.at[q], gzr.at[q], zss, zrs, te("Z"))
        gown[q, :, mine] = total(mine)

    def gt_final():
        mine = pl.ds(pl.multiple_of(zh * 128, 128), 128)
        got(gzr, zrs)

        def body(b):
            at = pl.ds(pl.multiple_of(b * BLOCK, BLOCK), BLOCK)
            s = [gown[q, at, mine] + gzr[q, at, :].astype(F32) for q in range(ROUNDS)]
            row = jnp.concatenate([v[:, :64] for v in s] + [v[:, 64:] for v in s], axis=1)
            gt_out[at, :] = row.astype(BF)

        each(0, 6, body)

    t_make()
    dq_make()
    make_gain()
    wloc.wait()
    pl.semaphore_wait(barrier, 16)
    w_A(0)
    u_cross()
    u_own()
    w_A(1)
    t_A(0)
    w_B(0)
    w_C(0)
    w_A(2)
    u_fwd()
    t_A(1)
    t_Z(0)
    t_Z(1)
    t_C(0)
    u_recv(0)
    w_D(0)
    w_B(1)
    w_C(1)
    w_A(3)
    u_recv(1)
    uloc.wait()
    dloc.wait()
    cloc.wait()
    u_from_partner()
    compact(0, cot, uall)
    compact(1, tok, dall)
    each(1, 8, lambda k: b_desc(k).start())
    t_C(1)
    t_B(1)
    w_E(0)
    b_sum()
    each(1, 8, lambda k: ag_desc(k).start())
    t_B(0)
    w_A(4)
    w_D(1)
    x_C(2)
    ag_use()
    w_P(0)
    compute_g(0)
    w_B(3)
    w_C(3)
    grad_down_part()
    grad_up_part(0, 2)
    gx(0)
    grad_up_part(2, 7)
    gx(1)
    w_E(1)
    t_D(1)
    w_B(4)
    x_O(2)
    rs_z(0)
    t_D(0)
    w_P(1)
    compute_g(1)
    g_acc(0)
    x_D(2)
    w_D(3)
    w_C(4)
    rs_z(1)
    x_E(2)
    w_P(2)
    compute_g(2)
    g_acc(1)
    w_D(4)
    t_E()
    compute_h(0)
    w_E(3)
    rs_x(0)
    w_P(3)
    compute_g(3)
    g_acc(2)
    rs_x(1)
    g_sum(0)
    w_E(4)
    compute_h(1)
    rs_sum(0)
    w_P(4)
    compute_g(4)
    g_acc(3)
    rs_sum(1)
    g_sum(1)
    compute_h(2)
    g_sum(2)
    ag_x(0)
    g_acc(4)
    ag_x(1)
    compute_h(3)
    g_sum(3)
    g_sum(4)
    compute_h(4)
    grads_out(0)
    grads_out(1)
    gt_final()

    gone(wall.at[:, pl.ds(0, 15 * SUB)], wss)
    gone(tokq.at[pl.ds(0, 7)], tss)
    for s, all_ in ((0, dall), (1, uall)):
        gone(all_.at[pl.ds(0, 5)], uss.at[s])
        gone(all_.at[pl.ds(0, 7), pl.ds(0, 32)], upss.at[s])
    gone(brecv.at[pl.ds(0, 7)], bss)
    gone(agx.at[pl.ds(0, 7)], ass_)
    gone(gopp, gos)
    gone(gn, gns)
    gone(gzs, zss)
    gone(gpr, xss)
    gone(rss.at[pl.ds(0, 7)], rss_s)
    gone(agg.at[pl.ds(0, 7)], ags_s)


def store(*refs):
    sems = refs[8]
    copies = [pltpu.make_async_copy(refs[i], refs[4 + i], sems.at[i]) for i in range(4)]
    for d in copies:
        d.start()
    for d in copies:
        d.wait()


def shards(tokens, bti, ranks, w, down, up, cot):
    rows, ld = tokens.shape
    lf = cot.shape[1]
    up = up.reshape(up.shape[1:])
    w = w.reshape(ROUNDS, SUB, lf)
    down = down.reshape(down.shape[1:])
    dma = pltpu.SemaphoreType.DMA
    vm = pltpu.VMEM
    smem = pl.BlockSpec(memory_space=pltpu.SMEM)
    hbm = pl.BlockSpec(memory_space=pl.ANY)
    out = pl.BlockSpec(memory_space=pltpu.VMEM)
    half = rows // 2
    hid, gt, gd, gu = pl.pallas_call(
        kernel,
        out_shape=(
            pltpu.VMEM((rows, lf), BF),
            pltpu.VMEM((rows, ld), BF),
            pltpu.VMEM((256, ld), F32),
            pltpu.VMEM((256, lf), F32),
        ),
        in_specs=[smem, smem, hbm, hbm, hbm, hbm, hbm],
        out_specs=(out, out, out, out),
        scratch_shapes=[
            vm((rows, ld), BF),
            vm((ROUNDS, 64, 1024), BF),
            vm((rows, lf), BF),
            vm((ROUNDS, 1024, lf), BF),
            vm((8, ROUNDS, rows, 128), BF),
            vm((64, 5120), BF),
            vm((8, 64, lf), BF),
            vm((8, 64, ld), BF),
            vm((4, 32, lf), BF),
            vm((4, 32, ld), BF),
            vm((rows, lf), F32),
            vm((ROUNDS, rows, 256), BF),
            vm((ROUNDS, 2, rows, 256), BF),
            vm((ROUNDS, 2, half, 256), F32),
            vm((ROUNDS, 2, half, 256), BF),
            vm((ROUNDS, rows, 256), F32),
            vm((ROUNDS, 2, rows, 256), BF),
            vm((ROUNDS, rows, 128), BF),
            vm((ROUNDS, rows, 128), BF),
            vm((rows, 128), F32),
            vm((rows, 128), F32),
            vm((8, 48, 128), F32),
            vm((8, 48, 128), BF),
            vm((rows, 64), BF),
            vm((rows, 512), BF),
            vm((rows, 512), BF),
            vm((2, 256, ld + lf), F32),
            vm((256, ld + lf), F32),
            vm((8, 32, ld + lf), BF),
            vm((8, 32, ld + lf), BF),
            vm((8, 32, ld + lf), BF),
            dma((6,)),
            dma,
            dma((ROUNDS, 7)),
            dma((ROUNDS,)),
            dma,
            dma((2, 6)),
            dma((2,)),
            dma((2, 5)),
            dma((2,)),
            dma((2,)),
            dma,
            dma,
            dma,
            dma,
            dma,
            dma((ROUNDS,)),
            dma,
            dma((ROUNDS,)),
            dma,
            dma,
            dma,
            dma((2,)),
            dma,
            dma((2, 2)),
            dma,
            dma((2, 2)),
        ],
        compiler_params=pltpu.CompilerParams(
            collective_id=0, has_side_effects=True, vmem_limit_bytes=58 << 20
        ),
    )(bti, ranks, tokens, w, down, up, cot)
    kept = [pltpu.with_memory_space_constraint(r, pltpu.VMEM) for r in (hid, gt, gd, gu)]
    hid, gt, gd, gu = pl.pallas_call(
        store,
        out_shape=tuple(jax.ShapeDtypeStruct(r.shape, r.dtype) for r in kept),
        in_specs=[out] * 4,
        out_specs=[hbm] * 4,
        scratch_shapes=[dma((4,))],
        compiler_params=pltpu.CompilerParams(vmem_limit_bytes=1 << 20),
    )(*kept)
    return hid, gt, gd.reshape(4, 64, ld), gu.reshape(4, 64, lf)


def solution(mesh):
    return jax.shard_map(
        shards,
        mesh=mesh,
        in_specs=(
            P(("fsdp", "dp"), "tenant"),
            P(("fsdp", "dp")),
            P(),
            P(("fsdp", "dp"), "tenant"),
            P("tenant", None, None),
            P("tenant", None, None),
            P(("fsdp", "dp"), "tenant"),
        ),
        out_specs=(
            P(("fsdp", "dp"), "tenant"),
            P(("fsdp", "dp"), "tenant"),
            P("dp", None, "tenant"),
            P("dp", None, "tenant"),
        ),
        check_vma=False,
    )
```

```python
import jax
import jax.numpy as jnp
from jax import lax
from jax.experimental import pallas as pl
from jax.experimental.pallas import tpu as pltpu
from jax.sharding import PartitionSpec as P

MESH = pl.DeviceIdType.MESH
BF = jnp.bfloat16
F32 = jnp.float32
BLOCK = 64
ALPHA = 32.0
ROUNDS = 5
SUB = 64


def dot(a, b, ca, cb):
    return lax.dot_general(a, b, (((ca,), (cb,)), ((), ())), preferred_element_type=F32)


def kernel(
    bti,
    ranks,
    tok_h,
    w_h,
    d_h,
    u_h,
    cot_h,
    hid_out,
    gt_out,
    gd_out,
    gu_out,
    tok,
    dq,
    cot,
    wall,
    tokq,
    dmine,
    uall,
    dall,
    ux,
    dx,
    hacc,
    gopp,
    gn,
    gf,
    gor,
    gown,
    grecv,
    gzs,
    gzr,
    gcomp,
    cp2,
    brecv,
    agx,
    agj,
    agexp,
    aexp,
    gpart,
    gpr,
    rss,
    rsr,
    agg,
    lsem,
    wss,
    wrs,
    prs,
    tss,
    trs,
    uss,
    urs,
    upss,
    uprs,
    bss,
    brs,
    ass_,
    ars,
    gos,
    gors,
    gns,
    grs,
    zss,
    zrs,
    xss,
    xrs,
    rss_s,
    rss_r,
    ags_s,
    ags_r,
):
    f = lax.axis_index("fsdp")
    j = lax.axis_index("tenant")
    c = lax.axis_index("dp")
    rows = cot.shape[0]
    half = rows // 2
    lf, ld = cot.shape[1], tok.shape[1]

    def ring(i):
        flip = 1 - 2 * lax.rem(i, 2)
        right, left, opp = lax.rem(i + 2, 8), lax.rem(i + 6, 8), lax.rem(i + 4, 8)
        return dict(
            Z=i + flip,
            R=right,
            L=left,
            O=opp,
            RZ=right + flip,
            LZ=left + flip,
            OZ=opp + flip,
        )

    fn, tn = ring(f), ring(j)
    y, zh = j // 2, lax.rem(j, 2)
    partner = {"dp": 1 - c}

    def rc(src, dst, ss, rs, dev):
        return pltpu.make_async_remote_copy(
            src_ref=src, dst_ref=dst, send_sem=ss, recv_sem=rs, device_id=dev, device_id_type=MESH
        )

    def each(lo, hi, body):
        def step(k, carry):
            body(k)
            return carry

        lax.fori_loop(lo, hi, step, 0)

    def go(src, dst, ss, rs, dev):
        rc(src, dst, ss, rs, dev).start()

    def gone(ref, ss):
        rc(ref, ref, ss, ss, partner).wait_send()

    def got(dst, rs):
        rc(dst, dst, rs, rs, partner).wait_recv()

    barrier = pltpu.get_barrier_semaphore()
    for k in range(1, 8):
        pl.semaphore_signal(barrier, 1, device_id={"fsdp": lax.rem(f + k, 8)}, device_id_type=MESH)
        pl.semaphore_signal(
            barrier, 1, device_id={"tenant": lax.rem(j + k, 8)}, device_id_type=MESH
        )
    pl.semaphore_signal(barrier, 1, device_id=partner, device_id_type=MESH)
    pl.semaphore_signal(
        barrier, 1, device_id={"fsdp": fn["Z"], "tenant": tn["Z"]}, device_id_type=MESH
    )

    def slot(q, fi, ci):
        return wall.at[q, pl.ds((2 * fi + ci) * SUB, SUB)]

    def part(q, fi, ci, h):
        return wall.at[q, pl.ds((2 * fi + ci) * SUB + h * (SUB // 2), SUB // 2)]

    wloc = pltpu.make_async_copy(w_h, wall.at[:, pl.ds((2 * f + c) * SUB, SUB)], lsem.at[0])
    ucol = pl.ds(pl.multiple_of(j * lf, 128), lf)
    dcol = pl.ds(pl.multiple_of(j * ld, 128), ld)
    kloc = pltpu.make_async_copy(tok_h, tok, lsem.at[1])
    mloc = pltpu.make_async_copy(d_h, dmine, lsem.at[2])
    uloc = pltpu.make_async_copy(u_h.at[:, ucol], uall.at[j], lsem.at[3])
    dloc = pltpu.make_async_copy(d_h.at[:, dcol], dall.at[j], lsem.at[4])
    cloc = pltpu.make_async_copy(cot_h, cot, lsem.at[5])
    for d in [wloc, kloc, mloc, uloc, dloc, cloc]:
        d.start()

    def fs(i):
        return {"fsdp": fn[i]}

    def w_send(q, name, rsem, to, src=None):
        ref = slot(q, fn[name] if name else f, c) if src is None else src
        go(ref, ref, wss, rsem, to)

    def w_got(q, k, ref):
        got(ref, wrs.at[q, k])

    def w_A(q):
        w_send(q, None, wrs.at[q, 1], fs("R"))
        w_send(q, None, wrs.at[q, 2], fs("L"))
        w_send(q, None, wrs.at[q, 0], fs("Z"))
        w_send(q, None, prs.at[q], partner)

    def w_B(q):
        w_got(q, 0, slot(q, fn["Z"], c))
        w_send(q, "Z", wrs.at[q, 3], fs("R"))
        w_send(q, "Z", wrs.at[q, 4], fs("L"))
        w_send(q, "Z", prs.at[q], partner)

    def w_CD(q, left, right, kl, kr, ko):
        w_got(q, kl, slot(q, fn[left], c))
        w_send(q, left, wrs.at[q, ko], fs("R"), part(q, fn[left], c, 0))
        w_send(q, left, prs.at[q], partner)
        w_got(q, kr, slot(q, fn[right], c))
        w_send(q, right, wrs.at[q, ko], fs("L"), part(q, fn[right], c, 1))
        w_send(q, right, prs.at[q], partner)

    def w_C(q):
        w_CD(q, "L", "R", 1, 2, 5)

    def w_D(q):
        w_CD(q, "LZ", "RZ", 3, 4, 6)

    def w_E(q):
        for name, k in (("O", 5), ("OZ", 6)):
            w_got(q, k, slot(q, fn[name], c))
            w_send(q, name, prs.at[q], partner)

    def x_C(q):
        for name, k, h, kz, to in (("L", 1, 0, 3, "R"), ("R", 2, 1, 4, "L")):
            w_got(q, k, slot(q, fn[name], c))
            w_send(q, name, wrs.at[q, 5], fs(to), part(q, fn[name], c, h))
            w_send(q, name, wrs.at[q, kz], fs("Z"))
            w_send(q, name, prs.at[q], partner)

    def x_D(q):
        for name, k in (("Z", 0), ("LZ", 3), ("RZ", 4)):
            w_got(q, k, slot(q, fn[name], c))
            w_send(q, name, prs.at[q], partner)

    def x_O(q):
        w_got(q, 5, slot(q, fn["O"], c))
        w_send(q, "O", wrs.at[q, 6], fs("Z"))
        w_send(q, "O", prs.at[q], partner)

    def x_E(q):
        w_got(q, 6, slot(q, fn["OZ"], c))
        w_send(q, "OZ", prs.at[q], partner)

    def w_P(q):
        got(wall.at[q, pl.ds(0, 8 * SUB)], prs.at[q])

    def te(i):
        return {"tenant": tn[i]}

    tq = (pl.ds(0, 3), pl.ds(3, 2))

    def t_ref(ji, p, h=None):
        rows_ = slice(None) if h is None else pl.ds(h * half, half)
        return tokq.at[ji, tq[p], rows_]

    def t_send(p, ji, k, to, h=None):
        ref = t_ref(ji, p, h)
        go(ref, ref, tss, trs.at[p, k], to)

    def pieces(v):
        return [
            jnp.concatenate([v[:, SUB * q : SUB * q + SUB], v[:, 320 + SUB * q : 384 + SUB * q]], axis=1)
            for q in range(ROUNDS)
        ]

    def t_make():
        kloc.wait()
        for q, v in enumerate(pieces(tok[...])):
            tokq[j, q] = v

    def dq_make():
        mloc.wait()
        for i in range(8):
            for q, v in enumerate(pieces(dmine[:, ld * i : ld * i + ld])):
                dq[q, :, 128 * i : 128 * i + 128] = v

    def t_A(p):
        t_send(p, j, 1, te("R"))
        t_send(p, j, 2, te("L"))

    def t_Z(p):
        t_send(p, j, 0, te("Z"))

    def t_B(p):
        got(t_ref(tn["Z"], p), trs.at[p, 0])
        t_send(p, tn["Z"], 3, te("R"))
        t_send(p, tn["Z"], 4, te("L"))

    def t_CD(p, left, right, kl, kr):
        got(t_ref(tn[left], p), trs.at[p, kl])
        t_send(p, tn[left], 5, te("R"), 0)
        got(t_ref(tn[right], p), trs.at[p, kr])
        t_send(p, tn[right], 5, te("L"), 1)

    def t_C(p):
        t_CD(p, "L", "R", 1, 2)

    def t_D(p):
        t_CD(p, "LZ", "RZ", 3, 4)

    def t_E(p):
        got(tokq.at[pl.ds(0, 2), tq[p]], trs.at[p, 5])

    def adapter(src, width, all_, relay, s):
        def own(ji, ci):
            return all_.at[ji, pl.ds(ci * 32, 32)]

        def out(ji):
            return src.at[pl.ds(c * 32, 32), pl.ds(pl.multiple_of(ji * width, 128), width)]

        return own, out, relay, s

    kinds = (adapter(d_h, ld, dall, dx, 0), adapter(u_h, lf, uall, ux, 1))
    cross = {"fsdp": fn["Z"], "tenant": tn["Z"]}

    def at_y(r):
        return lax.rem(y + r, 4)

    def u_cross():
        for own, out, relay, s in kinds:
            for r in (1, 2, 3, 0):
                dst = own(j, c) if r == 0 else relay.at[r]
                go(out(2 * at_y(r) + 1 - zh), dst, uss.at[s], urs.at[s, r], cross)

    def u_own():
        for own, out, relay, s in kinds:
            for r in range(1, 4):
                to = 2 * at_y(r) + zh
                go(out(to), own(j, c), uss.at[s], urs.at[s, 0], {"tenant": to})

    def u_fwd():
        for own, out, relay, s in kinds:
            for r in range(1, 4):
                got(relay.at[r], urs.at[s, r])
                to = 2 * at_y(r) + zh
                go(relay.at[r], own(tn["Z"], c), uss.at[s], urs.at[s, 4], {"tenant": to})

    def u_recv(e):
        for (own, out, relay, s), all_ in zip(kinds, (dall, uall)):
            got(all_.at[pl.ds(0, 4 - e), pl.ds(0, 32)], urs.at[s, 4 * e])
            for r in range(e, 4):
                ji = 2 * at_y(4 - r) + (1 - zh if e == 1 or r == 0 else zh)
                go(own(ji, c), own(ji, c), upss.at[s], uprs.at[s], partner)

    def u_from_partner():
        for s, all_ in ((0, dall), (1, uall)):
            got(all_.at[pl.ds(0, 7), pl.ds(0, 32)], uprs.at[s])

    def tenant_is(b, t, shape):
        return jnp.full(shape, bti[b], jnp.int32) == t

    def make_gain():
        shape = (BLOCK, 128)
        slot_ = lax.rem(lax.broadcasted_iota(jnp.int32, shape, 1), 64)
        gains = []
        for t in range(8):
            r = jnp.full(shape, ranks[t], jnp.int32)
            gains.append(jnp.where(slot_ < r, ALPHA / r.astype(F32), 0.0))
        for b in range(6):
            g = jnp.zeros(shape, F32)
            for t in range(8):
                g = jnp.where(tenant_is(b, t, g.shape), gains[t], g)
            gcomp[pl.ds(b * BLOCK, BLOCK), :] = g

    def compact(w, a, all_):
        for h in range(2):
            u = all_[pl.ds(4 * h, 4)].reshape(256, a.shape[1])
            p = dot(a[...], u, 1, 1)
            for b in range(6):
                rs = slice(b * BLOCK, (b + 1) * BLOCK)
                acc = jnp.zeros((BLOCK, BLOCK), F32)
                for t in range(4):
                    acc = jnp.where(
                        tenant_is(b, 4 * h + t, acc.shape), p[rs, 64 * t : 64 * t + 64], acc
                    )
                at = (rs, slice(64 * w, 64 * w + 64))
                cp2[at] = acc if h == 0 else cp2[at] + acc

    def b_desc(k):
        to = lax.rem(j + k, 8)
        return rc(cp2.at[pl.ds(to * 48, 48)], brecv.at[k], bss, brs, {"tenant": to})

    def b_sum():
        at = pl.ds(pl.multiple_of(j * 48, 16), 48)
        s = cp2[at, :]
        got(brecv.at[pl.ds(1, 7)], brs)
        for k in range(1, 8):
            s = s + brecv[k]
        agx[j] = (s * gcomp[at, :]).astype(BF)

    def ag_desc(k):
        return rc(agx.at[j], agx.at[j], ass_, ars, {"tenant": lax.rem(j + k, 8)})

    def ag_use():
        got(agx.at[pl.ds(0, 7)], ars)
        both = jnp.concatenate([agx[k] for k in range(8)], axis=0).astype(F32)
        for w, dst in ((0, agexp), (1, aexp)):
            for b in range(6):
                rs = slice(b * BLOCK, (b + 1) * BLOCK)
                v = both[rs, 64 * w : 64 * w + 64]
                zero = jnp.zeros_like(v)
                if w == 0:
                    agj[rs, :] = jnp.where(tenant_is(b, j, v.shape), v, zero).astype(BF)
                for t in range(0, 8, 2):
                    pair = jnp.concatenate(
                        [jnp.where(tenant_is(b, t + e, v.shape), v, zero) for e in range(2)], axis=1
                    )
                    dst[rs, 64 * t : 64 * t + 128] = pair.astype(BF)

    def lhs(q):
        return jnp.concatenate([tokq[i, q] for i in range(8)], axis=1)

    def grad_down_part():
        p = dot(agexp[...], tok[...], 0, 0)
        gpart[0, :, 0:ld] = p[:256]
        gpart[1, :, 0:ld] = p[256:]

    def grad_up_part(lo, hi):
        def body(n):
            at = pl.ds(pl.multiple_of(n * 256, 256), 256)
            to = pl.ds(pl.multiple_of(ld + n * 256, 128), 256)
            p = dot(aexp[...], cot[:, at], 0, 0)
            gpart[0, :, to] = p[:256]
            gpart[1, :, to] = p[256:]

        each(lo, hi, body)

    fx, fz = f // 2, lax.rem(f, 2)
    cols = (pl.ds(0, 1152), pl.ds(1152, 1280))

    def gx(p):
        go(gpart.at[1 - c, :, cols[p]], gpr.at[:, cols[p]], xss, xrs.at[p], partner)

    def chunk(k, p):
        at = pl.ds(pl.multiple_of(k * 32, 32), 32)
        return gpart[c, at, cols[p]] + gpr[at, cols[p]]

    def rs_z(p):
        got(gpr.at[:, cols[p]], xrs.at[p])

        def body(k):
            rss[k, :, cols[p]] = chunk(2 * k + 1 - fz, p).astype(BF)

        each(0, 4, body)
        at = (pl.ds(0, 4), slice(None), cols[p])
        go(rss.at[at], rsr.at[at], rss_s, rss_r.at[p, 0], fs("Z"))

    def fx_to(r):
        return {"fsdp": lax.rem(f + 2 * r, 8)}

    def rs_x(p):
        got(rsr.at[pl.ds(0, 4), :, cols[p]], rss_r.at[p, 0])
        for r in range(1, 4):
            k = lax.rem(fx + r, 4)
            rss[3 + r, :, cols[p]] = (
                chunk(2 * k + fz, p) + rsr[k, :, cols[p]].astype(F32)
            ).astype(BF)
            at = (3 + r, slice(None), cols[p])
            go(rss.at[at], rsr.at[at], rss_s, rss_r.at[p, 1], fx_to(r))

    def to_x(ref, p, k):
        go(ref, ref, ags_s, ags_r.at[p, k], fs("R"))
        go(ref, ref, ags_s, ags_r.at[p, k + 1], fs("L"))

    def on_x(p, left, right, k):
        for name, e, to in ((left, 0, "R"), (right, 1, "L")):
            got(agg.at[fn[name], :, cols[p]], ags_r.at[p, k + e])
            ref = agg.at[fn[name], pl.ds(16 * e, 16), cols[p]]
            go(ref, ref, ags_s, ags_r.at[p, 5], fs(to))

    def rs_sum(p):
        s = chunk(f, p) + rsr[fx, :, cols[p]].astype(F32)
        got(rsr.at[pl.ds(4, 3), :, cols[p]], rss_r.at[p, 1])
        for r in range(1, 4):
            s = s + rsr[3 + r, :, cols[p]].astype(F32)
        agg[f, :, cols[p]] = s.astype(BF)
        ref = agg.at[f, :, cols[p]]
        go(ref, ref, ags_s, ags_r.at[p, 2], fs("Z"))
        to_x(ref, p, 0)

    def ag_x(p):
        ref = agg.at[fn["Z"], :, cols[p]]
        got(ref, ags_r.at[p, 2])
        to_x(ref, p, 3)

    def ag_o(p):
        on_x(p, "L", "R", 0)

    def ag_oz(p):
        on_x(p, "LZ", "RZ", 3)

    def grads_out(p):
        got(agg.at[pl.ds(0, 2), :, cols[p]], ags_r.at[p, 5])

        def body(k):
            at = pl.ds(pl.multiple_of(k * 32, 32), 32)
            v = agg[k, :, cols[p]].astype(F32)
            if p == 0:
                gd_out[at, :] = v[:, :ld]
                gu_out[at, 0:512] = v[:, ld:]
            else:
                gu_out[at, 512:] = v

        each(0, 8, body)

    top, bottom = pl.ds(0, half), pl.ds(half, half)

    def g_near(q, e, at):
        go(gn.at[q, e, at], grecv.at[q, e, at], gns, grs.at[q], te("RL"[e]))

    def compute_g(q):
        def body(k):
            i = lax.rem(y + 2 + 3 * k, 4)
            at = pl.ds(pl.multiple_of(i * 256, 256), 256)
            p = dot(cot[...], wall[q, at, :], 1, 1) + dot(agj[...], dq[q, :, at], 1, 0)

            @pl.when(k == 0)
            def _():
                gopp[q] = p.astype(BF)
                go(gopp.at[q, top], gor.at[q, 0], gos, gors.at[q], te("R"))
                go(gopp.at[q, bottom], gor.at[q, 1], gos, gors.at[q], te("L"))

            @pl.when(k == 1)
            def _():
                gf[q, 0] = p[:half]
                gn[q, 0, half:] = p[half:].astype(BF)
                g_near(q, 0, bottom)

            @pl.when(k == 2)
            def _():
                gown[q] = p

            @pl.when(k == 3)
            def _():
                gf[q, 1] = p[half:]
                gn[q, 1, :half] = p[:half].astype(BF)
                g_near(q, 1, top)

        each(0, 4, body)

    def g_acc(q):
        got(gor.at[q], gors.at[q])
        for e, at in enumerate((top, bottom)):
            gn[q, e, at] = (gf[q, e] + gor[q, e].astype(F32)).astype(BF)
            g_near(q, e, at)

    def compute_h(q):
        def body(n):
            at = pl.ds(pl.multiple_of(n * 256, 256), 256)
            p = dot(lhs(q), wall[q, :, at], 1, 0)
            if q == 0:
                hacc[:, at] = p
            elif q < ROUNDS - 1:
                hacc[:, at] += p
            else:
                u = uall[:, :, at].reshape(512, 256)
                hid_out[:, at] = (hacc[:, at] + p + dot(aexp[...], u, 1, 0)).astype(BF)

        each(0, lf // 256, body)

    def g_sum(q):
        got(grecv.at[q], grs.at[q])
        mine = pl.ds(pl.multiple_of(zh * 128, 128), 128)
        other = pl.ds(pl.multiple_of(128 - zh * 128, 128), 128)

        def total(at):
            s = gown[q, :, at]
            for k in range(2):
                s = s + grecv[q, k, :, at].astype(F32)
            return s

        gzs[q] = total(other).astype(BF)
        go(gzs.at[q], gzr.at[q], zss, zrs, te("Z"))
        gown[q, :, mine] = total(mine)

    def gt_final():
        mine = pl.ds(pl.multiple_of(zh * 128, 128), 128)
        got(gzr, zrs)

        def body(b):
            at = pl.ds(pl.multiple_of(b * BLOCK, BLOCK), BLOCK)
            s = [gown[q, at, mine] + gzr[q, at, :].astype(F32) for q in range(ROUNDS)]
            row = jnp.concatenate([v[:, :64] for v in s] + [v[:, 64:] for v in s], axis=1)
            gt_out[at, :] = row.astype(BF)

        each(0, 6, body)

    pl.semaphore_wait(barrier, 16)
    u_cross()
    u_own()
    wloc.wait()
    w_A(0)
    w_A(1)
    t_make()
    t_A(0)
    dq_make()
    make_gain()
    w_B(0)
    w_C(0)
    w_A(2)
    u_fwd()
    t_A(1)
    t_Z(0)
    t_Z(1)
    t_C(0)
    u_recv(0)
    w_D(0)
    w_B(1)
    w_C(1)
    w_A(3)
    u_recv(1)
    uloc.wait()
    dloc.wait()
    cloc.wait()
    u_from_partner()
    compact(0, cot, uall)
    compact(1, tok, dall)
    each(1, 8, lambda k: b_desc(k).start())
    t_C(1)
    t_B(1)
    w_E(0)
    b_sum()
    each(1, 8, lambda k: ag_desc(k).start())
    t_B(0)
    w_A(4)
    w_D(1)
    x_C(2)
    ag_use()
    w_P(0)
    compute_g(0)
    w_B(3)
    w_C(3)
    grad_down_part()
    grad_up_part(0, 2)
    gx(0)
    grad_up_part(2, 7)
    gx(1)
    w_E(1)
    w_B(4)
    x_O(2)
    rs_z(0)
    t_D(0)
    t_D(1)
    w_P(1)
    compute_g(1)
    g_acc(0)
    x_D(2)
    w_D(3)
    w_C(4)
    rs_z(1)
    x_E(2)
    w_P(2)
    compute_g(2)
    g_acc(1)
    w_D(4)
    t_E(0)
    t_E(1)
    compute_h(0)
    w_E(3)
    rs_x(0)
    w_P(3)
    compute_g(3)
    g_acc(2)
    rs_x(1)
    g_sum(0)
    w_E(4)
    compute_h(1)
    rs_sum(0)
    w_P(4)
    compute_g(4)
    g_acc(3)
    rs_sum(1)
    g_sum(1)
    compute_h(2)
    ag_o(0)
    g_sum(2)
    ag_x(0)
    g_acc(4)
    ag_x(1)
    compute_h(3)
    ag_o(1)
    g_sum(3)
    g_sum(4)
    ag_oz(0)
    ag_oz(1)
    compute_h(4)
    grads_out(0)
    grads_out(1)
    gt_final()

    gone(wall.at[:, pl.ds(0, 15 * SUB)], wss)
    gone(tokq.at[pl.ds(0, 7)], tss)
    for s, all_ in ((0, dall), (1, uall)):
        gone(all_.at[pl.ds(0, 5)], uss.at[s])
        gone(all_.at[pl.ds(0, 7), pl.ds(0, 32)], upss.at[s])
    gone(brecv.at[pl.ds(0, 7)], bss)
    gone(agx.at[pl.ds(0, 7)], ass_)
    gone(gopp, gos)
    gone(gn, gns)
    gone(gzs, zss)
    gone(gpr, xss)
    gone(rss.at[pl.ds(0, 7)], rss_s)
    gone(agg.at[pl.ds(0, 7)], ags_s)


def store(*refs):
    sems = refs[8]
    copies = [pltpu.make_async_copy(refs[i], refs[4 + i], sems.at[i]) for i in range(4)]
    for d in copies:
        d.start()
    for d in copies:
        d.wait()


def shards(tokens, bti, ranks, w, down, up, cot):
    rows, ld = tokens.shape
    lf = cot.shape[1]
    up = up.reshape(up.shape[1:])
    w = w.reshape(ROUNDS, SUB, lf)
    down = down.reshape(down.shape[1:])
    dma = pltpu.SemaphoreType.DMA
    vm = pltpu.VMEM
    smem = pl.BlockSpec(memory_space=pltpu.SMEM)
    hbm = pl.BlockSpec(memory_space=pl.ANY)
    out = pl.BlockSpec(memory_space=pltpu.VMEM)
    half = rows // 2
    hid, gt, gd, gu = pl.pallas_call(
        kernel,
        out_shape=(
            pltpu.VMEM((rows, lf), BF),
            pltpu.VMEM((rows, ld), BF),
            pltpu.VMEM((256, ld), F32),
            pltpu.VMEM((256, lf), F32),
        ),
        in_specs=[smem, smem, hbm, hbm, hbm, hbm, hbm],
        out_specs=(out, out, out, out),
        scratch_shapes=[
            vm((rows, ld), BF),
            vm((ROUNDS, 64, 1024), BF),
            vm((rows, lf), BF),
            vm((ROUNDS, 1024, lf), BF),
            vm((8, ROUNDS, rows, 128), BF),
            vm((64, 5120), BF),
            vm((8, 64, lf), BF),
            vm((8, 64, ld), BF),
            vm((4, 32, lf), BF),
            vm((4, 32, ld), BF),
            vm((rows, lf), F32),
            vm((ROUNDS, rows, 256), BF),
            vm((ROUNDS, 2, rows, 256), BF),
            vm((ROUNDS, 2, half, 256), F32),
            vm((ROUNDS, 2, half, 256), BF),
            vm((ROUNDS, rows, 256), F32),
            vm((ROUNDS, 2, rows, 256), BF),
            vm((ROUNDS, rows, 128), BF),
            vm((ROUNDS, rows, 128), BF),
            vm((rows, 128), F32),
            vm((rows, 128), F32),
            vm((8, 48, 128), F32),
            vm((8, 48, 128), BF),
            vm((rows, 64), BF),
            vm((rows, 512), BF),
            vm((rows, 512), BF),
            vm((2, 256, ld + lf), F32),
            vm((256, ld + lf), F32),
            vm((8, 32, ld + lf), BF),
            vm((8, 32, ld + lf), BF),
            vm((8, 32, ld + lf), BF),
            dma((6,)),
            dma,
            dma((ROUNDS, 7)),
            dma((ROUNDS,)),
            dma,
            dma((2, 6)),
            dma((2,)),
            dma((2, 5)),
            dma((2,)),
            dma((2,)),
            dma,
            dma,
            dma,
            dma,
            dma,
            dma((ROUNDS,)),
            dma,
            dma((ROUNDS,)),
            dma,
            dma,
            dma,
            dma((2,)),
            dma,
            dma((2, 2)),
            dma,
            dma((2, 6)),
        ],
        compiler_params=pltpu.CompilerParams(
            collective_id=0, has_side_effects=True, vmem_limit_bytes=58 << 20
        ),
    )(bti, ranks, tokens, w, down, up, cot)
    kept = [pltpu.with_memory_space_constraint(r, pltpu.VMEM) for r in (hid, gt, gd, gu)]
    hid, gt, gd, gu = pl.pallas_call(
        store,
        out_shape=tuple(jax.ShapeDtypeStruct(r.shape, r.dtype) for r in kept),
        in_specs=[out] * 4,
        out_specs=[hbm] * 4,
        scratch_shapes=[dma((4,))],
        compiler_params=pltpu.CompilerParams(vmem_limit_bytes=1 << 20),
    )(*kept)
    return hid, gt, gd.reshape(4, 64, ld), gu.reshape(4, 64, lf)


def solution(mesh):
    return jax.shard_map(
        shards,
        mesh=mesh,
        in_specs=(
            P(("fsdp", "dp"), "tenant"),
            P(("fsdp", "dp")),
            P(),
            P(("fsdp", "dp"), "tenant"),
            P("tenant", None, None),
            P("tenant", None, None),
            P(("fsdp", "dp"), "tenant"),
        ),
        out_specs=(
            P(("fsdp", "dp"), "tenant"),
            P(("fsdp", "dp"), "tenant"),
            P("dp", None, "tenant"),
            P("dp", None, "tenant"),
        ),
        check_vma=False,
    )
```

```python
import jax
import jax.numpy as jnp
from jax import lax
from jax.experimental import pallas as pl
from jax.experimental.pallas import tpu as pltpu
from jax.sharding import PartitionSpec as P

MESH = pl.DeviceIdType.MESH
BF = jnp.bfloat16
F32 = jnp.float32
BLOCK = 64
ALPHA = 32.0
ROUNDS = 5
SUB = 64


def dot(a, b, ca, cb):
    return lax.dot_general(a, b, (((ca,), (cb,)), ((), ())), preferred_element_type=F32)


def kernel(
    bti,
    ranks,
    tok_h,
    w_h,
    d_h,
    u_h,
    cot_h,
    hid_out,
    gt_out,
    gd_out,
    gu_out,
    tok,
    dq,
    cot,
    wall,
    tokq,
    dmine,
    uall,
    dall,
    ux,
    dx,
    hacc,
    gopp,
    gn,
    gf,
    gor,
    gown,
    grecv,
    gzs,
    gzr,
    gcomp,
    cp2,
    brecv,
    agx,
    agj,
    agexp,
    aexp,
    gpart,
    gpr,
    rss,
    rsr,
    agg,
    lsem,
    wss,
    wrs,
    prs,
    tss,
    trs,
    uss,
    urs,
    upss,
    uprs,
    bss,
    brs,
    ass_,
    ars,
    gos,
    gors,
    gns,
    grs,
    zss,
    zrs,
    xss,
    xrs,
    rss_s,
    rss_r,
    ags_s,
    ags_r,
):
    f = lax.axis_index("fsdp")
    j = lax.axis_index("tenant")
    c = lax.axis_index("dp")
    rows = cot.shape[0]
    half = rows // 2
    lf, ld = cot.shape[1], tok.shape[1]

    def ring(i):
        flip = 1 - 2 * lax.rem(i, 2)
        right, left, opp = lax.rem(i + 2, 8), lax.rem(i + 6, 8), lax.rem(i + 4, 8)
        return dict(
            Z=i + flip,
            R=right,
            L=left,
            O=opp,
            RZ=right + flip,
            LZ=left + flip,
            OZ=opp + flip,
        )

    fn, tn = ring(f), ring(j)
    y, zh = j // 2, lax.rem(j, 2)
    partner = {"dp": 1 - c}

    def rc(src, dst, ss, rs, dev):
        return pltpu.make_async_remote_copy(
            src_ref=src, dst_ref=dst, send_sem=ss, recv_sem=rs, device_id=dev, device_id_type=MESH
        )

    def each(lo, hi, body):
        def step(k, carry):
            body(k)
            return carry

        lax.fori_loop(lo, hi, step, 0)

    def go(src, dst, ss, rs, dev):
        rc(src, dst, ss, rs, dev).start()

    def gone(ref, ss):
        rc(ref, ref, ss, ss, partner).wait_send()

    def got(dst, rs):
        rc(dst, dst, rs, rs, partner).wait_recv()

    barrier = pltpu.get_barrier_semaphore()
    for k in range(1, 8):
        pl.semaphore_signal(barrier, 1, device_id={"fsdp": lax.rem(f + k, 8)}, device_id_type=MESH)
        pl.semaphore_signal(
            barrier, 1, device_id={"tenant": lax.rem(j + k, 8)}, device_id_type=MESH
        )
    pl.semaphore_signal(barrier, 1, device_id=partner, device_id_type=MESH)
    pl.semaphore_signal(
        barrier, 1, device_id={"fsdp": fn["Z"], "tenant": tn["Z"]}, device_id_type=MESH
    )

    def slot(q, fi, ci):
        return wall.at[q, pl.ds((2 * fi + ci) * SUB, SUB)]

    def part(q, fi, ci, h):
        return wall.at[q, pl.ds((2 * fi + ci) * SUB + h * (SUB // 2), SUB // 2)]

    wloc = pltpu.make_async_copy(w_h, wall.at[:, pl.ds((2 * f + c) * SUB, SUB)], lsem.at[0])
    ucol = pl.ds(pl.multiple_of(j * lf, 128), lf)
    dcol = pl.ds(pl.multiple_of(j * ld, 128), ld)
    kloc = pltpu.make_async_copy(tok_h, tok, lsem.at[1])
    mloc = pltpu.make_async_copy(d_h, dmine, lsem.at[2])
    uloc = pltpu.make_async_copy(u_h.at[:, ucol], uall.at[j], lsem.at[3])
    dloc = pltpu.make_async_copy(d_h.at[:, dcol], dall.at[j], lsem.at[4])
    cloc = pltpu.make_async_copy(cot_h, cot, lsem.at[5])
    for d in [wloc, kloc, mloc, uloc, dloc, cloc]:
        d.start()

    def fs(i):
        return {"fsdp": fn[i]}

    def w_send(q, name, rsem, to, src=None):
        ref = slot(q, fn[name] if name else f, c) if src is None else src
        go(ref, ref, wss, rsem, to)

    def w_got(q, k, ref):
        got(ref, wrs.at[q, k])

    def w_A(q):
        w_send(q, None, wrs.at[q, 1], fs("R"))
        w_send(q, None, wrs.at[q, 2], fs("L"))
        w_send(q, None, wrs.at[q, 0], fs("Z"))
        w_send(q, None, prs.at[q], partner)

    def w_B(q):
        w_got(q, 0, slot(q, fn["Z"], c))
        w_send(q, "Z", wrs.at[q, 3], fs("R"))
        w_send(q, "Z", wrs.at[q, 4], fs("L"))
        w_send(q, "Z", prs.at[q], partner)

    def w_CD(q, left, right, kl, kr, ko):
        w_got(q, kl, slot(q, fn[left], c))
        w_send(q, left, wrs.at[q, ko], fs("R"), part(q, fn[left], c, 0))
        w_send(q, left, prs.at[q], partner)
        w_got(q, kr, slot(q, fn[right], c))
        w_send(q, right, wrs.at[q, ko], fs("L"), part(q, fn[right], c, 1))
        w_send(q, right, prs.at[q], partner)

    def w_C(q):
        w_CD(q, "L", "R", 1, 2, 5)

    def w_D(q):
        w_CD(q, "LZ", "RZ", 3, 4, 6)

    def w_E(q):
        for name, k in (("O", 5), ("OZ", 6)):
            w_got(q, k, slot(q, fn[name], c))
            w_send(q, name, prs.at[q], partner)

    def x_C(q):
        for name, k, h, kz, to in (("L", 1, 0, 3, "R"), ("R", 2, 1, 4, "L")):
            w_got(q, k, slot(q, fn[name], c))
            w_send(q, name, wrs.at[q, 5], fs(to), part(q, fn[name], c, h))
            w_send(q, name, wrs.at[q, kz], fs("Z"))
            w_send(q, name, prs.at[q], partner)

    def x_D(q):
        for name, k in (("Z", 0), ("LZ", 3), ("RZ", 4)):
            w_got(q, k, slot(q, fn[name], c))
            w_send(q, name, prs.at[q], partner)

    def x_O(q):
        w_got(q, 5, slot(q, fn["O"], c))
        w_send(q, "O", wrs.at[q, 6], fs("Z"))
        w_send(q, "O", prs.at[q], partner)

    def x_E(q):
        w_got(q, 6, slot(q, fn["OZ"], c))
        w_send(q, "OZ", prs.at[q], partner)

    def w_P(q):
        got(wall.at[q, pl.ds(0, 8 * SUB)], prs.at[q])

    def te(i):
        return {"tenant": tn[i]}

    tq = (pl.ds(0, 3), pl.ds(3, 2))

    def t_ref(ji, p, h=None):
        rows_ = slice(None) if h is None else pl.ds(h * half, half)
        return tokq.at[ji, tq[p], rows_]

    def t_send(p, ji, k, to, h=None):
        ref = t_ref(ji, p, h)
        go(ref, ref, tss, trs.at[p, k], to)

    def pieces(v):
        return [
            jnp.concatenate([v[:, SUB * q : SUB * q + SUB], v[:, 320 + SUB * q : 384 + SUB * q]], axis=1)
            for q in range(ROUNDS)
        ]

    def t_make():
        kloc.wait()
        for q, v in enumerate(pieces(tok[...])):
            tokq[j, q] = v

    def dq_make():
        mloc.wait()
        for i in range(8):
            for q, v in enumerate(pieces(dmine[:, ld * i : ld * i + ld])):
                dq[q, :, 128 * i : 128 * i + 128] = v

    def t_A(p):
        t_send(p, j, 1, te("R"))
        t_send(p, j, 2, te("L"))

    def t_Z(p):
        t_send(p, j, 0, te("Z"))

    def t_B(p):
        got(t_ref(tn["Z"], p), trs.at[p, 0])
        t_send(p, tn["Z"], 3, te("R"))
        t_send(p, tn["Z"], 4, te("L"))

    def t_CD(p, left, right, kl, kr):
        got(t_ref(tn[left], p), trs.at[p, kl])
        t_send(p, tn[left], 5, te("R"), 0)
        got(t_ref(tn[right], p), trs.at[p, kr])
        t_send(p, tn[right], 5, te("L"), 1)

    def t_C(p):
        t_CD(p, "L", "R", 1, 2)

    def t_D(p):
        t_CD(p, "LZ", "RZ", 3, 4)

    def t_E(p):
        got(tokq.at[pl.ds(0, 2), tq[p]], trs.at[p, 5])

    def adapter(src, width, all_, relay, s):
        def own(ji, ci):
            return all_.at[ji, pl.ds(ci * 32, 32)]

        def out(ji):
            return src.at[pl.ds(c * 32, 32), pl.ds(pl.multiple_of(ji * width, 128), width)]

        return own, out, relay, s

    kinds = (adapter(d_h, ld, dall, dx, 0), adapter(u_h, lf, uall, ux, 1))
    cross = {"fsdp": fn["Z"], "tenant": tn["Z"]}

    def at_y(r):
        return lax.rem(y + r, 4)

    def u_cross():
        for own, out, relay, s in kinds:
            for r in (1, 2, 3, 0):
                dst = own(j, c) if r == 0 else relay.at[r]
                go(out(2 * at_y(r) + 1 - zh), dst, uss.at[s], urs.at[s, r], cross)

    def u_own():
        for own, out, relay, s in kinds:
            for r in range(1, 4):
                to = 2 * at_y(r) + zh
                go(out(to), own(j, c), uss.at[s], urs.at[s, 0], {"tenant": to})

    def u_fwd():
        for own, out, relay, s in kinds:
            for r in range(1, 4):
                got(relay.at[r], urs.at[s, r])
                to = 2 * at_y(r) + zh
                go(relay.at[r], own(tn["Z"], c), uss.at[s], urs.at[s, 4], {"tenant": to})

    def u_recv(e):
        for (own, out, relay, s), all_ in zip(kinds, (dall, uall)):
            got(all_.at[pl.ds(0, 4 - e), pl.ds(0, 32)], urs.at[s, 4 * e])
            for r in range(e, 4):
                ji = 2 * at_y(4 - r) + (1 - zh if e == 1 or r == 0 else zh)
                go(own(ji, c), own(ji, c), upss.at[s], uprs.at[s], partner)

    def u_from_partner():
        for s, all_ in ((0, dall), (1, uall)):
            got(all_.at[pl.ds(0, 7), pl.ds(0, 32)], uprs.at[s])

    def tenant_is(b, t, shape):
        return jnp.full(shape, bti[b], jnp.int32) == t

    def make_gain():
        shape = (BLOCK, 128)
        slot_ = lax.rem(lax.broadcasted_iota(jnp.int32, shape, 1), 64)
        gains = []
        for t in range(8):
            r = jnp.full(shape, ranks[t], jnp.int32)
            gains.append(jnp.where(slot_ < r, ALPHA / r.astype(F32), 0.0))
        for b in range(6):
            g = jnp.zeros(shape, F32)
            for t in range(8):
                g = jnp.where(tenant_is(b, t, g.shape), gains[t], g)
            gcomp[pl.ds(b * BLOCK, BLOCK), :] = g

    def compact(w, a, all_):
        for h in range(2):
            u = all_[pl.ds(4 * h, 4)].reshape(256, a.shape[1])
            p = dot(a[...], u, 1, 1)
            for b in range(6):
                rs = slice(b * BLOCK, (b + 1) * BLOCK)
                acc = jnp.zeros((BLOCK, BLOCK), F32)
                for t in range(4):
                    acc = jnp.where(
                        tenant_is(b, 4 * h + t, acc.shape), p[rs, 64 * t : 64 * t + 64], acc
                    )
                at = (rs, slice(64 * w, 64 * w + 64))
                cp2[at] = acc if h == 0 else cp2[at] + acc

    def b_desc(k):
        to = lax.rem(j + k, 8)
        return rc(cp2.at[pl.ds(to * 48, 48)], brecv.at[k], bss, brs, {"tenant": to})

    def b_sum():
        at = pl.ds(pl.multiple_of(j * 48, 16), 48)
        s = cp2[at, :]
        got(brecv.at[pl.ds(1, 7)], brs)
        for k in range(1, 8):
            s = s + brecv[k]
        agx[j] = (s * gcomp[at, :]).astype(BF)

    def ag_desc(k):
        return rc(agx.at[j], agx.at[j], ass_, ars, {"tenant": lax.rem(j + k, 8)})

    def ag_use():
        got(agx.at[pl.ds(0, 7)], ars)
        both = jnp.concatenate([agx[k] for k in range(8)], axis=0).astype(F32)
        for w, dst in ((0, agexp), (1, aexp)):
            for b in range(6):
                rs = slice(b * BLOCK, (b + 1) * BLOCK)
                v = both[rs, 64 * w : 64 * w + 64]
                zero = jnp.zeros_like(v)
                if w == 0:
                    agj[rs, :] = jnp.where(tenant_is(b, j, v.shape), v, zero).astype(BF)
                for t in range(0, 8, 2):
                    pair = jnp.concatenate(
                        [jnp.where(tenant_is(b, t + e, v.shape), v, zero) for e in range(2)], axis=1
                    )
                    dst[rs, 64 * t : 64 * t + 128] = pair.astype(BF)

    def lhs(q):
        return jnp.concatenate([tokq[i, q] for i in range(8)], axis=1)

    def grad_down_part():
        p = dot(agexp[...], tok[...], 0, 0)
        gpart[0, :, 0:ld] = p[:256]
        gpart[1, :, 0:ld] = p[256:]

    def grad_up_part(lo, hi):
        def body(n):
            at = pl.ds(pl.multiple_of(n * 256, 256), 256)
            to = pl.ds(pl.multiple_of(ld + n * 256, 128), 256)
            p = dot(aexp[...], cot[:, at], 0, 0)
            gpart[0, :, to] = p[:256]
            gpart[1, :, to] = p[256:]

        each(lo, hi, body)

    fx, fz = f // 2, lax.rem(f, 2)
    cols = (pl.ds(0, 1408), pl.ds(1408, 1024))

    def gx(p):
        go(gpart.at[1 - c, :, cols[p]], gpr.at[:, cols[p]], xss, xrs.at[p], partner)

    def chunk(k, p):
        at = pl.ds(pl.multiple_of(k * 32, 32), 32)
        return gpart[c, at, cols[p]] + gpr[at, cols[p]]

    def rs_z(p):
        got(gpr.at[:, cols[p]], xrs.at[p])

        def body(k):
            rss[k, :, cols[p]] = chunk(2 * k + 1 - fz, p).astype(BF)

        each(0, 4, body)
        at = (pl.ds(0, 4), slice(None), cols[p])
        go(rss.at[at], rsr.at[at], rss_s, rss_r.at[p, 0], fs("Z"))

    def fx_to(r):
        return {"fsdp": lax.rem(f + 2 * r, 8)}

    def rs_x(p):
        got(rsr.at[pl.ds(0, 4), :, cols[p]], rss_r.at[p, 0])
        for r in range(1, 4):
            k = lax.rem(fx + r, 4)
            rss[3 + r, :, cols[p]] = (
                chunk(2 * k + fz, p) + rsr[k, :, cols[p]].astype(F32)
            ).astype(BF)
            at = (3 + r, slice(None), cols[p])
            go(rss.at[at], rsr.at[at], rss_s, rss_r.at[p, 1], fx_to(r))

    def to_x(ref, p, k):
        go(ref, ref, ags_s, ags_r.at[p, k], fs("R"))
        go(ref, ref, ags_s, ags_r.at[p, k + 1], fs("L"))

    def on_x(p, left, right, k):
        for name, e, to in ((left, 0, "R"), (right, 1, "L")):
            got(agg.at[fn[name], :, cols[p]], ags_r.at[p, k + e])
            ref = agg.at[fn[name], pl.ds(16 * e, 16), cols[p]]
            go(ref, ref, ags_s, ags_r.at[p, 5], fs(to))

    def rs_sum(p):
        s = chunk(f, p) + rsr[fx, :, cols[p]].astype(F32)
        got(rsr.at[pl.ds(4, 3), :, cols[p]], rss_r.at[p, 1])
        for r in range(1, 4):
            s = s + rsr[3 + r, :, cols[p]].astype(F32)
        agg[f, :, cols[p]] = s.astype(BF)
        ref = agg.at[f, :, cols[p]]
        go(ref, ref, ags_s, ags_r.at[p, 2], fs("Z"))
        to_x(ref, p, 0)

    def ag_x(p):
        ref = agg.at[fn["Z"], :, cols[p]]
        got(ref, ags_r.at[p, 2])
        to_x(ref, p, 3)

    def ag_o(p):
        on_x(p, "L", "R", 0)

    def ag_oz(p):
        on_x(p, "LZ", "RZ", 3)

    def grads_out(p):
        got(agg.at[pl.ds(0, 2), :, cols[p]], ags_r.at[p, 5])

        def body(k):
            at = pl.ds(pl.multiple_of(k * 32, 32), 32)
            v = agg[k, :, cols[p]].astype(F32)
            if p == 0:
                gd_out[at, :] = v[:, :ld]
                gu_out[at, 0:768] = v[:, ld:]
            else:
                gu_out[at, 768:] = v

        each(0, 8, body)

    top, bottom = pl.ds(0, half), pl.ds(half, half)

    def g_near(q, e, at):
        go(gn.at[q, e, at], grecv.at[q, e, at], gns, grs.at[q], te("RL"[e]))

    def compute_g(q):
        def body(k):
            i = lax.rem(y + 2 + 3 * k, 4)
            at = pl.ds(pl.multiple_of(i * 256, 256), 256)
            p = dot(cot[...], wall[q, at, :], 1, 1) + dot(agj[...], dq[q, :, at], 1, 0)

            @pl.when(k == 0)
            def _():
                gopp[q] = p.astype(BF)
                go(gopp.at[q, top], gor.at[q, 0], gos, gors.at[q], te("R"))
                go(gopp.at[q, bottom], gor.at[q, 1], gos, gors.at[q], te("L"))

            @pl.when(k == 1)
            def _():
                gf[q, 0] = p[:half]
                gn[q, 0, half:] = p[half:].astype(BF)
                g_near(q, 0, bottom)

            @pl.when(k == 2)
            def _():
                gown[q] = p

            @pl.when(k == 3)
            def _():
                gf[q, 1] = p[half:]
                gn[q, 1, :half] = p[:half].astype(BF)
                g_near(q, 1, top)

        each(0, 4, body)

    def g_acc(q):
        got(gor.at[q], gors.at[q])
        for e, at in enumerate((top, bottom)):
            gn[q, e, at] = (gf[q, e] + gor[q, e].astype(F32)).astype(BF)
            g_near(q, e, at)

    def compute_h(q):
        def body(n):
            at = pl.ds(pl.multiple_of(n * 256, 256), 256)
            p = dot(lhs(q), wall[q, :, at], 1, 0)
            if q == 0:
                hacc[:, at] = p
            elif q < ROUNDS - 1:
                hacc[:, at] += p
            else:
                u = uall[:, :, at].reshape(512, 256)
                hid_out[:, at] = (hacc[:, at] + p + dot(aexp[...], u, 1, 0)).astype(BF)

        each(0, lf // 256, body)

    def g_sum(q):
        got(grecv.at[q], grs.at[q])
        mine = pl.ds(pl.multiple_of(zh * 128, 128), 128)
        other = pl.ds(pl.multiple_of(128 - zh * 128, 128), 128)

        def total(at):
            s = gown[q, :, at]
            for k in range(2):
                s = s + grecv[q, k, :, at].astype(F32)
            return s

        gzs[q] = total(other).astype(BF)
        go(gzs.at[q], gzr.at[q], zss, zrs, te("Z"))
        gown[q, :, mine] = total(mine)

    def gt_final():
        mine = pl.ds(pl.multiple_of(zh * 128, 128), 128)
        got(gzr, zrs)

        def body(b):
            at = pl.ds(pl.multiple_of(b * BLOCK, BLOCK), BLOCK)
            s = [gown[q, at, mine] + gzr[q, at, :].astype(F32) for q in range(ROUNDS)]
            row = jnp.concatenate([v[:, :64] for v in s] + [v[:, 64:] for v in s], axis=1)
            gt_out[at, :] = row.astype(BF)

        each(0, 6, body)

    pl.semaphore_wait(barrier, 16)
    u_cross()
    u_own()
    wloc.wait()
    w_A(0)
    w_A(1)
    t_make()
    t_A(0)
    dq_make()
    make_gain()
    w_B(0)
    w_C(0)
    w_A(2)
    u_fwd()
    t_A(1)
    t_Z(0)
    t_Z(1)
    t_C(0)
    u_recv(0)
    w_D(0)
    w_B(1)
    w_C(1)
    w_A(3)
    u_recv(1)
    uloc.wait()
    dloc.wait()
    cloc.wait()
    u_from_partner()
    compact(0, cot, uall)
    compact(1, tok, dall)
    each(1, 8, lambda k: b_desc(k).start())
    t_C(1)
    t_B(1)
    w_E(0)
    b_sum()
    each(1, 8, lambda k: ag_desc(k).start())
    t_B(0)
    w_A(4)
    w_D(1)
    x_C(2)
    ag_use()
    w_P(0)
    compute_g(0)
    w_B(3)
    w_C(3)
    grad_down_part()
    grad_up_part(0, 3)
    gx(0)
    grad_up_part(3, 7)
    gx(1)
    w_E(1)
    w_B(4)
    x_O(2)
    rs_z(0)
    t_D(0)
    t_D(1)
    w_P(1)
    compute_g(1)
    g_acc(0)
    x_D(2)
    w_D(3)
    w_C(4)
    rs_z(1)
    x_E(2)
    w_P(2)
    compute_g(2)
    g_acc(1)
    w_D(4)
    t_E(0)
    t_E(1)
    compute_h(0)
    w_E(3)
    rs_x(0)
    w_P(3)
    compute_g(3)
    g_acc(2)
    rs_x(1)
    g_sum(0)
    w_E(4)
    compute_h(1)
    rs_sum(0)
    w_P(4)
    compute_g(4)
    g_acc(3)
    rs_sum(1)
    g_sum(1)
    compute_h(2)
    ag_o(0)
    g_sum(2)
    ag_x(0)
    g_acc(4)
    ag_x(1)
    compute_h(3)
    ag_o(1)
    g_sum(3)
    g_sum(4)
    ag_oz(0)
    ag_oz(1)
    compute_h(4)
    grads_out(0)
    grads_out(1)
    gt_final()

    gone(wall.at[:, pl.ds(0, 15 * SUB)], wss)
    gone(tokq.at[pl.ds(0, 7)], tss)
    for s, all_ in ((0, dall), (1, uall)):
        gone(all_.at[pl.ds(0, 5)], uss.at[s])
        gone(all_.at[pl.ds(0, 7), pl.ds(0, 32)], upss.at[s])
    gone(brecv.at[pl.ds(0, 7)], bss)
    gone(agx.at[pl.ds(0, 7)], ass_)
    gone(gopp, gos)
    gone(gn, gns)
    gone(gzs, zss)
    gone(gpr, xss)
    gone(rss.at[pl.ds(0, 7)], rss_s)
    gone(agg.at[pl.ds(0, 7)], ags_s)


def store(*refs):
    sems = refs[8]
    copies = [pltpu.make_async_copy(refs[i], refs[4 + i], sems.at[i]) for i in range(4)]
    for d in copies:
        d.start()
    for d in copies:
        d.wait()


def shards(tokens, bti, ranks, w, down, up, cot):
    rows, ld = tokens.shape
    lf = cot.shape[1]
    up = up.reshape(up.shape[1:])
    w = w.reshape(ROUNDS, SUB, lf)
    down = down.reshape(down.shape[1:])
    dma = pltpu.SemaphoreType.DMA
    vm = pltpu.VMEM
    smem = pl.BlockSpec(memory_space=pltpu.SMEM)
    hbm = pl.BlockSpec(memory_space=pl.ANY)
    out = pl.BlockSpec(memory_space=pltpu.VMEM)
    half = rows // 2
    hid, gt, gd, gu = pl.pallas_call(
        kernel,
        out_shape=(
            pltpu.VMEM((rows, lf), BF),
            pltpu.VMEM((rows, ld), BF),
            pltpu.VMEM((256, ld), F32),
            pltpu.VMEM((256, lf), F32),
        ),
        in_specs=[smem, smem, hbm, hbm, hbm, hbm, hbm],
        out_specs=(out, out, out, out),
        scratch_shapes=[
            vm((rows, ld), BF),
            vm((ROUNDS, 64, 1024), BF),
            vm((rows, lf), BF),
            vm((ROUNDS, 1024, lf), BF),
            vm((8, ROUNDS, rows, 128), BF),
            vm((64, 5120), BF),
            vm((8, 64, lf), BF),
            vm((8, 64, ld), BF),
            vm((4, 32, lf), BF),
            vm((4, 32, ld), BF),
            vm((rows, lf), F32),
            vm((ROUNDS, rows, 256), BF),
            vm((ROUNDS, 2, rows, 256), BF),
            vm((ROUNDS, 2, half, 256), F32),
            vm((ROUNDS, 2, half, 256), BF),
            vm((ROUNDS, rows, 256), F32),
            vm((ROUNDS, 2, rows, 256), BF),
            vm((ROUNDS, rows, 128), BF),
            vm((ROUNDS, rows, 128), BF),
            vm((rows, 128), F32),
            vm((rows, 128), F32),
            vm((8, 48, 128), F32),
            vm((8, 48, 128), BF),
            vm((rows, 64), BF),
            vm((rows, 512), BF),
            vm((rows, 512), BF),
            vm((2, 256, ld + lf), F32),
            vm((256, ld + lf), F32),
            vm((8, 32, ld + lf), BF),
            vm((8, 32, ld + lf), BF),
            vm((8, 32, ld + lf), BF),
            dma((6,)),
            dma,
            dma((ROUNDS, 7)),
            dma((ROUNDS,)),
            dma,
            dma((2, 6)),
            dma((2,)),
            dma((2, 5)),
            dma((2,)),
            dma((2,)),
            dma,
            dma,
            dma,
            dma,
            dma,
            dma((ROUNDS,)),
            dma,
            dma((ROUNDS,)),
            dma,
            dma,
            dma,
            dma((2,)),
            dma,
            dma((2, 2)),
            dma,
            dma((2, 6)),
        ],
        compiler_params=pltpu.CompilerParams(
            collective_id=0, has_side_effects=True, vmem_limit_bytes=58 << 20
        ),
    )(bti, ranks, tokens, w, down, up, cot)
    kept = [pltpu.with_memory_space_constraint(r, pltpu.VMEM) for r in (hid, gt, gd, gu)]
    hid, gt, gd, gu = pl.pallas_call(
        store,
        out_shape=tuple(jax.ShapeDtypeStruct(r.shape, r.dtype) for r in kept),
        in_specs=[out] * 4,
        out_specs=[hbm] * 4,
        scratch_shapes=[dma((4,))],
        compiler_params=pltpu.CompilerParams(vmem_limit_bytes=1 << 20),
    )(*kept)
    return hid, gt, gd.reshape(4, 64, ld), gu.reshape(4, 64, lf)


def solution(mesh):
    return jax.shard_map(
        shards,
        mesh=mesh,
        in_specs=(
            P(("fsdp", "dp"), "tenant"),
            P(("fsdp", "dp")),
            P(),
            P(("fsdp", "dp"), "tenant"),
            P("tenant", None, None),
            P("tenant", None, None),
            P(("fsdp", "dp"), "tenant"),
        ),
        out_specs=(
            P(("fsdp", "dp"), "tenant"),
            P(("fsdp", "dp"), "tenant"),
            P("dp", None, "tenant"),
            P("dp", None, "tenant"),
        ),
        check_vma=False,
    )
```

```python
import jax
import jax.numpy as jnp
from jax import lax
from jax.experimental import pallas as pl
from jax.experimental.pallas import tpu as pltpu
from jax.sharding import PartitionSpec as P

MESH = pl.DeviceIdType.MESH
BF = jnp.bfloat16
F32 = jnp.float32
BLOCK = 64
ALPHA = 32.0
ROUNDS = 5
SUB = 64


def dot(a, b, ca, cb):
    return lax.dot_general(a, b, (((ca,), (cb,)), ((), ())), preferred_element_type=F32)


def kernel(
    bti,
    ranks,
    tok_h,
    w_h,
    d_h,
    u_h,
    cot_h,
    hid_out,
    gt_out,
    gd_out,
    gu_out,
    tok,
    dq,
    cot,
    wall,
    tokq,
    dmine,
    uall,
    dall,
    ux,
    dx,
    hacc,
    gopp,
    gn,
    gf,
    gor,
    gown,
    grecv,
    gzs,
    gzr,
    gcomp,
    cp2,
    brecv,
    agx,
    agj,
    agexp,
    aexp,
    gpart,
    gpr,
    rss,
    rsr,
    agg,
    lsem,
    wss,
    wrs,
    prs,
    tss,
    trs,
    uss,
    urs,
    upss,
    uprs,
    bss,
    brs,
    ass_,
    ars,
    gos,
    gors,
    gns,
    grs,
    zss,
    zrs,
    xss,
    xrs,
    rss_s,
    rss_r,
    ags_s,
    ags_r,
):
    f = lax.axis_index("fsdp")
    j = lax.axis_index("tenant")
    c = lax.axis_index("dp")
    rows = cot.shape[0]
    half = rows // 2
    lf, ld = cot.shape[1], tok.shape[1]

    def ring(i):
        flip = 1 - 2 * lax.rem(i, 2)
        right, left, opp = lax.rem(i + 2, 8), lax.rem(i + 6, 8), lax.rem(i + 4, 8)
        return dict(
            Z=i + flip,
            R=right,
            L=left,
            O=opp,
            RZ=right + flip,
            LZ=left + flip,
            OZ=opp + flip,
        )

    fn, tn = ring(f), ring(j)
    y, zh = j // 2, lax.rem(j, 2)
    partner = {"dp": 1 - c}

    def rc(src, dst, ss, rs, dev):
        return pltpu.make_async_remote_copy(
            src_ref=src, dst_ref=dst, send_sem=ss, recv_sem=rs, device_id=dev, device_id_type=MESH
        )

    def each(lo, hi, body):
        def step(k, carry):
            body(k)
            return carry

        lax.fori_loop(lo, hi, step, 0)

    def go(src, dst, ss, rs, dev):
        rc(src, dst, ss, rs, dev).start()

    def gone(ref, ss):
        rc(ref, ref, ss, ss, partner).wait_send()

    def got(dst, rs):
        rc(dst, dst, rs, rs, partner).wait_recv()

    barrier = pltpu.get_barrier_semaphore()
    for k in range(1, 8):
        pl.semaphore_signal(barrier, 1, device_id={"fsdp": lax.rem(f + k, 8)}, device_id_type=MESH)
        pl.semaphore_signal(
            barrier, 1, device_id={"tenant": lax.rem(j + k, 8)}, device_id_type=MESH
        )
    pl.semaphore_signal(barrier, 1, device_id=partner, device_id_type=MESH)
    pl.semaphore_signal(
        barrier, 1, device_id={"fsdp": fn["Z"], "tenant": tn["Z"]}, device_id_type=MESH
    )

    def slot(q, fi, ci):
        return wall.at[q, pl.ds((2 * fi + ci) * SUB, SUB)]

    def part(q, fi, ci, h):
        return wall.at[q, pl.ds((2 * fi + ci) * SUB + h * (SUB // 2), SUB // 2)]

    wloc = pltpu.make_async_copy(w_h, wall.at[:, pl.ds((2 * f + c) * SUB, SUB)], lsem.at[0])
    ucol = pl.ds(pl.multiple_of(j * lf, 128), lf)
    dcol = pl.ds(pl.multiple_of(j * ld, 128), ld)
    kloc = pltpu.make_async_copy(tok_h, tok, lsem.at[1])
    mloc = pltpu.make_async_copy(d_h, dmine, lsem.at[2])
    uloc = pltpu.make_async_copy(u_h.at[:, ucol], uall.at[j], lsem.at[3])
    dloc = pltpu.make_async_copy(d_h.at[:, dcol], dall.at[j], lsem.at[4])
    cloc = pltpu.make_async_copy(cot_h, cot, lsem.at[5])
    for d in [wloc, kloc, mloc, uloc, dloc, cloc]:
        d.start()

    def fs(i):
        return {"fsdp": fn[i]}

    def w_send(q, name, rsem, to, src=None):
        ref = slot(q, fn[name] if name else f, c) if src is None else src
        go(ref, ref, wss, rsem, to)

    def w_got(q, k, ref):
        got(ref, wrs.at[q, k])

    def w_A(q):
        w_send(q, None, wrs.at[q, 1], fs("R"))
        w_send(q, None, wrs.at[q, 2], fs("L"))
        w_send(q, None, wrs.at[q, 0], fs("Z"))
        w_send(q, None, prs.at[q], partner)

    def w_B(q):
        w_got(q, 0, slot(q, fn["Z"], c))
        w_send(q, "Z", wrs.at[q, 3], fs("R"))
        w_send(q, "Z", wrs.at[q, 4], fs("L"))
        w_send(q, "Z", prs.at[q], partner)

    def w_CD(q, left, right, kl, kr, ko):
        w_got(q, kl, slot(q, fn[left], c))
        w_send(q, left, wrs.at[q, ko], fs("R"), part(q, fn[left], c, 0))
        w_send(q, left, prs.at[q], partner)
        w_got(q, kr, slot(q, fn[right], c))
        w_send(q, right, wrs.at[q, ko], fs("L"), part(q, fn[right], c, 1))
        w_send(q, right, prs.at[q], partner)

    def w_C(q):
        w_CD(q, "L", "R", 1, 2, 5)

    def w_D(q):
        w_CD(q, "LZ", "RZ", 3, 4, 6)

    def w_E(q):
        for name, k in (("O", 5), ("OZ", 6)):
            w_got(q, k, slot(q, fn[name], c))
            w_send(q, name, prs.at[q], partner)

    def x_C(q):
        for name, k, h, kz, to in (("L", 1, 0, 3, "R"), ("R", 2, 1, 4, "L")):
            w_got(q, k, slot(q, fn[name], c))
            w_send(q, name, wrs.at[q, 5], fs(to), part(q, fn[name], c, h))
            w_send(q, name, wrs.at[q, kz], fs("Z"))
            w_send(q, name, prs.at[q], partner)

    def x_D(q):
        for name, k in (("Z", 0), ("LZ", 3), ("RZ", 4)):
            w_got(q, k, slot(q, fn[name], c))
            w_send(q, name, prs.at[q], partner)

    def x_O(q):
        w_got(q, 5, slot(q, fn["O"], c))
        w_send(q, "O", wrs.at[q, 6], fs("Z"))
        w_send(q, "O", prs.at[q], partner)

    def x_E(q):
        w_got(q, 6, slot(q, fn["OZ"], c))
        w_send(q, "OZ", prs.at[q], partner)

    def w_P(q):
        got(wall.at[q, pl.ds(0, 8 * SUB)], prs.at[q])

    def te(i):
        return {"tenant": tn[i]}

    tq = (pl.ds(0, 3), pl.ds(3, 2))

    def t_ref(ji, p, h=None):
        rows_ = slice(None) if h is None else pl.ds(h * half, half)
        return tokq.at[ji, tq[p], rows_]

    def t_send(p, ji, k, to, h=None):
        ref = t_ref(ji, p, h)
        go(ref, ref, tss, trs.at[p, k], to)

    def pieces(v):
        return [
            jnp.concatenate([v[:, SUB * q : SUB * q + SUB], v[:, 320 + SUB * q : 384 + SUB * q]], axis=1)
            for q in range(ROUNDS)
        ]

    def t_make():
        kloc.wait()
        for q, v in enumerate(pieces(tok[...])):
            tokq[j, q] = v

    def dq_make():
        mloc.wait()
        for i in range(8):
            for q, v in enumerate(pieces(dmine[:, ld * i : ld * i + ld])):
                dq[q, :, 128 * i : 128 * i + 128] = v

    def t_A(p):
        t_send(p, j, 1, te("R"))
        t_send(p, j, 2, te("L"))

    def t_Z(p):
        t_send(p, j, 0, te("Z"))

    def t_B(p):
        got(t_ref(tn["Z"], p), trs.at[p, 0])
        t_send(p, tn["Z"], 3, te("R"))
        t_send(p, tn["Z"], 4, te("L"))

    def t_CD(p, left, right, kl, kr):
        got(t_ref(tn[left], p), trs.at[p, kl])
        t_send(p, tn[left], 5, te("R"), 0)
        got(t_ref(tn[right], p), trs.at[p, kr])
        t_send(p, tn[right], 5, te("L"), 1)

    def t_C(p):
        t_CD(p, "L", "R", 1, 2)

    def t_D(p):
        t_CD(p, "LZ", "RZ", 3, 4)

    def t_E(p):
        got(tokq.at[pl.ds(0, 2), tq[p]], trs.at[p, 5])

    def adapter(src, width, all_, relay, s):
        def own(ji, ci):
            return all_.at[ji, pl.ds(ci * 32, 32)]

        def out(ji):
            return src.at[pl.ds(c * 32, 32), pl.ds(pl.multiple_of(ji * width, 128), width)]

        return own, out, relay, s

    kinds = (adapter(d_h, ld, dall, dx, 0), adapter(u_h, lf, uall, ux, 1))
    cross = {"fsdp": fn["Z"], "tenant": tn["Z"]}

    def at_y(r):
        return lax.rem(y + r, 4)

    def u_cross():
        for own, out, relay, s in kinds:
            for r in (1, 2, 3, 0):
                dst = own(j, c) if r == 0 else relay.at[r]
                go(out(2 * at_y(r) + 1 - zh), dst, uss.at[s], urs.at[s, r], cross)

    def u_own():
        for own, out, relay, s in kinds:
            for r in range(1, 4):
                to = 2 * at_y(r) + zh
                go(out(to), own(j, c), uss.at[s], urs.at[s, 0], {"tenant": to})

    def u_fwd():
        for own, out, relay, s in kinds:
            for r in range(1, 4):
                got(relay.at[r], urs.at[s, r])
                to = 2 * at_y(r) + zh
                go(relay.at[r], own(tn["Z"], c), uss.at[s], urs.at[s, 4], {"tenant": to})

    def u_recv(e):
        for (own, out, relay, s), all_ in zip(kinds, (dall, uall)):
            got(all_.at[pl.ds(0, 4 - e), pl.ds(0, 32)], urs.at[s, 4 * e])
            for r in range(e, 4):
                ji = 2 * at_y(4 - r) + (1 - zh if e == 1 or r == 0 else zh)
                go(own(ji, c), own(ji, c), upss.at[s], uprs.at[s], partner)

    def u_from_partner():
        for s, all_ in ((0, dall), (1, uall)):
            got(all_.at[pl.ds(0, 7), pl.ds(0, 32)], uprs.at[s])

    def tenant_is(b, t, shape):
        return jnp.full(shape, bti[b], jnp.int32) == t

    def make_gain():
        shape = (BLOCK, 128)
        slot_ = lax.rem(lax.broadcasted_iota(jnp.int32, shape, 1), 64)
        gains = []
        for t in range(8):
            r = jnp.full(shape, ranks[t], jnp.int32)
            gains.append(jnp.where(slot_ < r, ALPHA / r.astype(F32), 0.0))
        for b in range(6):
            g = jnp.zeros(shape, F32)
            for t in range(8):
                g = jnp.where(tenant_is(b, t, g.shape), gains[t], g)
            gcomp[pl.ds(b * BLOCK, BLOCK), :] = g

    def compact(w, a, all_):
        for h in range(2):
            u = all_[pl.ds(4 * h, 4)].reshape(256, a.shape[1])
            p = dot(a[...], u, 1, 1)
            for b in range(6):
                rs = slice(b * BLOCK, (b + 1) * BLOCK)
                acc = jnp.zeros((BLOCK, BLOCK), F32)
                for t in range(4):
                    acc = jnp.where(
                        tenant_is(b, 4 * h + t, acc.shape), p[rs, 64 * t : 64 * t + 64], acc
                    )
                at = (rs, slice(64 * w, 64 * w + 64))
                cp2[at] = acc if h == 0 else cp2[at] + acc

    def b_desc(k):
        to = lax.rem(j + k, 8)
        return rc(cp2.at[pl.ds(to * 48, 48)], brecv.at[k], bss, brs, {"tenant": to})

    def b_sum():
        at = pl.ds(pl.multiple_of(j * 48, 16), 48)
        s = cp2[at, :]
        got(brecv.at[pl.ds(1, 7)], brs)
        for k in range(1, 8):
            s = s + brecv[k]
        agx[j] = (s * gcomp[at, :]).astype(BF)

    def ag_desc(k):
        return rc(agx.at[j], agx.at[j], ass_, ars, {"tenant": lax.rem(j + k, 8)})

    def ag_use():
        got(agx.at[pl.ds(0, 7)], ars)
        both = jnp.concatenate([agx[k] for k in range(8)], axis=0).astype(F32)
        for w, dst in ((0, agexp), (1, aexp)):
            for b in range(6):
                rs = slice(b * BLOCK, (b + 1) * BLOCK)
                v = both[rs, 64 * w : 64 * w + 64]
                zero = jnp.zeros_like(v)
                if w == 0:
                    agj[rs, :] = jnp.where(tenant_is(b, j, v.shape), v, zero).astype(BF)
                for t in range(0, 8, 2):
                    pair = jnp.concatenate(
                        [jnp.where(tenant_is(b, t + e, v.shape), v, zero) for e in range(2)], axis=1
                    )
                    dst[rs, 64 * t : 64 * t + 128] = pair.astype(BF)

    def lhs(q):
        return jnp.concatenate([tokq[i, q] for i in range(8)], axis=1)

    def grad_down_part():
        p = dot(agexp[...], tok[...], 0, 0)
        gpart[0, :, 0:ld] = p[:256]
        gpart[1, :, 0:ld] = p[256:]

    def grad_up_part(lo, hi):
        def body(n):
            at = pl.ds(pl.multiple_of(n * 256, 256), 256)
            to = pl.ds(pl.multiple_of(ld + n * 256, 128), 256)
            p = dot(aexp[...], cot[:, at], 0, 0)
            gpart[0, :, to] = p[:256]
            gpart[1, :, to] = p[256:]

        each(lo, hi, body)

    fx, fz = f // 2, lax.rem(f, 2)
    cols = (pl.ds(0, 1408), pl.ds(1408, 1024))

    def gx(p):
        go(gpart.at[1 - c, :, cols[p]], gpr.at[:, cols[p]], xss, xrs.at[p], partner)

    def chunk(k, p):
        at = pl.ds(pl.multiple_of(k * 32, 32), 32)
        return gpart[c, at, cols[p]] + gpr[at, cols[p]]

    def rs_z(p):
        got(gpr.at[:, cols[p]], xrs.at[p])

        def body(k):
            rss[k, :, cols[p]] = chunk(2 * k + 1 - fz, p).astype(BF)

        each(0, 4, body)
        at = (pl.ds(0, 4), slice(None), cols[p])
        go(rss.at[at], rsr.at[at], rss_s, rss_r.at[p, 0], fs("Z"))

    def fx_to(r):
        return {"fsdp": lax.rem(f + 2 * r, 8)}

    def rs_x(p):
        got(rsr.at[pl.ds(0, 4), :, cols[p]], rss_r.at[p, 0])
        for r in range(1, 4):
            k = lax.rem(fx + r, 4)
            rss[3 + r, :, cols[p]] = (
                chunk(2 * k + fz, p) + rsr[k, :, cols[p]].astype(F32)
            ).astype(BF)
            at = (3 + r, slice(None), cols[p])
            go(rss.at[at], rsr.at[at], rss_s, rss_r.at[p, 1], fx_to(r))

    def to_x(ref, p, k):
        go(ref, ref, ags_s, ags_r.at[p, k], fs("R"))
        go(ref, ref, ags_s, ags_r.at[p, k + 1], fs("L"))

    def on_x(p, left, right, k):
        for name, e, to in ((left, 0, "R"), (right, 1, "L")):
            got(agg.at[fn[name], :, cols[p]], ags_r.at[p, k + e])
            ref = agg.at[fn[name], pl.ds(16 * e, 16), cols[p]]
            go(ref, ref, ags_s, ags_r.at[p, 5], fs(to))

    def rs_sum(p):
        s = chunk(f, p) + rsr[fx, :, cols[p]].astype(F32)
        got(rsr.at[pl.ds(4, 3), :, cols[p]], rss_r.at[p, 1])
        for r in range(1, 4):
            s = s + rsr[3 + r, :, cols[p]].astype(F32)
        agg[f, :, cols[p]] = s.astype(BF)
        ref = agg.at[f, :, cols[p]]
        go(ref, ref, ags_s, ags_r.at[p, 2], fs("Z"))
        to_x(ref, p, 0)

    def ag_x(p):
        ref = agg.at[fn["Z"], :, cols[p]]
        got(ref, ags_r.at[p, 2])
        to_x(ref, p, 3)

    def ag_o(p):
        on_x(p, "L", "R", 0)

    def ag_oz(p):
        on_x(p, "LZ", "RZ", 3)

    def grads_out(p):
        got(agg.at[pl.ds(0, 2), :, cols[p]], ags_r.at[p, 5])

        def body(k):
            at = pl.ds(pl.multiple_of(k * 32, 32), 32)
            v = agg[k, :, cols[p]].astype(F32)
            if p == 0:
                gd_out[at, :] = v[:, :ld]
                gu_out[at, 0:768] = v[:, ld:]
            else:
                gu_out[at, 768:] = v

        each(0, 8, body)

    top, bottom = pl.ds(0, half), pl.ds(half, half)

    def g_near(q, e, at):
        go(gn.at[q, e, at], grecv.at[q, e, at], gns, grs.at[q], te("RL"[e]))

    def compute_g(q):
        def body(k):
            i = lax.rem(y + 2 + 3 * k, 4)
            at = pl.ds(pl.multiple_of(i * 256, 256), 256)
            p = dot(cot[...], wall[q, at, :], 1, 1) + dot(agj[...], dq[q, :, at], 1, 0)

            @pl.when(k == 0)
            def _():
                gopp[q] = p.astype(BF)
                go(gopp.at[q, top], gor.at[q, 0], gos, gors.at[q], te("R"))
                go(gopp.at[q, bottom], gor.at[q, 1], gos, gors.at[q], te("L"))

            @pl.when(k == 1)
            def _():
                gf[q, 0] = p[:half]
                gn[q, 0, half:] = p[half:].astype(BF)
                g_near(q, 0, bottom)

            @pl.when(k == 2)
            def _():
                gown[q] = p

            @pl.when(k == 3)
            def _():
                gf[q, 1] = p[half:]
                gn[q, 1, :half] = p[:half].astype(BF)
                g_near(q, 1, top)

        each(0, 4, body)

    def g_acc(q):
        got(gor.at[q], gors.at[q])
        for e, at in enumerate((top, bottom)):
            gn[q, e, at] = (gf[q, e] + gor[q, e].astype(F32)).astype(BF)
            g_near(q, e, at)

    def compute_h(q):
        def body(n):
            at = pl.ds(pl.multiple_of(n * 256, 256), 256)
            p = dot(lhs(q), wall[q, :, at], 1, 0)
            if q == 0:
                hacc[:, at] = p
            elif q < ROUNDS - 1:
                hacc[:, at] += p
            else:
                u = uall[:, :, at].reshape(512, 256)
                hid_out[:, at] = (hacc[:, at] + p + dot(aexp[...], u, 1, 0)).astype(BF)

        each(0, lf // 256, body)

    def g_sum(q):
        got(grecv.at[q], grs.at[q])
        mine = pl.ds(pl.multiple_of(zh * 128, 128), 128)
        other = pl.ds(pl.multiple_of(128 - zh * 128, 128), 128)

        def total(at):
            s = gown[q, :, at]
            for k in range(2):
                s = s + grecv[q, k, :, at].astype(F32)
            return s

        gzs[q] = total(other).astype(BF)
        go(gzs.at[q], gzr.at[q], zss, zrs, te("Z"))
        gown[q, :, mine] = total(mine)

    def gt_final():
        mine = pl.ds(pl.multiple_of(zh * 128, 128), 128)
        got(gzr, zrs)

        def body(b):
            at = pl.ds(pl.multiple_of(b * BLOCK, BLOCK), BLOCK)
            s = [gown[q, at, mine] + gzr[q, at, :].astype(F32) for q in range(ROUNDS)]
            row = jnp.concatenate([v[:, :64] for v in s] + [v[:, 64:] for v in s], axis=1)
            gt_out[at, :] = row.astype(BF)

        each(0, 6, body)

    pl.semaphore_wait(barrier, 16)
    u_cross()
    u_own()
    wloc.wait()
    w_A(0)
    w_A(1)
    t_make()
    t_A(0)
    dq_make()
    make_gain()
    w_B(0)
    w_C(0)
    w_A(2)
    u_fwd()
    t_A(1)
    t_Z(0)
    t_Z(1)
    t_C(0)
    u_recv(0)
    w_D(0)
    w_B(1)
    w_C(1)
    w_A(3)
    u_recv(1)
    uloc.wait()
    dloc.wait()
    cloc.wait()
    u_from_partner()
    compact(0, cot, uall)
    compact(1, tok, dall)
    each(1, 8, lambda k: b_desc(k).start())
    t_C(1)
    t_B(1)
    w_E(0)
    b_sum()
    each(1, 8, lambda k: ag_desc(k).start())
    t_B(0)
    w_A(4)
    w_D(1)
    x_C(2)
    ag_use()
    w_P(0)
    compute_g(0)
    w_B(3)
    w_C(3)
    grad_down_part()
    grad_up_part(0, 3)
    gx(0)
    grad_up_part(3, 7)
    gx(1)
    w_E(1)
    w_B(4)
    x_O(2)
    rs_z(0)
    t_D(0)
    t_D(1)
    w_P(1)
    compute_g(1)
    g_acc(0)
    x_D(2)
    w_D(3)
    w_C(4)
    rs_z(1)
    x_E(2)
    w_P(2)
    compute_g(2)
    g_acc(1)
    w_D(4)
    t_E(0)
    t_E(1)
    compute_h(0)
    w_E(3)
    rs_x(0)
    w_P(3)
    compute_g(3)
    g_acc(2)
    g_sum(0)
    w_E(4)
    rs_x(1)
    compute_h(1)
    rs_sum(0)
    w_P(4)
    compute_g(4)
    g_acc(3)
    rs_sum(1)
    g_sum(1)
    compute_h(2)
    ag_o(0)
    g_sum(2)
    ag_x(0)
    g_acc(4)
    ag_x(1)
    compute_h(3)
    ag_o(1)
    g_sum(3)
    g_sum(4)
    ag_oz(0)
    ag_oz(1)
    compute_h(4)
    grads_out(0)
    grads_out(1)
    gt_final()

    gone(wall.at[:, pl.ds(0, 15 * SUB)], wss)
    gone(tokq.at[pl.ds(0, 7)], tss)
    for s, all_ in ((0, dall), (1, uall)):
        gone(all_.at[pl.ds(0, 5)], uss.at[s])
        gone(all_.at[pl.ds(0, 7), pl.ds(0, 32)], upss.at[s])
    gone(brecv.at[pl.ds(0, 7)], bss)
    gone(agx.at[pl.ds(0, 7)], ass_)
    gone(gopp, gos)
    gone(gn, gns)
    gone(gzs, zss)
    gone(gpr, xss)
    gone(rss.at[pl.ds(0, 7)], rss_s)
    gone(agg.at[pl.ds(0, 7)], ags_s)


def store(*refs):
    sems = refs[8]
    copies = [pltpu.make_async_copy(refs[i], refs[4 + i], sems.at[i]) for i in range(4)]
    for d in copies:
        d.start()
    for d in copies:
        d.wait()


def shards(tokens, bti, ranks, w, down, up, cot):
    rows, ld = tokens.shape
    lf = cot.shape[1]
    up = up.reshape(up.shape[1:])
    w = w.reshape(ROUNDS, SUB, lf)
    down = down.reshape(down.shape[1:])
    dma = pltpu.SemaphoreType.DMA
    vm = pltpu.VMEM
    smem = pl.BlockSpec(memory_space=pltpu.SMEM)
    hbm = pl.BlockSpec(memory_space=pl.ANY)
    out = pl.BlockSpec(memory_space=pltpu.VMEM)
    half = rows // 2
    hid, gt, gd, gu = pl.pallas_call(
        kernel,
        out_shape=(
            pltpu.VMEM((rows, lf), BF),
            pltpu.VMEM((rows, ld), BF),
            pltpu.VMEM((256, ld), F32),
            pltpu.VMEM((256, lf), F32),
        ),
        in_specs=[smem, smem, hbm, hbm, hbm, hbm, hbm],
        out_specs=(out, out, out, out),
        scratch_shapes=[
            vm((rows, ld), BF),
            vm((ROUNDS, 64, 1024), BF),
            vm((rows, lf), BF),
            vm((ROUNDS, 1024, lf), BF),
            vm((8, ROUNDS, rows, 128), BF),
            vm((64, 5120), BF),
            vm((8, 64, lf), BF),
            vm((8, 64, ld), BF),
            vm((4, 32, lf), BF),
            vm((4, 32, ld), BF),
            vm((rows, lf), F32),
            vm((ROUNDS, rows, 256), BF),
            vm((ROUNDS, 2, rows, 256), BF),
            vm((ROUNDS, 2, half, 256), F32),
            vm((ROUNDS, 2, half, 256), BF),
            vm((ROUNDS, rows, 256), F32),
            vm((ROUNDS, 2, rows, 256), BF),
            vm((ROUNDS, rows, 128), BF),
            vm((ROUNDS, rows, 128), BF),
            vm((rows, 128), F32),
            vm((rows, 128), F32),
            vm((8, 48, 128), F32),
            vm((8, 48, 128), BF),
            vm((rows, 64), BF),
            vm((rows, 512), BF),
            vm((rows, 512), BF),
            vm((2, 256, ld + lf), F32),
            vm((256, ld + lf), F32),
            vm((8, 32, ld + lf), BF),
            vm((8, 32, ld + lf), BF),
            vm((8, 32, ld + lf), BF),
            dma((6,)),
            dma,
            dma((ROUNDS, 7)),
            dma((ROUNDS,)),
            dma,
            dma((2, 6)),
            dma((2,)),
            dma((2, 5)),
            dma((2,)),
            dma((2,)),
            dma,
            dma,
            dma,
            dma,
            dma,
            dma((ROUNDS,)),
            dma,
            dma((ROUNDS,)),
            dma,
            dma,
            dma,
            dma((2,)),
            dma,
            dma((2, 2)),
            dma,
            dma((2, 6)),
        ],
        compiler_params=pltpu.CompilerParams(
            collective_id=0, has_side_effects=True, vmem_limit_bytes=58 << 20
        ),
    )(bti, ranks, tokens, w, down, up, cot)
    kept = [pltpu.with_memory_space_constraint(r, pltpu.VMEM) for r in (hid, gt, gd, gu)]
    hid, gt, gd, gu = pl.pallas_call(
        store,
        out_shape=tuple(jax.ShapeDtypeStruct(r.shape, r.dtype) for r in kept),
        in_specs=[out] * 4,
        out_specs=[hbm] * 4,
        scratch_shapes=[dma((4,))],
        compiler_params=pltpu.CompilerParams(vmem_limit_bytes=1 << 20),
    )(*kept)
    return hid, gt, gd.reshape(4, 64, ld), gu.reshape(4, 64, lf)


def solution(mesh):
    return jax.shard_map(
        shards,
        mesh=mesh,
        in_specs=(
            P(("fsdp", "dp"), "tenant"),
            P(("fsdp", "dp")),
            P(),
            P(("fsdp", "dp"), "tenant"),
            P("tenant", None, None),
            P("tenant", None, None),
            P(("fsdp", "dp"), "tenant"),
        ),
        out_specs=(
            P(("fsdp", "dp"), "tenant"),
            P(("fsdp", "dp"), "tenant"),
            P("dp", None, "tenant"),
            P("dp", None, "tenant"),
        ),
        check_vma=False,
    )
```
